32 devices in a mesh: gz: 4 (over z), gy: 2 (over y), gx: 4 (over x, core).
Axes of the slice: x: 2, y: 2, z: 4, core: 2. Of those that a mesh axis runs over, the one named last changes fastest.
Arguments:
- velocity: float32 [3, 128, 32, 512], P(None, 'gx', 'gy', 'gz'), may hold values from -3.5 to 5.5
- pressure: float32 [128, 32, 512], P('gx', 'gy', 'gz'), may hold values from -6 to 6
- voidage: float32 [128, 32, 512], P('gx', 'gy', 'gz'), may hold values from 0.5 to 0.95
- particle_vel: float32 [3, 128, 32, 512], P(None, 'gx', 'gy', 'gz'), may hold values from -6 to 6
- forcing: float32 [1], replicated, may hold values from 0.5 to 2
- target_flux: float32 [1], replicated, may hold values from 0.5 to 1.5
Outputs:
- vel_new: float32 [3, 128, 32, 512], P(None, 'gx', 'gy', 'gz')
- source: float32 [128, 32, 512], P('gx', 'gy', 'gz')
- forcing_new: float32 [1], replicated
The draws below stay inside these ranges and needn't reach their ends.
All inputs are finite; a program needn't handle non-finite values.
Results may differ from the reference program's by a relative error of at most 0.000079.
Values sent between devices are 32-bit elements; how exact they have to be, the bound alone decides.
A program may use at most 64 MiB of HBM per device.

```python
import jax
import jax.numpy as jnp
from jax import lax

NX = 128
NY = 32
NZ = 512


def draw_velocity(key, part):
    jitter_field = jnp.clip(jax.random.normal(key, (3, NX, NY, NZ), jnp.float32), -3.5, 3.5)
    mean_lift = 2.0
    upward_mask = (jnp.arange(3) == 2).astype(jnp.float32).reshape(3, 1, 1, 1)
    return (jitter_field + mean_lift * upward_mask).astype(jnp.float32)


def levels(stream_key, shape, split, low, top_value):
    factor_of = 1.0
    for dim, shards_of in split:
        draws = jax.random.uniform(jax.random.fold_in(jax.random.fold_in(stream_key, 6), dim), (shards_of,), jnp.float32, low / len(split), top_value / len(split))
        factor_of = factor_of * jnp.repeat(jnp.exp(draws), shape[dim] // shards_of).reshape((-1,) + (1,) * (len(shape) - 1 - dim))
    return factor_of


def noise(key, extent, deviation, reach, split=(), kind=jnp.bfloat16):
    result = jax.random.normal(key, extent, jnp.float32) * deviation
    if len(split) > 0:
        result = levels(key, extent, split, -0.22, 0.18) * result
    return jnp.clip(result, min=-reach, max=reach).astype(kind)


def setup_inputs(seed: int = 0) -> dict:
    seeds = jax.random.split(jax.random.key(seed), 7)
    velocity = draw_velocity(jax.random.fold_in(seeds[6], 71), 0)
    pressure = noise(seeds[1], (NX, NY, NZ), 1.0, 6.0, ((0, 4), (1, 2), (2, 4)), jnp.float32)
    voidage = jnp.clip(0.5 + 0.45 * jax.random.uniform(seeds[2], (NX, NY, NZ), jnp.float32) ** levels(seeds[2], (NX, NY, NZ), ((0, 4), (1, 2), (2, 4)), -0.2, 0.2), 0.5, 0.95)
    particle_vel = noise(seeds[3], (3, NX, NY, NZ), 1.0, 6.0, ((1, 4), (2, 2), (3, 4)), jnp.float32)
    forcing = jnp.clip(jax.random.uniform(seeds[4], (1,), jnp.float32, 0.5, 2.0), 0.5, 2.0)
    target_flux = jnp.clip(jax.random.uniform(seeds[5], (1,), jnp.float32, 0.5, 1.5), 0.5, 1.5)
    return {"velocity": velocity, "pressure": pressure, "voidage": voidage, "particle_vel": particle_vel, "forcing": forcing, "target_flux": target_flux}


time_step = 0.2
viscosity = 0.1
drag_scale = 1.0

def shifted(field, axis_no, offset):
    slices = [slice(1, -1)] * 3
    length = field.shape[field.ndim - 3 + axis_no]
    slices[axis_no] = slice(1 + offset, length - 1 + offset)
    return field[tuple([slice(None)] * (field.ndim - 3) + slices)]

def upward():
    return (jnp.arange(3) == 2).astype(jnp.float32).reshape(3, 1, 1, 1)

def predict(vel_pad, pres_pad, voidage, particle_vel, forcing):
    centre = shifted(vel_pad, 0, 0)
    advection = jnp.zeros_like(centre)
    laplace = -6.0 * centre
    grads = []
    for axis_no in range(3):
        upper = shifted(vel_pad, axis_no, 1)
        lower = shifted(vel_pad, axis_no, -1)
        advection = advection + centre[axis_no] * (upper - lower) * 0.5
        laplace = laplace + upper + lower
        grads.append((shifted(pres_pad, axis_no, 1) - shifted(pres_pad, axis_no, -1)) * 0.5)
    forces = -advection + viscosity * laplace - jnp.stack(grads) + forcing * upward()
    slip_speed = jnp.sqrt(lax.optimization_barrier(jnp.sum((centre - particle_vel) ** 2, axis=0)))
    drag_rate = drag_scale * (1.0 - voidage) * voidage ** (-2.65) * (1.0 + slip_speed)
    return (centre + time_step * (forces + drag_rate * particle_vel)) / (1.0 + time_step * drag_rate)

def reference(velocity, pressure, voidage, particle_vel, forcing, target_flux):
    vel_pad = jnp.pad(velocity, ((0, 0), (1, 1), (1, 1), (0, 0)))
    vel_pad = jnp.pad(vel_pad, ((0, 0), (0, 0), (0, 0), (1, 1)), mode='wrap')
    pres_pad = jnp.pad(pressure, ((0, 0), (0, 0), (1, 1)), mode='wrap')
    pres_pad = jnp.pad(pres_pad, ((1, 1), (1, 1), (0, 0)), mode='edge')
    ustar = predict(vel_pad, pres_pad, voidage, particle_vel, forcing[0])
    flow_sum = jnp.sum(voidage * ustar[2])
    void_sum = jnp.sum(voidage)
    cells = voidage.size
    force_step = (target_flux[0] * cells - flow_sum) / (time_step * void_sum)
    vel_new = ustar + time_step * force_step * upward()
    flux = voidage * vel_new
    flux_pad = jnp.pad(flux, ((0, 0), (1, 1), (1, 1), (0, 0)))
    flux_pad = jnp.pad(flux_pad, ((0, 0), (0, 0), (0, 0), (1, 1)), mode='wrap')
    source = jnp.zeros_like(voidage)
    for axis_no in range(3):
        source = source + (shifted(flux_pad[axis_no], axis_no, 1) - shifted(flux_pad[axis_no], axis_no, -1)) * 0.5
    return (vel_new, source, forcing + force_step)
```

```python
import functools
import math

import jax
import jax.numpy as jnp
from jax import lax
from jax.experimental import pallas as pl
from jax.experimental.pallas import tpu as pltpu
from jax.sharding import PartitionSpec as P

time_step = 0.2
viscosity = 0.1
drag_scale = 1.0
MESH = pl.DeviceIdType.MESH
DIRECT_LIMIT = 64


def ring_index(axes):
    index = 0
    for axis in axes:
        index = index * lax.axis_size(axis) + lax.axis_index(axis)
    return index


def ring_device(axes, index):
    device = {}
    for axis in reversed(axes):
        size = lax.axis_size(axis)
        device[axis] = lax.rem(index, size)
        index = lax.div(index, size)
    return device


def kernel(
    sizes, greet, phases,
    vel_hbm, pres_hbm, void_hbm, part_hbm, forcing, target,
    ustar, div, slope, lines,
    blk, vp, inv, weight, flux, acc, ypack, yhalo, zpack, zhalo, cpack, chalo,
    vzpack, vzhalo, fypack, fyhalo, fxhalo, fzpack, fzhalo, slots,
    load_sem, send, recv, sum_send, sum_recv, entered,
):
    gx, gy, gz = sizes
    nx, ny, nz = div.shape
    x_at, y_at, z_at = (lax.axis_index(a) for a in ("gx", "gy", "gz"))
    not_low_x, not_high_x = x_at > 0, x_at < gx - 1
    not_low_y, not_high_y = y_at > 0, y_at < gy - 1
    z_up, z_down = lax.rem(z_at + 1, gz), lax.rem(z_at + gz - 1, gz)
    z_first, z_last = z_at == 0, z_at == gz - 1

    inside = pl.ds(1, nx)
    for load in (
        pltpu.make_async_copy(vel_hbm, blk.at[pl.ds(1, 3), inside], load_sem.at[0]),
        pltpu.make_async_copy(pres_hbm, blk.at[0, inside], load_sem.at[0]),
        pltpu.make_async_copy(void_hbm, vp.at[0], load_sem.at[1]),
        pltpu.make_async_copy(part_hbm, vp.at[pl.ds(1, 3)], load_sem.at[1]),
    ):
        load.start()

    barrier = pltpu.get_barrier_semaphore()
    peers = 0
    for axes in greet:
        count = math.prod(lax.axis_size(a) for a in axes)
        me = ring_index(axes)
        for k in range(1, count):
            pl.semaphore_signal(
                barrier, inc=1, device_id=ring_device(axes, lax.rem(me + k, count)),
                device_id_type=MESH,
            )
        peers += count - 1

    lane = lax.broadcasted_iota(jnp.int32, (ny, nz), 1)
    row = lax.broadcasted_iota(jnp.int32, (ny, nz), 0)
    zero = jnp.zeros((ny, nz), jnp.float32)

    def pack_z(fields, read, at=0):
        low = high = zero
        for f in range(fields):
            for x in range(nx):
                turned = read(f, x)
                to = at + f * nx + x
                if to % nz:
                    turned = pltpu.roll(turned, to % nz, 1)
                low = jnp.where(lane == to, turned, low)
                high = jnp.where(lane == (to + nz - 1) % nz, turned, high)
        return low, high

    def copy_to(src, dst, send_at, recv_at, axis, device):
        return pltpu.make_async_remote_copy(
            src, dst, send.at[send_at], recv.at[recv_at],
            device_id={axis: device}, device_id_type=MESH)

    def exchange(low, high, dst_low, dst_high, sends, recvs, axis, up, down):
        return (copy_to(high, dst_low, sends[0], recvs[0], axis, up),
                copy_to(low, dst_high, sends[1], recvs[1], axis, down))

    def start(pair, high, low):
        pl.when(high)(pair[0].start)
        pl.when(low)(pair[1].start)

    def finish(pair, high, low):
        pl.when(low)(pair[0].wait_recv)
        pl.when(high)(pair[1].wait_recv)

    def drain(pair, high, low):
        pl.when(high)(pair[0].wait_send)
        pl.when(low)(pair[1].wait_send)

    up_x, down_x = jnp.minimum(x_at + 1, gx - 1), jnp.maximum(x_at - 1, 0)
    up_y, down_y = jnp.minimum(y_at + 1, gy - 1), jnp.maximum(y_at - 1, 0)
    rest = pl.ds(0, 3)

    def along_x(fields, recvs):
        return exchange(blk.at[fields, 1], blk.at[fields, nx], blk.at[fields, 0], blk.at[fields, nx + 1],
                        (0, 1), recvs, "gx", up_x, down_x)

    def along_y(fields, recvs):
        return exchange(ypack.at[0, fields], ypack.at[1, fields], yhalo.at[0, fields], yhalo.at[1, fields],
                        (2, 3), recvs, "gy", up_y, down_y)

    x1, x1_rest = along_x(3, (0, 1)), along_x(rest, (2, 3))
    y1, y1_rest = along_y(3, (4, 5)), along_y(rest, (6, 7))
    z1 = exchange(zpack.at[0], zpack.at[1], zhalo.at[0], zhalo.at[1], (4, 4), (8, 9), "gz", z_up, z_down)
    zv = exchange(vzpack.at[0], vzpack.at[1], vzhalo.at[0], vzhalo.at[1], (5, 5), (10, 10), "gz", z_up, z_down)
    zc = copy_to(cpack, chalo, 6, 11, "gz", z_up)

    pltpu.make_async_copy(blk.at[:, inside], blk.at[:, inside], load_sem.at[0]).wait()
    for f in (3, 0, 1, 2):
        ypack[0, f] = blk[f, inside, 0, :]
        ypack[1, f] = blk[f, inside, ny - 1, :]
    low, high = pack_z(4, lambda f, x: blk[f, x + 1])
    zpack[0] = low
    zpack[1] = high
    pl.semaphore_wait(barrier, peers)
    for copy in z1:
        copy.start()
    start(y1, not_high_y, not_low_y)
    start(x1, not_high_x, not_low_x)
    start(x1_rest, not_high_x, not_low_x)
    start(y1_rest, not_high_y, not_low_y)

    spread = len(phases) < len(greet)
    if spread:
        for k in range(1, gz):
            pl.semaphore_signal(
                entered, inc=1, device_id={"gz": lax.rem(z_at + k, gz)}, device_id_type=MESH)

    def wall_x(within, halo_plane, edge_plane):
        @pl.when(jnp.logical_not(within))
        def _():
            for f in range(1, 4):
                blk[f, halo_plane] = zero
            blk[0, halo_plane] = blk[0, edge_plane]

    wall_x(not_low_x, 0, 1)
    wall_x(not_high_x, nx + 1, nx)

    def wall_y(within, side):
        @pl.when(jnp.logical_not(within))
        def _():
            for f in range(1, 4):
                yhalo[side, f] = jnp.zeros((nx, nz), jnp.float32)
            yhalo[side, 0] = ypack[side, 0]

    wall_y(not_low_y, 0)
    wall_y(not_high_y, 1)

    pltpu.make_async_copy(vp, vp, load_sem.at[1]).wait()
    force = forcing[0]

    def drag_body(x, total):
        v = vp[0, x]
        c = [blk[1 + k, x + 1] for k in range(3)]
        q = [vp[1 + k, x] for k in range(3)]
        slip = jnp.sqrt(sum((c[k] - q[k]) ** 2 for k in range(3)))
        drag = drag_scale * (1.0 - v) * jnp.exp(-2.65 * jnp.log(v)) * (1.0 + slip)
        step_drag = time_step * drag
        inverse = 1.0 / (1.0 + step_drag)
        inv[x] = inverse
        weight[x] = v * inverse
        for k in range(3):
            ustar[k, x] = c[k] + step_drag * q[k]
        return total + v

    void_total = lax.fori_loop(0, nx, drag_body, zero, unroll=4)

    w_low, w_high = pack_z(1, lambda f, x: weight[x], 3 * nx)

    def coefficients(face, w, sign, at):
        upward = w * (time_step * viscosity + (sign * 0.5 * time_step) * face)
        pressed = (sign * 0.5 * time_step) * pltpu.roll(w, nz - 3 * nx, 1)
        return jnp.where(at < nx, pressed,
                         jnp.where((at >= 3 * nx) & (at < 4 * nx), upward, 0.0))

    c_low = pltpu.roll(coefficients(zpack[0], w_low, 1.0, lane), nz - 1, 1)
    c_high = pltpu.roll(coefficients(zpack[1], w_high, -1.0, lax.rem(lane + 1, nz)), 1, 1)
    cpack[...] = c_high
    pl.when(z_last)(zc.start)

    def stencil(x, k):
        p = x + 1
        centre = [blk[1 + f, p] for f in range(3)]

        def pair(f, axis_no):
            if axis_no == 0:
                return blk[f, p - 1], blk[f, p + 1]
            field = blk[f, p]
            if axis_no == 1:
                return (jnp.where(row == 0, 0.0, pltpu.roll(field, 1, 0)),
                        jnp.where(row == ny - 1, 0.0, pltpu.roll(field, ny - 1, 0)))
            return (jnp.where(lane == 0, 0.0, pltpu.roll(field, 1, 1)),
                    jnp.where(lane == nz - 1, 0.0, pltpu.roll(field, nz - 1, 1)))

        advect = total = None
        for axis_no in range(3):
            low, high = pair(1 + k, axis_no)
            term = centre[axis_no] * (high - low)
            both = high + low
            advect = term if advect is None else advect + term
            total = both if total is None else total + both
        low, high = pair(0, k)
        forces = (viscosity * (total - 6.0 * centre[k])
                  - 0.5 * (advect + (high - low)))
        if k == 2:
            forces = forces + force
        value = ustar[k, x] + time_step * forces
        ustar[k, x] = value * inv[x]
        return value

    def upward_body(i, flow):
        for x in (1 + 2 * i, 2 + 2 * i):
            flow = flow + weight[x] * stencil(x, 2)
        return flow

    flow = lax.fori_loop(0, (nx - 2) // 2, upward_body, zero, unroll=3)

    def along_y_coefficients(side, sign):
        w = weight[:, 0 if side == 0 else ny - 1, :]
        return w * (time_step * viscosity + (sign * 0.5 * time_step) * ypack[side, 2])

    cy_low, cy_high = along_y_coefficients(0, 1.0), along_y_coefficients(1, -1.0)

    def fold(value):
        value = jnp.sum(value, axis=0, keepdims=True)
        return value + pltpu.roll(value, nz // 2, 1)

    line = lax.broadcasted_iota(jnp.int32, (1, nz), 1)
    void_line = fold(void_total)

    finish(x1, not_high_x, not_low_x)
    flow = flow + weight[0] * stencil(0, 2) + weight[nx - 1] * stencil(nx - 1, 2)
    acc[...] = flow
    finish(y1, not_high_y, not_low_y)
    y_line = jnp.sum(cy_low * yhalo[0, 3] + cy_high * yhalo[1, 3], axis=0, keepdims=True)
    z1[0].wait_recv()
    acc[...] += c_low * zhalo[0]

    @pl.when(jnp.logical_not(z_last))
    def _():
        z1[1].wait_recv()
        acc[...] += c_high * zhalo[1]

    @pl.when(z_first)
    def _():
        zc.wait_recv()
        acc[...] += chalo[...] * zpack[0]

    flow_line = jnp.sum(acc[...], axis=0, keepdims=True) + y_line
    flow_line = flow_line + pltpu.roll(flow_line, nz // 2, 1)
    partial = jnp.where(line < nz // 2, flow_line, void_line)

    if spread:
        pl.semaphore_wait(entered, gz - 1)

    def members(which):
        axes = phases[which]
        count = math.prod(lax.axis_size(a) for a in axes)
        base = sum(math.prod(lax.axis_size(a) for a in phases[w]) for w in range(which))
        return axes, count, base, ring_index(axes)

    def sum_copy(which, src, dst, device):
        return pltpu.make_async_remote_copy(
            src, dst, sum_send.at[which], sum_recv.at[which], device_id=device, device_id_type=MESH)

    def send_sum(which, value):
        axes, count, base, me = members(which)
        slots[base + me] = value
        for k in range(count - 1):
            other = jnp.where(k < me, k, k + 1)
            sum_copy(which, slots.at[base + me], slots.at[base + me], ring_device(axes, other)).start()

    def all_sums(which):
        axes, count, base, me = members(which)
        others = slots.at[pl.ds(base, count - 1)]
        return sum_copy(which, others, others, ring_device(axes, lax.rem(me + 1, count)))

    def recv_sum(which):
        axes, count, base, me = members(which)
        all_sums(which).wait_recv()
        return jnp.sum(slots[pl.ds(base, count)], axis=0)

    send_sum(0, partial)

    pl.when(z_last)(z1[1].wait_recv)

    first_row = row == 0
    last_row = row == ny - 1
    first_lane = lane == 0
    last_lane = lane == nz - 1
    row_sign = jnp.where(first_row, 1.0, jnp.where(last_row, -1.0, 0.0))
    lane_sign = jnp.where(first_lane, 1.0, jnp.where(last_lane, -1.0, 0.0))
    row_sign, lane_sign = (s * (0.5 * time_step) for s in (row_sign, lane_sign))
    row_visc, lane_visc = (jnp.abs(s) * (2.0 * viscosity) for s in (row_sign, lane_sign))

    def join_z(halo):
        low = pltpu.roll(halo[0], 1, 1)
        high = pltpu.roll(halo[1], nz - 1, 1)
        even = lax.rem(lane, 2) == 0
        return jnp.where(even, low, high), jnp.where(even, high, low)

    joined = join_z(zhalo)

    def unpack(which, at):
        return pltpu.roll(which, lax.rem(2 * nz - at, nz), 1)

    def rows(f, x):
        return jnp.where(
            row < ny // 2,
            jnp.broadcast_to(yhalo[0, f, pl.ds(x, 1), :], (ny, nz)),
            jnp.broadcast_to(yhalo[1, f, pl.ds(x, 1), :], (ny, nz)))

    def correct(x, which, components):
        by_row = row_visc + row_sign * blk[2, x + 1]
        by_lane = lane_visc + lane_sign * blk[3, x + 1]
        inverse, v = inv[x], vp[0, x]
        for k in components:
            value = by_row * rows(1 + k, x) + by_lane * unpack(which, (1 + k) * nx + x)
            if k == 1:
                value = value + row_sign * rows(0, x)
            if k == 2:
                value = value + lane_sign * unpack(which, x)
            value = ustar[k, x] + value * inverse
            ustar[k, x] = value
            flux[k, x] = v * value

    def correct_up_body(i, carry):
        correct(2 * i, joined[0], (2,))
        correct(2 * i + 1, joined[1], (2,))
        return carry

    lax.fori_loop(0, nx // 2, correct_up_body, 0, unroll=4)

    x2 = exchange(flux.at[0, 0], flux.at[0, nx - 1], fxhalo.at[0], fxhalo.at[1], (7, 8), (12, 13), "gx", up_x, down_x)
    y2 = exchange(fypack.at[0], fypack.at[1], fyhalo.at[0], fyhalo.at[1], (9, 10), (14, 15), "gy", up_y, down_y)
    z2 = exchange(fzpack.at[0], fzpack.at[1], fzhalo.at[0], fzhalo.at[1], (11, 11), (16, 16), "gz", z_up, z_down)
    low, high = pack_z(1, lambda f, x: flux[2, x])
    fzpack[0] = low
    fzpack[1] = high
    for copy in z2:
        copy.start()
    low, high = pack_z(1, lambda f, x: vp[0, x])
    vzpack[0] = low
    vzpack[1] = high
    for copy in zv:
        copy.start()

    def across_body(i, carry):
        for x in (1 + 2 * i, 2 + 2 * i):
            stencil(x, 0)
            stencil(x, 1)
        return carry

    lax.fori_loop(0, (nx - 2) // 2, across_body, 0)
    finish(x1_rest, not_high_x, not_low_x)
    for x in (0, nx - 1):
        stencil(x, 0)
        stencil(x, 1)
    finish(y1_rest, not_high_y, not_low_y)

    def correct_across_body(i, carry):
        correct(2 * i, joined[0], (0, 1))
        correct(2 * i + 1, joined[1], (0, 1))
        return carry

    lax.fori_loop(0, nx // 2, correct_across_body, 0, unroll=2)
    start(x2, not_high_x, not_low_x)
    fypack[0] = flux[1, :, 0, :]
    fypack[1] = flux[1, :, ny - 1, :]
    start(y2, not_high_y, not_low_y)

    for within, side in ((not_low_x, 0), (not_high_x, 1)):
        @pl.when(jnp.logical_not(within))
        def _():
            fxhalo[side] = zero
    for within, side in ((not_low_y, 0), (not_high_y, 1)):
        @pl.when(jnp.logical_not(within))
        def _():
            fyhalo[side] = jnp.zeros((nx, nz), jnp.float32)

    def source_plane(x, x_low, x_high):
        fy, fz, v = flux[1, x], flux[2, x], vp[0, x]
        y_low = jnp.where(first_row, 0.0, pltpu.roll(fy, 1, 0))
        y_high = jnp.where(last_row, 0.0, pltpu.roll(fy, ny - 1, 0))
        z_low = jnp.where(first_lane, 0.0, pltpu.roll(fz, 1, 1))
        z_high = jnp.where(last_lane, 0.0, pltpu.roll(fz, nz - 1, 1))
        v_low = jnp.where(first_lane, 0.0, pltpu.roll(v, 1, 1))
        v_high = jnp.where(last_lane, 0.0, pltpu.roll(v, nz - 1, 1))
        div[x] = 0.5 * ((x_high - x_low) + (y_high - y_low) + (z_high - z_low))
        slope[x] = (0.5 * time_step) * (v_high - v_low)

    def source_body(i, carry):
        x = 2 * i + 1
        source_plane(x, flux[0, x - 1], flux[0, x + 1])
        source_plane(x + 1, flux[0, x], flux[0, x + 2])
        return carry

    lax.fori_loop(0, nx // 2 - 1, source_body, 0, unroll=3)
    phase = 0
    while phase < len(phases) - 1:
        total = recv_sum(phase)
        phase += 1
        send_sum(phase, total)
    finish(x2, not_high_x, not_low_x)
    source_plane(0, fxhalo[0], flux[0, 1])
    source_plane(nx - 1, flux[0, nx - 2], fxhalo[1])
    finish(y2, not_high_y, not_low_y)
    copy_to(vzpack, vzhalo, 5, 10, "gz", z_up).wait()
    v_joined = join_z(vzhalo)
    copy_to(fzpack, fzhalo, 11, 16, "gz", z_up).wait()
    f_joined = join_z(fzhalo)
    row_half, lane_half = row_sign / time_step, lane_sign / time_step

    def edge_plane(x, odd):
        y_halo = jnp.where(
            row < ny // 2,
            jnp.broadcast_to(fyhalo[0, pl.ds(x, 1), :], (ny, nz)),
            jnp.broadcast_to(fyhalo[1, pl.ds(x, 1), :], (ny, nz)))
        div[x] = div[x] - row_half * y_halo - lane_half * unpack(f_joined[odd], x)
        slope[x] = slope[x] - lane_sign * unpack(v_joined[odd], x)

    def edge_body(i, carry):
        edge_plane(2 * i, 0)
        edge_plane(2 * i + 1, 1)
        return carry

    lax.fori_loop(0, nx // 2, edge_body, 0, unroll=4)

    for which in range(len(phases)):
        all_sums(which).wait_send()
    drain(along_x(slice(None), (0, 1)), not_high_x, not_low_x)
    drain(along_y(slice(None), (4, 5)), not_high_y, not_low_y)
    copy_to(zpack, zhalo, 4, 8, "gz", z_up).wait_send()
    pl.when(z_last)(zc.wait_send)
    drain(x2, not_high_x, not_low_x)
    drain(y2, not_high_y, not_low_y)

    total = recv_sum(phase)
    half = line < nz // 2
    flow_sum = jnp.sum(jnp.where(half, total, 0.0), axis=1, keepdims=True)
    void_sum = jnp.sum(jnp.where(half, 0.0, total), axis=1, keepdims=True)
    cells = float(nx * ny * nz * gx * gy * gz)
    step = (target[0] * cells - flow_sum) / (time_step * void_sum)
    lines[0] = jnp.broadcast_to(step, (1, nz)) + force
    lines[1] = jnp.broadcast_to(step, (1, nz))


def shift_kernel(ustar, div, slope, lines, vel_out, source_out, forcing_out, upward, source, sem):
    nx, ny, nz = div.shape
    half = nx // 2
    copies = [
        pltpu.make_async_copy(ustar.at[pl.ds(0, 2)], vel_out.at[pl.ds(0, 2)], sem.at[0]),
        pltpu.make_async_copy(lines.at[0], forcing_out, sem.at[1]),
    ]
    for copy in copies:
        copy.start()
    step = jnp.broadcast_to(lines[1], (ny, nz))
    for part in range(2):
        def body(i, carry):
            x = part * half + i
            upward[x] = ustar[2, x] + time_step * step
            source[x] = div[x] + step * slope[x]
            return carry

        lax.fori_loop(0, half, body, 0, unroll=8)
        planes = pl.ds(part * half, half)
        for copy in (
            pltpu.make_async_copy(upward.at[planes], vel_out.at[2, planes], sem.at[2 + 2 * part]),
            pltpu.make_async_copy(source.at[planes], source_out.at[planes], sem.at[3 + 2 * part]),
        ):
            copy.start()
            copies.append(copy)
    for copy in copies:
        copy.wait()


def local(velocity, pressure, voidage, particle_vel, forcing, target_flux):
    nx, ny, nz = voidage.shape
    sizes = tuple(lax.axis_size(a) for a in ("gx", "gy", "gz"))
    greet = (("gy", "gx"), ("gz",))
    if math.prod(sizes) <= DIRECT_LIMIT:
        phases = (("gz", "gy", "gx"),)
    else:
        phases = greet
    slot_count = sum(math.prod(lax.axis_size(a) for a in axes) for axes in phases)
    f32 = jnp.float32
    vmem = pl.BlockSpec(memory_space=pltpu.VMEM)
    smem = pl.BlockSpec(memory_space=pltpu.SMEM)
    hbm = pl.BlockSpec(memory_space=pltpu.HBM)
    dma = pltpu.SemaphoreType.DMA
    faces = [pltpu.VMEM((2, ny, nz), f32), pltpu.VMEM((2, ny, nz), f32)]
    face = [pltpu.VMEM((ny, nz), f32)]
    results = pl.pallas_call(
        functools.partial(kernel, sizes, greet, phases),
        out_shape=(
            pltpu.VMEM((3, nx, ny, nz), f32),
            pltpu.VMEM((nx, ny, nz), f32),
            pltpu.VMEM((nx, ny, nz), f32),
            pltpu.VMEM((2, 1, nz), f32),
        ),
        in_specs=[hbm] * 4 + [smem] * 2,
        out_specs=(vmem,) * 4,
        scratch_shapes=[
            pltpu.VMEM((4, nx + 2, ny, nz), f32),
            pltpu.VMEM((4, nx, ny, nz), f32),
            pltpu.VMEM((nx, ny, nz), f32),
            pltpu.VMEM((nx, ny, nz), f32),
            pltpu.VMEM((3, nx, ny, nz), f32),
        ] + face + [
            pltpu.VMEM((2, 4, nx, nz), f32),
            pltpu.VMEM((2, 4, nx, nz), f32),
        ] + faces + face + face + faces + [
            pltpu.VMEM((2, nx, nz), f32),
            pltpu.VMEM((2, nx, nz), f32),
            pltpu.VMEM((2, ny, nz), f32),
        ] + faces + [
            pltpu.VMEM((slot_count, 1, nz), f32),
            dma((2,)), dma((12,)), dma((17,)),
            dma((len(phases),)), dma((len(phases),)),
            pltpu.SemaphoreType.REGULAR,
        ],
        compiler_params=pltpu.CompilerParams(collective_id=0, has_side_effects=True),
    )(velocity, pressure, voidage, particle_vel, forcing, target_flux)
    vel_new, source, forcing_new = pl.pallas_call(
        shift_kernel,
        out_shape=(
            jax.ShapeDtypeStruct((3, nx, ny, nz), f32),
            jax.ShapeDtypeStruct((nx, ny, nz), f32),
            jax.ShapeDtypeStruct((1, nz), f32),
        ),
        in_specs=[vmem] * 4,
        out_specs=(hbm,) * 3,
        scratch_shapes=[
            pltpu.VMEM((nx, ny, nz), f32),
            pltpu.VMEM((nx, ny, nz), f32),
            dma((6,)),
        ],
    )(*(pltpu.with_memory_space_constraint(a, pltpu.VMEM) for a in results))
    return vel_new, source, forcing_new[0, :1]


def solution(mesh):
    return jax.shard_map(
        local,
        mesh=mesh,
        in_specs=(
            P(None, "gx", "gy", "gz"),
            P("gx", "gy", "gz"),
            P("gx", "gy", "gz"),
            P(None, "gx", "gy", "gz"),
            P(),
            P(),
        ),
        out_specs=(P(None, "gx", "gy", "gz"), P("gx", "gy", "gz"), P()),
        check_vma=False,
    )
```

```python
import functools
import math

import jax
import jax.numpy as jnp
from jax import lax
from jax.experimental import pallas as pl
from jax.experimental.pallas import tpu as pltpu
from jax.sharding import PartitionSpec as P

time_step = 0.2
viscosity = 0.1
drag_scale = 1.0
MESH = pl.DeviceIdType.MESH
DIRECT_LIMIT = 64


def ring_index(axes):
    index = 0
    for axis in axes:
        index = index * lax.axis_size(axis) + lax.axis_index(axis)
    return index


def ring_device(axes, index):
    device = {}
    for axis in reversed(axes):
        size = lax.axis_size(axis)
        device[axis] = lax.rem(index, size)
        index = lax.div(index, size)
    return device


def kernel(
    sizes, greet, phases,
    vel_hbm, pres_hbm, void_hbm, part_hbm, forcing, target,
    ustar, div, slope, lines,
    blk, vp, inv, weight, flux, acc, ypack, yhalo, zpack, zhalo, cpack, chalo,
    vzpack, vzhalo, fypack, fyhalo, fxhalo, fzpack, fzhalo, slots,
    load_sem, send, recv, sum_send, sum_recv, entered,
):
    gx, gy, gz = sizes
    nx, ny, nz = div.shape
    x_at, y_at, z_at = (lax.axis_index(a) for a in ("gx", "gy", "gz"))
    not_low_x, not_high_x = x_at > 0, x_at < gx - 1
    not_low_y, not_high_y = y_at > 0, y_at < gy - 1
    z_up, z_down = lax.rem(z_at + 1, gz), lax.rem(z_at + gz - 1, gz)
    z_first, z_last = z_at == 0, z_at == gz - 1

    inside = pl.ds(1, nx)
    for load in (
        pltpu.make_async_copy(vel_hbm, blk.at[pl.ds(1, 3), inside], load_sem.at[0]),
        pltpu.make_async_copy(pres_hbm, blk.at[0, inside], load_sem.at[0]),
        pltpu.make_async_copy(void_hbm, vp.at[0], load_sem.at[1]),
        pltpu.make_async_copy(part_hbm, vp.at[pl.ds(1, 3)], load_sem.at[1]),
    ):
        load.start()

    barrier = pltpu.get_barrier_semaphore()
    peers = 0
    for axes in greet:
        count = math.prod(lax.axis_size(a) for a in axes)
        me = ring_index(axes)
        for k in range(1, count):
            pl.semaphore_signal(
                barrier, inc=1, device_id=ring_device(axes, lax.rem(me + k, count)),
                device_id_type=MESH,
            )
        peers += count - 1

    lane = lax.broadcasted_iota(jnp.int32, (ny, nz), 1)
    row = lax.broadcasted_iota(jnp.int32, (ny, nz), 0)
    zero = jnp.zeros((ny, nz), jnp.float32)

    def pack_z(fields, read, at=0):
        low = high = zero
        for f in range(fields):
            for x in range(nx):
                turned = read(f, x)
                to = at + f * nx + x
                if to % nz:
                    turned = pltpu.roll(turned, to % nz, 1)
                low = jnp.where(lane == to, turned, low)
                high = jnp.where(lane == (to + nz - 1) % nz, turned, high)
        return low, high

    def copy_to(src, dst, send_at, recv_at, axis, device):
        return pltpu.make_async_remote_copy(
            src, dst, send.at[send_at], recv.at[recv_at],
            device_id={axis: device}, device_id_type=MESH)

    def exchange(low, high, dst_low, dst_high, sends, recvs, axis, up, down):
        return (copy_to(high, dst_low, sends[0], recvs[0], axis, up),
                copy_to(low, dst_high, sends[1], recvs[1], axis, down))

    def start(pair, high, low):
        pl.when(high)(pair[0].start)
        pl.when(low)(pair[1].start)

    def finish(pair, high, low):
        pl.when(low)(pair[0].wait_recv)
        pl.when(high)(pair[1].wait_recv)

    def drain(pair, high, low):
        pl.when(high)(pair[0].wait_send)
        pl.when(low)(pair[1].wait_send)

    up_x, down_x = jnp.minimum(x_at + 1, gx - 1), jnp.maximum(x_at - 1, 0)
    up_y, down_y = jnp.minimum(y_at + 1, gy - 1), jnp.maximum(y_at - 1, 0)
    rest = pl.ds(0, 3)

    def along_x(fields, recvs):
        return exchange(blk.at[fields, 1], blk.at[fields, nx], blk.at[fields, 0], blk.at[fields, nx + 1],
                        (0, 1), recvs, "gx", up_x, down_x)

    def along_y(fields, recvs):
        return exchange(ypack.at[0, fields], ypack.at[1, fields], yhalo.at[0, fields], yhalo.at[1, fields],
                        (2, 3), recvs, "gy", up_y, down_y)

    x1, x1_rest = along_x(3, (0, 1)), along_x(rest, (2, 3))
    y1, y1_rest = along_y(3, (4, 5)), along_y(rest, (6, 7))
    z1 = exchange(zpack.at[0], zpack.at[1], zhalo.at[0], zhalo.at[1], (4, 4), (8, 9), "gz", z_up, z_down)
    zv = exchange(vzpack.at[0], vzpack.at[1], vzhalo.at[0], vzhalo.at[1], (5, 5), (10, 10), "gz", z_up, z_down)
    zc = copy_to(cpack, chalo, 6, 11, "gz", z_up)

    pltpu.make_async_copy(blk.at[:, inside], blk.at[:, inside], load_sem.at[0]).wait()
    low, high = pack_z(4, lambda f, x: blk[f, x + 1])
    zpack[0] = low
    zpack[1] = high
    for f in (3, 0, 1, 2):
        ypack[0, f] = blk[f, inside, 0, :]
        ypack[1, f] = blk[f, inside, ny - 1, :]
    pltpu.make_async_copy(vp, vp, load_sem.at[1]).wait()
    force = forcing[0]

    def drag_body(x, total):
        v = vp[0, x]
        c = [blk[1 + k, x + 1] for k in range(3)]
        q = [vp[1 + k, x] for k in range(3)]
        slip = jnp.sqrt(sum((c[k] - q[k]) ** 2 for k in range(3)))
        drag = drag_scale * (1.0 - v) * jnp.exp(-2.65 * jnp.log(v)) * (1.0 + slip)
        step_drag = time_step * drag
        inverse = 1.0 / (1.0 + step_drag)
        inv[x] = inverse
        weight[x] = v * inverse
        for k in range(3):
            ustar[k, x] = c[k] + step_drag * q[k]
        return total + v

    void_total = lax.fori_loop(0, nx, drag_body, zero, unroll=4)

    w_low, w_high = pack_z(1, lambda f, x: weight[x], 3 * nx)

    def coefficients(face, w, sign, at):
        upward = w * (time_step * viscosity + (sign * 0.5 * time_step) * face)
        pressed = (sign * 0.5 * time_step) * pltpu.roll(w, nz - 3 * nx, 1)
        return jnp.where(at < nx, pressed,
                         jnp.where((at >= 3 * nx) & (at < 4 * nx), upward, 0.0))

    c_low = pltpu.roll(coefficients(zpack[0], w_low, 1.0, lane), nz - 1, 1)
    c_high = pltpu.roll(coefficients(zpack[1], w_high, -1.0, lax.rem(lane + 1, nz)), 1, 1)
    cpack[...] = c_high

    pl.semaphore_wait(barrier, peers)
    pl.when(z_last)(zc.start)
    for copy in z1:
        copy.start()
    start(y1, not_high_y, not_low_y)
    start(x1, not_high_x, not_low_x)

    spread = len(phases) < len(greet)
    if spread:
        for k in range(1, gz):
            pl.semaphore_signal(
                entered, inc=1, device_id={"gz": lax.rem(z_at + k, gz)}, device_id_type=MESH)

    def wall_x(within, halo_plane, edge_plane):
        @pl.when(jnp.logical_not(within))
        def _():
            for f in range(1, 4):
                blk[f, halo_plane] = zero
            blk[0, halo_plane] = blk[0, edge_plane]

    wall_x(not_low_x, 0, 1)
    wall_x(not_high_x, nx + 1, nx)

    def wall_y(within, side):
        @pl.when(jnp.logical_not(within))
        def _():
            for f in range(1, 4):
                yhalo[side, f] = jnp.zeros((nx, nz), jnp.float32)
            yhalo[side, 0] = ypack[side, 0]

    wall_y(not_low_y, 0)
    wall_y(not_high_y, 1)

    def stencil(x, k):
        p = x + 1
        centre = [blk[1 + f, p] for f in range(3)]

        def pair(f, axis_no):
            if axis_no == 0:
                return blk[f, p - 1], blk[f, p + 1]
            field = blk[f, p]
            if axis_no == 1:
                return (jnp.where(row == 0, 0.0, pltpu.roll(field, 1, 0)),
                        jnp.where(row == ny - 1, 0.0, pltpu.roll(field, ny - 1, 0)))
            return (jnp.where(lane == 0, 0.0, pltpu.roll(field, 1, 1)),
                    jnp.where(lane == nz - 1, 0.0, pltpu.roll(field, nz - 1, 1)))

        advect = total = None
        for axis_no in range(3):
            low, high = pair(1 + k, axis_no)
            term = centre[axis_no] * (high - low)
            both = high + low
            advect = term if advect is None else advect + term
            total = both if total is None else total + both
        low, high = pair(0, k)
        forces = (viscosity * (total - 6.0 * centre[k])
                  - 0.5 * (advect + (high - low)))
        if k == 2:
            forces = forces + force
        value = ustar[k, x] + time_step * forces
        ustar[k, x] = value * inv[x]
        return value

    def upward_body(i, flow):
        for x in (1 + 2 * i, 2 + 2 * i):
            flow = flow + weight[x] * stencil(x, 2)
        return flow

    flow = lax.fori_loop(0, (nx - 2) // 2, upward_body, zero, unroll=3)

    start(y1_rest, not_high_y, not_low_y)
    start(x1_rest, not_high_x, not_low_x)

    low, high = pack_z(1, lambda f, x: vp[0, x])
    vzpack[0] = low
    vzpack[1] = high
    for copy in zv:
        copy.start()

    def along_y_coefficients(side, sign):
        w = weight[:, 0 if side == 0 else ny - 1, :]
        return w * (time_step * viscosity + (sign * 0.5 * time_step) * ypack[side, 2])

    cy_low, cy_high = along_y_coefficients(0, 1.0), along_y_coefficients(1, -1.0)

    def fold(value):
        value = jnp.sum(value, axis=0, keepdims=True)
        return value + pltpu.roll(value, nz // 2, 1)

    line = lax.broadcasted_iota(jnp.int32, (1, nz), 1)
    void_line = fold(void_total)

    def across_body(i, carry):
        for x in (1 + 2 * i, 2 + 2 * i):
            stencil(x, 0)
            stencil(x, 1)
        return carry

    lax.fori_loop(0, (nx - 2) // 2, across_body, 0, unroll=3)
    def members(which):
        axes = phases[which]
        count = math.prod(lax.axis_size(a) for a in axes)
        base = sum(math.prod(lax.axis_size(a) for a in phases[w]) for w in range(which))
        return axes, count, base, ring_index(axes)

    def sum_copy(which, src, dst, device):
        return pltpu.make_async_remote_copy(
            src, dst, sum_send.at[which], sum_recv.at[which], device_id=device, device_id_type=MESH)

    def send_sum(which, value):
        axes, count, base, me = members(which)
        slots[base + me] = value
        for k in range(count - 1):
            other = jnp.where(k < me, k, k + 1)
            sum_copy(which, slots.at[base + me], slots.at[base + me], ring_device(axes, other)).start()

    def all_sums(which):
        axes, count, base, me = members(which)
        others = slots.at[pl.ds(base, count - 1)]
        return sum_copy(which, others, others, ring_device(axes, lax.rem(me + 1, count)))

    def recv_sum(which):
        axes, count, base, me = members(which)
        all_sums(which).wait_recv()
        return jnp.sum(slots[pl.ds(base, count)], axis=0)

    finish(x1, not_high_x, not_low_x)
    flow = flow + weight[0] * stencil(0, 2) + weight[nx - 1] * stencil(nx - 1, 2)
    acc[...] = flow
    finish(y1, not_high_y, not_low_y)
    y_line = jnp.sum(cy_low * yhalo[0, 3] + cy_high * yhalo[1, 3], axis=0, keepdims=True)
    z1[0].wait_recv()
    acc[...] += c_low * zhalo[0]

    @pl.when(jnp.logical_not(z_last))
    def _():
        z1[1].wait_recv()
        acc[...] += c_high * zhalo[1]

    def sum_up():
        flow_line = jnp.sum(acc[...], axis=0, keepdims=True) + y_line
        flow_line = flow_line + pltpu.roll(flow_line, nz // 2, 1)
        send_sum(0, jnp.where(line < nz // 2, flow_line, void_line))

    if spread:
        pl.semaphore_wait(entered, gz - 1)
    pl.when(jnp.logical_not(z_first))(sum_up)

    pl.when(z_last)(z1[1].wait_recv)

    first_row = row == 0
    last_row = row == ny - 1
    first_lane = lane == 0
    last_lane = lane == nz - 1
    row_sign = jnp.where(first_row, 1.0, jnp.where(last_row, -1.0, 0.0))
    lane_sign = jnp.where(first_lane, 1.0, jnp.where(last_lane, -1.0, 0.0))
    row_sign, lane_sign = (s * (0.5 * time_step) for s in (row_sign, lane_sign))
    row_visc, lane_visc = (jnp.abs(s) * (2.0 * viscosity) for s in (row_sign, lane_sign))

    def join_z(halo):
        low = pltpu.roll(halo[0], 1, 1)
        high = pltpu.roll(halo[1], nz - 1, 1)
        even = lax.rem(lane, 2) == 0
        return jnp.where(even, low, high), jnp.where(even, high, low)

    joined = join_z(zhalo)

    def unpack(which, at):
        return pltpu.roll(which, lax.rem(2 * nz - at, nz), 1)

    def rows(f, x):
        return jnp.where(
            row < ny // 2,
            jnp.broadcast_to(yhalo[0, f, pl.ds(x, 1), :], (ny, nz)),
            jnp.broadcast_to(yhalo[1, f, pl.ds(x, 1), :], (ny, nz)))

    def correct(x, which, components):
        by_row = row_visc + row_sign * blk[2, x + 1]
        by_lane = lane_visc + lane_sign * blk[3, x + 1]
        inverse, v = inv[x], vp[0, x]
        for k in components:
            value = by_row * rows(1 + k, x) + by_lane * unpack(which, (1 + k) * nx + x)
            if k == 1:
                value = value + row_sign * rows(0, x)
            if k == 2:
                value = value + lane_sign * unpack(which, x)
            value = ustar[k, x] + value * inverse
            ustar[k, x] = value
            flux[k, x] = v * value

    def correct_up_body(i, carry):
        correct(2 * i, joined[0], (2,))
        correct(2 * i + 1, joined[1], (2,))
        return carry

    lax.fori_loop(0, nx // 2, correct_up_body, 0, unroll=4)

    x2 = exchange(flux.at[0, 0], flux.at[0, nx - 1], fxhalo.at[0], fxhalo.at[1], (7, 8), (12, 13), "gx", up_x, down_x)
    y2 = exchange(fypack.at[0], fypack.at[1], fyhalo.at[0], fyhalo.at[1], (9, 10), (14, 15), "gy", up_y, down_y)
    z2 = exchange(fzpack.at[0], fzpack.at[1], fzhalo.at[0], fzhalo.at[1], (11, 11), (16, 16), "gz", z_up, z_down)
    low, high = pack_z(1, lambda f, x: flux[2, x])
    fzpack[0] = low
    fzpack[1] = high
    for copy in z2:
        copy.start()
    finish(x1_rest, not_high_x, not_low_x)
    for x in (0, nx - 1):
        stencil(x, 0)
        stencil(x, 1)
    finish(y1_rest, not_high_y, not_low_y)

    def correct_across_body(i, carry):
        correct(2 * i, joined[0], (0, 1))
        correct(2 * i + 1, joined[1], (0, 1))
        return carry

    lax.fori_loop(0, nx // 2, correct_across_body, 0, unroll=4)
    start(x2, not_high_x, not_low_x)
    fypack[0] = flux[1, :, 0, :]
    fypack[1] = flux[1, :, ny - 1, :]
    start(y2, not_high_y, not_low_y)

    @pl.when(z_first)
    def _():
        zc.wait_recv()
        acc[...] += chalo[...] * zpack[0]
        sum_up()

    for within, side in ((not_low_x, 0), (not_high_x, 1)):
        @pl.when(jnp.logical_not(within))
        def _():
            fxhalo[side] = zero
    for within, side in ((not_low_y, 0), (not_high_y, 1)):
        @pl.when(jnp.logical_not(within))
        def _():
            fyhalo[side] = jnp.zeros((nx, nz), jnp.float32)

    def source_plane(x, x_low, x_high):
        fy, fz, v = flux[1, x], flux[2, x], vp[0, x]
        y_low = jnp.where(first_row, 0.0, pltpu.roll(fy, 1, 0))
        y_high = jnp.where(last_row, 0.0, pltpu.roll(fy, ny - 1, 0))
        z_low = jnp.where(first_lane, 0.0, pltpu.roll(fz, 1, 1))
        z_high = jnp.where(last_lane, 0.0, pltpu.roll(fz, nz - 1, 1))
        v_low = jnp.where(first_lane, 0.0, pltpu.roll(v, 1, 1))
        v_high = jnp.where(last_lane, 0.0, pltpu.roll(v, nz - 1, 1))
        div[x] = 0.5 * ((x_high - x_low) + (y_high - y_low) + (z_high - z_low))
        slope[x] = (0.5 * time_step) * (v_high - v_low)

    def source_body(i, carry):
        x = 2 * i + 1
        source_plane(x, flux[0, x - 1], flux[0, x + 1])
        source_plane(x + 1, flux[0, x], flux[0, x + 2])
        return carry

    lax.fori_loop(0, nx // 2 - 1, source_body, 0, unroll=3)
    phase = 0
    while phase < len(phases) - 1:
        total = recv_sum(phase)
        phase += 1
        send_sum(phase, total)
    finish(x2, not_high_x, not_low_x)
    source_plane(0, fxhalo[0], flux[0, 1])
    source_plane(nx - 1, flux[0, nx - 2], fxhalo[1])
    finish(y2, not_high_y, not_low_y)
    copy_to(vzpack, vzhalo, 5, 10, "gz", z_up).wait()
    v_joined = join_z(vzhalo)
    copy_to(fzpack, fzhalo, 11, 16, "gz", z_up).wait()
    f_joined = join_z(fzhalo)
    row_half, lane_half = row_sign / time_step, lane_sign / time_step

    def edge_plane(x, odd):
        y_halo = jnp.where(
            row < ny // 2,
            jnp.broadcast_to(fyhalo[0, pl.ds(x, 1), :], (ny, nz)),
            jnp.broadcast_to(fyhalo[1, pl.ds(x, 1), :], (ny, nz)))
        div[x] = div[x] - row_half * y_halo - lane_half * unpack(f_joined[odd], x)
        slope[x] = slope[x] - lane_sign * unpack(v_joined[odd], x)

    def edge_body(i, carry):
        edge_plane(2 * i, 0)
        edge_plane(2 * i + 1, 1)
        return carry

    lax.fori_loop(0, nx // 2, edge_body, 0, unroll=16)

    for which in range(len(phases)):
        all_sums(which).wait_send()
    drain(along_x(slice(None), (0, 1)), not_high_x, not_low_x)
    drain(along_y(slice(None), (4, 5)), not_high_y, not_low_y)
    copy_to(zpack, zhalo, 4, 8, "gz", z_up).wait_send()
    pl.when(z_last)(zc.wait_send)
    drain(x2, not_high_x, not_low_x)
    drain(y2, not_high_y, not_low_y)

    total = recv_sum(phase)
    half = line < nz // 2
    flow_sum = jnp.sum(jnp.where(half, total, 0.0), axis=1, keepdims=True)
    void_sum = jnp.sum(jnp.where(half, 0.0, total), axis=1, keepdims=True)
    cells = float(nx * ny * nz * gx * gy * gz)
    step = (target[0] * cells - flow_sum) / (time_step * void_sum)
    lines[0] = jnp.broadcast_to(step, (1, nz)) + force
    lines[1] = jnp.broadcast_to(step, (1, nz))


def shift_kernel(ustar, div, slope, lines, vel_out, source_out, forcing_out, upward, source, sem):
    nx, ny, nz = div.shape
    half = nx // 2
    copies = [
        pltpu.make_async_copy(ustar.at[pl.ds(0, 2)], vel_out.at[pl.ds(0, 2)], sem.at[0]),
        pltpu.make_async_copy(lines.at[0], forcing_out, sem.at[1]),
    ]
    for copy in copies:
        copy.start()
    step = jnp.broadcast_to(lines[1], (ny, nz))
    for part in range(2):
        def body(i, carry):
            x = part * half + i
            upward[x] = ustar[2, x] + time_step * step
            source[x] = div[x] + step * slope[x]
            return carry

        lax.fori_loop(0, half, body, 0, unroll=8)
        planes = pl.ds(part * half, half)
        for copy in (
            pltpu.make_async_copy(upward.at[planes], vel_out.at[2, planes], sem.at[2 + 2 * part]),
            pltpu.make_async_copy(source.at[planes], source_out.at[planes], sem.at[3 + 2 * part]),
        ):
            copy.start()
            copies.append(copy)
    for copy in copies:
        copy.wait()


def local(velocity, pressure, voidage, particle_vel, forcing, target_flux):
    nx, ny, nz = voidage.shape
    sizes = tuple(lax.axis_size(a) for a in ("gx", "gy", "gz"))
    greet = (("gy", "gx"), ("gz",))
    if math.prod(sizes) <= DIRECT_LIMIT:
        phases = (("gz", "gy", "gx"),)
    else:
        phases = greet
    slot_count = sum(math.prod(lax.axis_size(a) for a in axes) for axes in phases)
    f32 = jnp.float32
    vmem = pl.BlockSpec(memory_space=pltpu.VMEM)
    smem = pl.BlockSpec(memory_space=pltpu.SMEM)
    hbm = pl.BlockSpec(memory_space=pltpu.HBM)
    dma = pltpu.SemaphoreType.DMA
    faces = [pltpu.VMEM((2, ny, nz), f32), pltpu.VMEM((2, ny, nz), f32)]
    face = [pltpu.VMEM((ny, nz), f32)]
    results = pl.pallas_call(
        functools.partial(kernel, sizes, greet, phases),
        out_shape=(
            pltpu.VMEM((3, nx, ny, nz), f32),
            pltpu.VMEM((nx, ny, nz), f32),
            pltpu.VMEM((nx, ny, nz), f32),
            pltpu.VMEM((2, 1, nz), f32),
        ),
        in_specs=[hbm] * 4 + [smem] * 2,
        out_specs=(vmem,) * 4,
        scratch_shapes=[
            pltpu.VMEM((4, nx + 2, ny, nz), f32),
            pltpu.VMEM((4, nx, ny, nz), f32),
            pltpu.VMEM((nx, ny, nz), f32),
            pltpu.VMEM((nx, ny, nz), f32),
            pltpu.VMEM((3, nx, ny, nz), f32),
        ] + face + [
            pltpu.VMEM((2, 4, nx, nz), f32),
            pltpu.VMEM((2, 4, nx, nz), f32),
        ] + faces + face + face + faces + [
            pltpu.VMEM((2, nx, nz), f32),
            pltpu.VMEM((2, nx, nz), f32),
            pltpu.VMEM((2, ny, nz), f32),
        ] + faces + [
            pltpu.VMEM((slot_count, 1, nz), f32),
            dma((2,)), dma((12,)), dma((17,)),
            dma((len(phases),)), dma((len(phases),)),
            pltpu.SemaphoreType.REGULAR,
        ],
        compiler_params=pltpu.CompilerParams(collective_id=0, has_side_effects=True),
    )(velocity, pressure, voidage, particle_vel, forcing, target_flux)
    vel_new, source, forcing_new = pl.pallas_call(
        shift_kernel,
        out_shape=(
            jax.ShapeDtypeStruct((3, nx, ny, nz), f32),
            jax.ShapeDtypeStruct((nx, ny, nz), f32),
            jax.ShapeDtypeStruct((1, nz), f32),
        ),
        in_specs=[vmem] * 4,
        out_specs=(hbm,) * 3,
        scratch_shapes=[
            pltpu.VMEM((nx, ny, nz), f32),
            pltpu.VMEM((nx, ny, nz), f32),
            dma((6,)),
        ],
    )(*(pltpu.with_memory_space_constraint(a, pltpu.VMEM) for a in results))
    return vel_new, source, forcing_new[0, :1]


def solution(mesh):
    return jax.shard_map(
        local,
        mesh=mesh,
        in_specs=(
            P(None, "gx", "gy", "gz"),
            P("gx", "gy", "gz"),
            P("gx", "gy", "gz"),
            P(None, "gx", "gy", "gz"),
            P(),
            P(),
        ),
        out_specs=(P(None, "gx", "gy", "gz"), P("gx", "gy", "gz"), P()),
        check_vma=False,
    )
```

```python
import functools
import math

import jax
import jax.numpy as jnp
from jax import lax
from jax.experimental import pallas as pl
from jax.experimental.pallas import tpu as pltpu
from jax.sharding import PartitionSpec as P

time_step = 0.2
viscosity = 0.1
drag_scale = 1.0
MESH = pl.DeviceIdType.MESH
DIRECT_LIMIT = 64


def ring_index(axes):
    index = 0
    for axis in axes:
        index = index * lax.axis_size(axis) + lax.axis_index(axis)
    return index


def ring_device(axes, index):
    device = {}
    for axis in reversed(axes):
        size = lax.axis_size(axis)
        device[axis] = lax.rem(index, size)
        index = lax.div(index, size)
    return device


def kernel(
    sizes, phases,
    vel_hbm, pres_hbm, void_hbm, part_hbm, forcing, target,
    ustar, div, slope, lines,
    blk, vp, inv, weight, flux, acc, edge, ypack, yhalo, zpack, zhalo, cpack, chalo,
    vzpack, vzhalo, fypack, fyhalo, fxhalo, fzpack, fzhalo, slots,
    load_sem, send, recv, sum_send, sum_recv, ready,
):
    gx, gy, gz = sizes
    nx, ny, nz = div.shape
    x_at, y_at, z_at = (lax.axis_index(a) for a in ("gx", "gy", "gz"))
    not_low_x, not_high_x = x_at > 0, x_at < gx - 1
    not_low_y, not_high_y = y_at > 0, y_at < gy - 1
    z_up, z_down = lax.rem(z_at + 1, gz), lax.rem(z_at + gz - 1, gz)
    z_first, z_last = z_at == 0, z_at == gz - 1
    not_first, not_last = z_at > 0, z_at < gz - 1

    inside = pl.ds(1, nx)
    for load in (
        pltpu.make_async_copy(vel_hbm, blk.at[pl.ds(1, 3), inside], load_sem.at[0]),
        pltpu.make_async_copy(pres_hbm, blk.at[0, inside], load_sem.at[0]),
        pltpu.make_async_copy(void_hbm, vp.at[0], load_sem.at[1]),
        pltpu.make_async_copy(part_hbm, vp.at[pl.ds(1, 3)], load_sem.at[1]),
    ):
        load.start()

    def signal(sem, device):
        pl.semaphore_signal(sem, inc=1, device_id=device, device_id_type=MESH)

    def members(which):
        axes = phases[which]
        count = math.prod(lax.axis_size(a) for a in axes)
        base = sum(math.prod(lax.axis_size(a) for a in phases[w]) for w in range(which))
        return axes, count, base, ring_index(axes)

    plane = gx * gy
    direct = len(phases) == 1
    if direct:
        near = ((1, gx, plane, plane * (gz - 1)),)
    else:
        near = ((1, gx), (1, gz - 1))
    barrier = pltpu.get_barrier_semaphore()
    pl.when(not_high_x)(lambda: signal(barrier, {"gx": x_at + 1}))
    pl.when(not_high_y)(lambda: signal(barrier, {"gy": y_at + 1}))
    pl.when(not_last)(lambda: signal(barrier, {"gz": z_at + 1}))
    pl.when(z_first)(lambda: signal(barrier, {"gz": gz - 1}))
    lower = sum(jnp.where(c, 1, 0) for c in (not_low_x, not_low_y, not_first, z_last))
    for which in range(len(phases)):
        axes, count, _, me = members(which)
        far = me < count - 1
        for d in near[which]:
            far = far & (me != count - 1 - d)
        pl.when(far)(lambda: signal(barrier, ring_device(axes, count - 1)))
        lower = lower + jnp.where(me == count - 1, count - 1 - len(near[which]), 0)

    lane = lax.broadcasted_iota(jnp.int32, (ny, nz), 1)
    row = lax.broadcasted_iota(jnp.int32, (ny, nz), 0)
    zero = jnp.zeros((ny, nz), jnp.float32)

    def pack_z(fields, read, at=0):
        low = high = zero
        for f in range(fields):
            for x in range(nx):
                turned = read(f, x)
                to = at + f * nx + x
                if to % nz:
                    turned = pltpu.roll(turned, to % nz, 1)
                low = jnp.where(lane == to, turned, low)
                high = jnp.where(lane == (to + nz - 1) % nz, turned, high)
        return low, high

    def copy_to(src, dst, send_at, recv_at, axis, device):
        return pltpu.make_async_remote_copy(
            src, dst, send.at[send_at], recv.at[recv_at],
            device_id={axis: device}, device_id_type=MESH)

    def exchange(low, high, dst_low, dst_high, sends, recvs, axis, up, down):
        return (copy_to(high, dst_low, sends[0], recvs[0], axis, up),
                copy_to(low, dst_high, sends[1], recvs[1], axis, down))

    def start(pair, high, low):
        pl.when(high)(pair[0].start)
        pl.when(low)(pair[1].start)

    def finish(pair, high, low):
        pl.when(low)(pair[0].wait_recv)
        pl.when(high)(pair[1].wait_recv)

    def drain(pair, high, low):
        pl.when(high)(pair[0].wait_send)
        pl.when(low)(pair[1].wait_send)

    up_x, down_x = jnp.minimum(x_at + 1, gx - 1), jnp.maximum(x_at - 1, 0)
    up_y, down_y = jnp.minimum(y_at + 1, gy - 1), jnp.maximum(y_at - 1, 0)
    rest = pl.ds(0, 3)

    def along_x(fields, recvs):
        return exchange(blk.at[fields, 1], blk.at[fields, nx], blk.at[fields, 0], blk.at[fields, nx + 1],
                        (0, 1), recvs, "gx", up_x, down_x)

    def along_y(fields, recvs):
        return exchange(ypack.at[0, fields], ypack.at[1, fields], yhalo.at[0, fields], yhalo.at[1, fields],
                        (2, 3), recvs, "gy", up_y, down_y)

    x1, x1_rest = along_x(3, (0, 1)), along_x(rest, (2, 3))
    y1, y1_rest = along_y(3, (4, 5)), along_y(rest, (6, 7))
    z1 = exchange(zpack.at[0], zpack.at[1], zhalo.at[0], zhalo.at[1], (4, 4), (8, 9), "gz", z_up, z_down)
    zv = exchange(vzpack.at[0], vzpack.at[1], vzhalo.at[0], vzhalo.at[1], (5, 5), (10, 10), "gz", z_up, z_down)
    zc = copy_to(cpack, chalo, 6, 11, "gz", z_up)

    pl.when(lower > 0)(lambda: pl.semaphore_wait(barrier, lower))
    pl.when(not_low_y)(lambda: signal(ready.at[1], {"gy": down_y}))
    pl.when(not_low_x)(lambda: signal(ready.at[0], {"gx": down_x}))
    pl.when(not_first)(lambda: signal(ready.at[2], {"gz": z_down}))
    pl.when(z_last)(lambda: signal(ready.at[3], {"gz": z_up}))
    for which in range(len(phases)):
        axes, count, _, me = members(which)

        @pl.when(me == count - 1)
        def _():
            for k in range(count - 1):
                signal(ready.at[4 + which], ring_device(axes, k))
    pltpu.make_async_copy(blk.at[:, inside], blk.at[:, inside], load_sem.at[0]).wait()
    for side, y in ((0, 0), (1, ny - 1)):
        ypack[side, 3] = blk[3, inside, y, :]
    pl.when(not_low_y)(y1[1].start)
    pl.when(not_low_x)(x1[1].start)
    low, high = pack_z(4, lambda f, x: blk[f, x + 1])
    zpack[0] = low
    zpack[1] = high
    pl.when(not_first)(z1[1].start)
    pl.when(z_last)(z1[0].start)
    pltpu.make_async_copy(vp, vp, load_sem.at[1]).wait()
    force = forcing[0]

    def drag_body(x, total):
        v = vp[0, x]
        c = [blk[1 + k, x + 1] for k in range(3)]
        q = [vp[1 + k, x] for k in range(3)]
        slip = jnp.sqrt(sum((c[k] - q[k]) ** 2 for k in range(3)))
        drag = drag_scale * (1.0 - v) * jnp.exp(-2.65 * jnp.log(v)) * (1.0 + slip)
        step_drag = time_step * drag
        inverse = 1.0 / (1.0 + step_drag)
        inv[x] = inverse
        weight[x] = v * inverse
        for k in range(3):
            ustar[k, x] = c[k] + step_drag * q[k]
        return total + v

    void_total = lax.fori_loop(0, nx, drag_body, zero, unroll=4)

    w_low, w_high = pack_z(1, lambda f, x: weight[x], 3 * nx)

    def coefficients(face, w, sign, at):
        upward = w * (time_step * viscosity + (sign * 0.5 * time_step) * face)
        pressed = (sign * 0.5 * time_step) * pltpu.roll(w, nz - 3 * nx, 1)
        return jnp.where(at < nx, pressed,
                         jnp.where((at >= 3 * nx) & (at < 4 * nx), upward, 0.0))

    c_low = pltpu.roll(coefficients(zpack[0], w_low, 1.0, lane), nz - 1, 1)
    c_high = pltpu.roll(coefficients(zpack[1], w_high, -1.0, lax.rem(lane + 1, nz)), 1, 1)
    cpack[...] = c_high

    pl.when(z_last)(zc.start)
    for higher, which, copy in ((not_high_x, 0, x1[0]), (not_high_y, 1, y1[0]), (not_last, 2, z1[0])):
        @pl.when(higher)
        def _():
            pl.semaphore_wait(ready.at[which], 1)
            copy.start()
    for f in range(3):
        ypack[0, f] = blk[f, inside, 0, :]
        ypack[1, f] = blk[f, inside, ny - 1, :]
    def wall_x(within, halo_plane, edge_plane):
        @pl.when(jnp.logical_not(within))
        def _():
            for f in range(1, 4):
                blk[f, halo_plane] = zero
            blk[0, halo_plane] = blk[0, edge_plane]

    wall_x(not_low_x, 0, 1)
    wall_x(not_high_x, nx + 1, nx)

    def wall_y(within, side):
        @pl.when(jnp.logical_not(within))
        def _():
            for f in range(1, 4):
                yhalo[side, f] = jnp.zeros((nx, nz), jnp.float32)
            yhalo[side, 0] = ypack[side, 0]

    wall_y(not_low_y, 0)
    wall_y(not_high_y, 1)

    def stencil(x, k):
        p = x + 1
        centre = [blk[1 + f, p] for f in range(3)]

        def pair(f, axis_no):
            if axis_no == 0:
                return blk[f, p - 1], blk[f, p + 1]
            field = blk[f, p]
            if axis_no == 1:
                return (jnp.where(row == 0, 0.0, pltpu.roll(field, 1, 0)),
                        jnp.where(row == ny - 1, 0.0, pltpu.roll(field, ny - 1, 0)))
            return (jnp.where(lane == 0, 0.0, pltpu.roll(field, 1, 1)),
                    jnp.where(lane == nz - 1, 0.0, pltpu.roll(field, nz - 1, 1)))

        advect = total = None
        for axis_no in range(3):
            low, high = pair(1 + k, axis_no)
            term = centre[axis_no] * (high - low)
            both = high + low
            advect = term if advect is None else advect + term
            total = both if total is None else total + both
        low, high = pair(0, k)
        forces = (viscosity * (total - 6.0 * centre[k])
                  - 0.5 * (advect + (high - low)))
        if k == 2:
            forces = forces + force
        value = ustar[k, x] + time_step * forces
        ustar[k, x] = value * inv[x]
        return value

    def upward_body(i, flow):
        for x in (1 + 2 * i, 2 + 2 * i):
            flow = flow + weight[x] * stencil(x, 2)
        return flow

    flow = lax.fori_loop(0, (nx - 2) // 2, upward_body, zero, unroll=3)

    start(y1_rest, not_high_y, not_low_y)
    start(x1_rest, not_high_x, not_low_x)

    low, high = pack_z(1, lambda f, x: vp[0, x])
    vzpack[0] = low
    vzpack[1] = high
    zv[0].start()
    pl.when(not_first)(zv[1].start)

    def along_y_coefficients(side, sign):
        w = weight[:, 0 if side == 0 else ny - 1, :]
        return w * (time_step * viscosity + (sign * 0.5 * time_step) * ypack[side, 2])

    cy_low, cy_high = along_y_coefficients(0, 1.0), along_y_coefficients(1, -1.0)

    def fold(value):
        value = jnp.sum(value, axis=0, keepdims=True)
        return value + pltpu.roll(value, nz // 2, 1)

    line = lax.broadcasted_iota(jnp.int32, (1, nz), 1)
    void_line = fold(void_total)

    def across_body(i, carry):
        for x in (1 + 2 * i, 2 + 2 * i):
            stencil(x, 0)
            stencil(x, 1)
        return carry

    lax.fori_loop(0, (nx - 2) // 2, across_body, 0, unroll=3)
    @pl.when(z_first)
    def _():
        pl.semaphore_wait(ready.at[3], 1)
        z1[1].start()
        zv[1].start()

    def sum_copy(which, src, dst, device):
        return pltpu.make_async_remote_copy(
            src, dst, sum_send.at[which], sum_recv.at[which], device_id=device, device_id_type=MESH)

    def all_in(which):
        _, count, _, me = members(which)

        @pl.when(me < count - 1)
        def _():
            pl.semaphore_wait(ready.at[4 + which], 1)

    def send_sum(which, value):
        axes, count, base, me = members(which)
        mine = slots.at[base + me]
        slots[base + me] = value
        for k in range(count - 1):
            other = jnp.where(k < me, k, k + 1)
            sum_copy(which, mine, mine, ring_device(axes, other)).start()

    def all_sums(which):
        axes, count, base, me = members(which)
        others = slots.at[pl.ds(base, count - 1)]
        return sum_copy(which, others, others, ring_device(axes, lax.rem(me + 1, count)))

    def recv_sum(which):
        axes, count, base, me = members(which)
        all_sums(which).wait_recv()
        return jnp.sum(slots[pl.ds(base, count)], axis=0)

    finish(x1, not_high_x, not_low_x)
    flow = flow + weight[0] * stencil(0, 2) + weight[nx - 1] * stencil(nx - 1, 2)
    acc[...] = flow
    finish(y1, not_high_y, not_low_y)
    y_line = jnp.sum(cy_low * yhalo[0, 3] + cy_high * yhalo[1, 3], axis=0, keepdims=True)
    z1[0].wait_recv()
    acc[...] += c_low * zhalo[0]

    @pl.when(jnp.logical_not(z_last))
    def _():
        z1[1].wait_recv()
        acc[...] += c_high * zhalo[1]

    def sum_up():
        flow_line = jnp.sum(acc[...], axis=0, keepdims=True) + y_line
        flow_line = flow_line + pltpu.roll(flow_line, nz // 2, 1)
        send_sum(0, jnp.where(line < nz // 2, flow_line, void_line))

    for which in range(len(phases)):
        all_in(which)
    pl.when(jnp.logical_not(z_first))(sum_up)

    first_row = row == 0
    last_row = row == ny - 1
    first_lane = lane == 0
    last_lane = lane == nz - 1
    row_sign = jnp.where(first_row, 1.0, jnp.where(last_row, -1.0, 0.0))
    lane_sign = jnp.where(first_lane, 1.0, jnp.where(last_lane, -1.0, 0.0))
    row_sign, lane_sign = (s * (0.5 * time_step) for s in (row_sign, lane_sign))
    row_visc, lane_visc = (jnp.abs(s) * (2.0 * viscosity) for s in (row_sign, lane_sign))

    def interleave(low, high):
        even = lax.rem(lane, 2) == 0
        return jnp.where(even, low, high), jnp.where(even, high, low)

    def unpack(which, at):
        return pltpu.roll(which, lax.rem(2 * nz - at, nz), 1)

    def rows(f, x):
        return jnp.where(
            row < ny // 2,
            jnp.broadcast_to(yhalo[0, f, pl.ds(x, 1), :], (ny, nz)),
            jnp.broadcast_to(yhalo[1, f, pl.ds(x, 1), :], (ny, nz)))

    def correct(x, which, components, with_rows=True):
        by_row = row_visc + row_sign * blk[2, x + 1]
        by_lane = lane_visc + lane_sign * blk[3, x + 1]
        inverse, v = inv[x], vp[0, x]
        for k in components:
            value = by_lane * unpack(which, (1 + k) * nx + x)
            if with_rows:
                value = value + by_row * rows(1 + k, x)
            if k == 1:
                value = value + row_sign * rows(0, x)
            if k == 2:
                value = value + lane_sign * unpack(which, x)
            value = ustar[k, x] + value * inverse
            ustar[k, x] = value
            flux[k, x] = v * value

    def correct_all(pair, components, with_rows=True):
        def body(i, carry):
            correct(2 * i, pair[0], components, with_rows)
            correct(2 * i + 1, pair[1], components, with_rows)
            return carry

        lax.fori_loop(0, nx // 2, body, 0, unroll=4)

    x2 = exchange(flux.at[0, 0], flux.at[0, nx - 1], fxhalo.at[0], fxhalo.at[1], (7, 8), (12, 13), "gx", up_x, down_x)
    y2 = exchange(fypack.at[0], fypack.at[1], fyhalo.at[0], fyhalo.at[1], (9, 10), (14, 15), "gy", up_y, down_y)
    z2 = exchange(fzpack.at[0], fzpack.at[1], fzhalo.at[0], fzhalo.at[1], (11, 11), (16, 16), "gz", z_up, z_down)

    def send_flux_z():
        low, high = pack_z(1, lambda f, x: flux[2, x])
        fzpack[0] = low
        fzpack[1] = high
        for copy in z2:
            copy.start()

    z_low = pltpu.roll(zhalo[0], 1, 1)
    @pl.when(z_last)
    def _():
        correct_all(interleave(z_low, zero), (2,))
        send_flux_z()

    pl.when(z_last)(z1[1].wait_recv)
    z_high = pltpu.roll(zhalo[1], nz - 1, 1)
    joined = interleave(z_low, z_high)
    finish(x1_rest, not_high_x, not_low_x)
    for x in (0, nx - 1):
        stencil(x, 0)
        stencil(x, 1)
    finish(y1_rest, not_high_y, not_low_y)
    correct_all(joined, (0, 1))
    start(x2, not_high_x, not_low_x)
    fypack[0] = flux[1, :, 0, :]
    fypack[1] = flux[1, :, ny - 1, :]
    start(y2, not_high_y, not_low_y)

    @pl.when(z_first)
    def _():
        zc.wait_recv()
        product = chalo[...] * zpack[0]
        acc[...] += product
        sum_up()
        product = product + pltpu.roll(product, nz - 3 * nx, 1)
        edge[...] = jnp.where(lane < nx, product, 0.0)

    @pl.when(not_first)
    def _():
        edge[...] = zero

    @pl.when(z_last)
    def _():
        correct_all(interleave(zero, z_high), (2,), False)

    @pl.when(not_last)
    def _():
        correct_all(joined, (2,))
        send_flux_z()

    for within, side in ((not_low_x, 0), (not_high_x, 1)):
        @pl.when(jnp.logical_not(within))
        def _():
            fxhalo[side] = zero
    for within, side in ((not_low_y, 0), (not_high_y, 1)):
        @pl.when(jnp.logical_not(within))
        def _():
            fyhalo[side] = jnp.zeros((nx, nz), jnp.float32)

    copy_to(vzpack, vzhalo, 5, 10, "gz", z_up).wait()
    v_joined = interleave(pltpu.roll(vzhalo[0], 1, 1), pltpu.roll(vzhalo[1], nz - 1, 1))

    def source_plane(x, odd, x_low, x_high):
        fy, fz, v = flux[1, x], flux[2, x], vp[0, x]
        y_low = jnp.where(first_row, 0.0, pltpu.roll(fy, 1, 0))
        y_high = jnp.where(last_row, 0.0, pltpu.roll(fy, ny - 1, 0))
        z_low = jnp.where(first_lane, 0.0, pltpu.roll(fz, 1, 1))
        z_high = jnp.where(last_lane, 0.0, pltpu.roll(fz, nz - 1, 1))
        v_halo = unpack(v_joined[odd], x)
        v_low = jnp.where(first_lane, v_halo, pltpu.roll(v, 1, 1))
        v_high = jnp.where(last_lane, v_halo, pltpu.roll(v, nz - 1, 1))
        div[x] = 0.5 * ((x_high - x_low) + (y_high - y_low) + (z_high - z_low))
        slope[x] = (0.5 * time_step) * (v_high - v_low)

    def source_body(i, carry):
        x = 2 * i + 1
        source_plane(x, 1, flux[0, x - 1], flux[0, x + 1])
        source_plane(x + 1, 0, flux[0, x], flux[0, x + 2])
        return carry

    lax.fori_loop(0, nx // 2 - 1, source_body, 0, unroll=3)
    phase = 0
    while phase < len(phases) - 1:
        total = recv_sum(phase)
        phase += 1
        send_sum(phase, total)
    finish(x2, not_high_x, not_low_x)
    source_plane(0, 0, fxhalo[0], flux[0, 1])
    source_plane(nx - 1, 1, flux[0, nx - 2], fxhalo[1])
    finish(y2, not_high_y, not_low_y)
    copy_to(fzpack, fzhalo, 11, 16, "gz", z_up).wait()
    f_joined = interleave(pltpu.roll(fzhalo[0], 1, 1) + edge[...], pltpu.roll(fzhalo[1], nz - 1, 1))
    row_half, lane_half = row_sign / time_step, lane_sign / time_step

    def edge_plane(x, odd):
        y_halo = jnp.where(
            row < ny // 2,
            jnp.broadcast_to(fyhalo[0, pl.ds(x, 1), :], (ny, nz)),
            jnp.broadcast_to(fyhalo[1, pl.ds(x, 1), :], (ny, nz)))
        div[x] = div[x] - row_half * y_halo - lane_half * unpack(f_joined[odd], x)

    def edge_body(i, carry):
        edge_plane(2 * i, 0)
        edge_plane(2 * i + 1, 1)
        return carry

    lax.fori_loop(0, nx // 2, edge_body, 0, unroll=16)

    for which in range(len(phases)):
        all_sums(which).wait_send()
    drain(along_x(slice(None), (0, 1)), not_high_x, not_low_x)
    drain(along_y(slice(None), (4, 5)), not_high_y, not_low_y)
    copy_to(zpack, zhalo, 4, 8, "gz", z_up).wait_send()
    pl.when(z_last)(zc.wait_send)
    drain(x2, not_high_x, not_low_x)
    drain(y2, not_high_y, not_low_y)

    total = recv_sum(phase)
    half = line < nz // 2
    flow_sum = jnp.sum(jnp.where(half, total, 0.0), axis=1, keepdims=True)
    void_sum = jnp.sum(jnp.where(half, 0.0, total), axis=1, keepdims=True)
    cells = float(nx * ny * nz * gx * gy * gz)
    step = (target[0] * cells - flow_sum) / (time_step * void_sum)
    lines[0] = jnp.broadcast_to(step, (1, nz)) + force
    lines[1] = jnp.broadcast_to(step, (1, nz))


def shift_kernel(ustar, div, slope, lines, vel_out, source_out, forcing_out, upward, source, sem):
    nx, ny, nz = div.shape
    half = nx // 2
    copies = [
        pltpu.make_async_copy(ustar.at[pl.ds(0, 2)], vel_out.at[pl.ds(0, 2)], sem.at[0]),
        pltpu.make_async_copy(lines.at[0], forcing_out, sem.at[1]),
    ]
    for copy in copies:
        copy.start()
    step = jnp.broadcast_to(lines[1], (ny, nz))
    for part in range(2):
        def body(i, carry):
            x = part * half + i
            upward[x] = ustar[2, x] + time_step * step
            source[x] = div[x] + step * slope[x]
            return carry

        lax.fori_loop(0, half, body, 0, unroll=8)
        planes = pl.ds(part * half, half)
        for copy in (
            pltpu.make_async_copy(upward.at[planes], vel_out.at[2, planes], sem.at[2 + 2 * part]),
            pltpu.make_async_copy(source.at[planes], source_out.at[planes], sem.at[3 + 2 * part]),
        ):
            copy.start()
            copies.append(copy)
    for copy in copies:
        copy.wait()


def local(velocity, pressure, voidage, particle_vel, forcing, target_flux):
    nx, ny, nz = voidage.shape
    sizes = tuple(lax.axis_size(a) for a in ("gx", "gy", "gz"))
    if math.prod(sizes) <= DIRECT_LIMIT:
        phases = (("gz", "gy", "gx"),)
    else:
        phases = (("gy", "gx"), ("gz",))
    slot_count = sum(math.prod(lax.axis_size(a) for a in axes) for axes in phases)
    f32 = jnp.float32
    vmem = pl.BlockSpec(memory_space=pltpu.VMEM)
    smem = pl.BlockSpec(memory_space=pltpu.SMEM)
    hbm = pl.BlockSpec(memory_space=pltpu.HBM)
    dma = pltpu.SemaphoreType.DMA
    faces = [pltpu.VMEM((2, ny, nz), f32), pltpu.VMEM((2, ny, nz), f32)]
    face = [pltpu.VMEM((ny, nz), f32)]
    results = pl.pallas_call(
        functools.partial(kernel, sizes, phases),
        out_shape=(
            pltpu.VMEM((3, nx, ny, nz), f32),
            pltpu.VMEM((nx, ny, nz), f32),
            pltpu.VMEM((nx, ny, nz), f32),
            pltpu.VMEM((2, 1, nz), f32),
        ),
        in_specs=[hbm] * 4 + [smem] * 2,
        out_specs=(vmem,) * 4,
        scratch_shapes=[
            pltpu.VMEM((4, nx + 2, ny, nz), f32),
            pltpu.VMEM((4, nx, ny, nz), f32),
            pltpu.VMEM((nx, ny, nz), f32),
            pltpu.VMEM((nx, ny, nz), f32),
            pltpu.VMEM((3, nx, ny, nz), f32),
        ] + face + face + [
            pltpu.VMEM((2, 4, nx, nz), f32),
            pltpu.VMEM((2, 4, nx, nz), f32),
        ] + faces + face + face + faces + [
            pltpu.VMEM((2, nx, nz), f32),
            pltpu.VMEM((2, nx, nz), f32),
            pltpu.VMEM((2, ny, nz), f32),
        ] + faces + [
            pltpu.VMEM((slot_count, 1, nz), f32),
            dma((2,)), dma((12,)), dma((17,)),
            dma((len(phases),)), dma((len(phases),)),
            pltpu.SemaphoreType.REGULAR((4 + len(phases),)),
        ],
        compiler_params=pltpu.CompilerParams(collective_id=0, has_side_effects=True),
    )(velocity, pressure, voidage, particle_vel, forcing, target_flux)
    vel_new, source, forcing_new = pl.pallas_call(
        shift_kernel,
        out_shape=(
            jax.ShapeDtypeStruct((3, nx, ny, nz), f32),
            jax.ShapeDtypeStruct((nx, ny, nz), f32),
            jax.ShapeDtypeStruct((1, nz), f32),
        ),
        in_specs=[vmem] * 4,
        out_specs=(hbm,) * 3,
        scratch_shapes=[
            pltpu.VMEM((nx, ny, nz), f32),
            pltpu.VMEM((nx, ny, nz), f32),
            dma((6,)),
        ],
    )(*(pltpu.with_memory_space_constraint(a, pltpu.VMEM) for a in results))
    return vel_new, source, forcing_new[0, :1]


def solution(mesh):
    return jax.shard_map(
        local,
        mesh=mesh,
        in_specs=(
            P(None, "gx", "gy", "gz"),
            P("gx", "gy", "gz"),
            P("gx", "gy", "gz"),
            P(None, "gx", "gy", "gz"),
            P(),
            P(),
        ),
        out_specs=(P(None, "gx", "gy", "gz"), P("gx", "gy", "gz"), P()),
        check_vma=False,
    )
```

```python
import functools
import math

import jax
import jax.numpy as jnp
from jax import lax
from jax.experimental import pallas as pl
from jax.experimental.pallas import tpu as pltpu
from jax.sharding import PartitionSpec as P

time_step = 0.2
viscosity = 0.1
drag_scale = 1.0
MESH = pl.DeviceIdType.MESH
DIRECT_LIMIT = 64


def ring_index(axes):
    index = 0
    for axis in axes:
        index = index * lax.axis_size(axis) + lax.axis_index(axis)
    return index


def ring_device(axes, index):
    device = {}
    for axis in reversed(axes):
        size = lax.axis_size(axis)
        device[axis] = lax.rem(index, size)
        index = lax.div(index, size)
    return device


def kernel(
    sizes, phases,
    vel_hbm, pres_hbm, void_hbm, part_hbm, forcing, target,
    ustar, div, slope, lines,
    blk, vp, inv, weight, flux, acc, edge, ypack, yhalo, zpack, zhalo, cpack, chalo,
    vzpack, vzhalo, fyhalo, fxhalo, fzpack, fzhalo, slots,
    load_sem, send, recv, sum_send, sum_recv, ready,
):
    gx, gy, gz = sizes
    nx, ny, nz = div.shape
    x_at, y_at, z_at = (lax.axis_index(a) for a in ("gx", "gy", "gz"))
    not_low_x, not_high_x = x_at > 0, x_at < gx - 1
    not_low_y, not_high_y = y_at > 0, y_at < gy - 1
    z_up, z_down = lax.rem(z_at + 1, gz), lax.rem(z_at + gz - 1, gz)
    z_first, z_last = z_at == 0, z_at == gz - 1
    not_first, not_last = z_at > 0, z_at < gz - 1

    def signal(sem, device):
        pl.semaphore_signal(sem, inc=1, device_id=device, device_id_type=MESH)

    def members(which):
        axes = phases[which]
        count = math.prod(lax.axis_size(a) for a in axes)
        base = sum(math.prod(lax.axis_size(a) for a in phases[w]) for w in range(which))
        return axes, count, base, ring_index(axes)

    plane = gx * gy
    direct = len(phases) == 1
    if direct:
        near = ((1, gx, plane, plane * (gz - 1)),)
    else:
        near = ((1, gx), (1, gz - 1))
    barrier = pltpu.get_barrier_semaphore()
    pl.when(not_high_x)(lambda: signal(barrier, {"gx": x_at + 1}))
    pl.when(not_high_y)(lambda: signal(barrier, {"gy": y_at + 1}))
    pl.when(not_last)(lambda: signal(barrier, {"gz": z_at + 1}))
    pl.when(z_first)(lambda: signal(barrier, {"gz": gz - 1}))
    lower = sum(jnp.where(c, 1, 0) for c in (not_low_x, not_low_y, not_first, z_last))
    for which in range(len(phases)):
        axes, count, _, me = members(which)
        far = me < count - 1
        for d in near[which]:
            far = far & (me != count - 1 - d)
        pl.when(far)(lambda: signal(barrier, ring_device(axes, count - 1)))
        lower = lower + jnp.where(me == count - 1, count - 1 - len(near[which]), 0)

    inside = pl.ds(1, nx)
    for load in (
        pltpu.make_async_copy(vel_hbm, blk.at[pl.ds(1, 3), inside], load_sem.at[0]),
        pltpu.make_async_copy(pres_hbm, blk.at[0, inside], load_sem.at[0]),
        pltpu.make_async_copy(void_hbm, vp.at[0], load_sem.at[1]),
        pltpu.make_async_copy(part_hbm, vp.at[pl.ds(1, 3)], load_sem.at[1]),
    ):
        load.start()

    lane = lax.broadcasted_iota(jnp.int32, (ny, nz), 1)
    row = lax.broadcasted_iota(jnp.int32, (ny, nz), 0)
    zero = jnp.zeros((ny, nz), jnp.float32)

    def pack_z(fields, read, at=0):
        low = high = zero
        for f in range(fields):
            for x in range(nx):
                turned = read(f, x)
                to = at + f * nx + x
                if to % nz:
                    turned = pltpu.roll(turned, to % nz, 1)
                low = jnp.where(lane == to, turned, low)
                high = jnp.where(lane == (to + nz - 1) % nz, turned, high)
        return low, high

    def copy_to(src, dst, send_at, recv_at, axis, device):
        return pltpu.make_async_remote_copy(
            src, dst, send.at[send_at], recv.at[recv_at],
            device_id={axis: device}, device_id_type=MESH)

    def exchange(low, high, dst_low, dst_high, send_at, recvs, axis, up, down):
        return (copy_to(high, dst_low, send_at, recvs[0], axis, up),
                copy_to(low, dst_high, send_at, recvs[-1], axis, down))

    def start(pair, high, low):
        pl.when(high)(pair[0].start)
        pl.when(low)(pair[1].start)

    def settle(both, one, send_at, recv_at, high, low, received):
        def wait(ref):
            copy = copy_to(ref, ref, send_at, recv_at, "gz", z_up)
            return copy.wait_recv if received else copy.wait_send

        pl.when(high & low)(wait(both))
        pl.when(high ^ low)(wait(one))

    def finish_x(both, one, recv_at):
        settle(both, one, 0, recv_at, not_high_x, not_low_x, True)

    def finish_y(both, one, recv_at):
        settle(both, one, 1, recv_at, not_high_y, not_low_y, True)

    up_x, down_x = jnp.minimum(x_at + 1, gx - 1), jnp.maximum(x_at - 1, 0)
    up_y, down_y = jnp.minimum(y_at + 1, gy - 1), jnp.maximum(y_at - 1, 0)
    rest = pl.ds(0, 3)

    def along_x(fields, recvs):
        return exchange(blk.at[fields, 1], blk.at[fields, nx], blk.at[fields, 0], blk.at[fields, nx + 1],
                        0, recvs, "gx", up_x, down_x)

    def along_y(fields, recvs):
        return exchange(ypack.at[0, fields], ypack.at[1, fields], yhalo.at[0, fields], yhalo.at[1, fields],
                        1, recvs, "gy", up_y, down_y)

    x1, x1_rest = along_x(3, (0,)), along_x(rest, (1,))
    y1, y1_rest = along_y(3, (2,)), along_y(rest, (3,))
    z1 = exchange(zpack.at[0], zpack.at[1], zhalo.at[0], zhalo.at[1], 2, (4, 5), "gz", z_up, z_down)
    zv = exchange(vzpack.at[0], vzpack.at[1], vzhalo.at[0], vzhalo.at[1], 2, (6,), "gz", z_up, z_down)
    zc = copy_to(cpack, chalo, 3, 7, "gz", z_up)

    pl.when(lower > 0)(lambda: pl.semaphore_wait(barrier, lower))
    pl.when(not_low_y)(lambda: signal(ready.at[1], {"gy": down_y}))
    pl.when(not_low_x)(lambda: signal(ready.at[0], {"gx": down_x}))
    pl.when(not_first)(lambda: signal(ready.at[2], {"gz": z_down}))
    pl.when(z_last)(lambda: signal(ready.at[3], {"gz": z_up}))
    for which in range(len(phases)):
        axes, count, _, me = members(which)

        @pl.when(me == count - 1)
        def _():
            for k in range(count - 1):
                signal(ready.at[4 + which], ring_device(axes, k))
    pltpu.make_async_copy(blk.at[:, inside], blk.at[:, inside], load_sem.at[0]).wait()
    for side, y in ((0, 0), (1, ny - 1)):
        ypack[side, 3] = blk[3, inside, y, :]
    pl.when(not_low_y)(y1[1].start)
    pl.when(not_low_x)(x1[1].start)
    low, high = pack_z(4, lambda f, x: blk[f, x + 1])
    zpack[0] = low
    zpack[1] = high
    pl.when(not_first)(z1[1].start)
    pl.when(z_last)(z1[0].start)
    pltpu.make_async_copy(vp, vp, load_sem.at[1]).wait()
    force = forcing[0]

    def drag_body(x, total):
        v = vp[0, x]
        c = [blk[1 + k, x + 1] for k in range(3)]
        q = [vp[1 + k, x] for k in range(3)]
        slip = jnp.sqrt(sum((c[k] - q[k]) ** 2 for k in range(3)))
        drag = drag_scale * (1.0 - v) * jnp.exp(-2.65 * jnp.log(v)) * (1.0 + slip)
        step_drag = time_step * drag
        inverse = 1.0 / (1.0 + step_drag)
        inv[x] = inverse
        weight[x] = v * inverse
        for k in range(3):
            ustar[k, x] = c[k] + step_drag * q[k]
        return total + v

    void_total = lax.fori_loop(0, nx, drag_body, zero, unroll=4)

    for higher, which, copy in ((not_high_x, 0, x1[0]), (not_high_y, 1, y1[0]), (not_last, 2, z1[0])):
        @pl.when(higher)
        def _():
            pl.semaphore_wait(ready.at[which], 1)
            copy.start()
    w_low, w_high = pack_z(1, lambda f, x: weight[x], 3 * nx)

    def coefficients(face, w, sign, at):
        upward = w * (time_step * viscosity + (sign * 0.5 * time_step) * face)
        pressed = (sign * 0.5 * time_step) * pltpu.roll(w, nz - 3 * nx, 1)
        return jnp.where(at < nx, pressed,
                         jnp.where((at >= 3 * nx) & (at < 4 * nx), upward, 0.0))

    c_low = pltpu.roll(coefficients(zpack[0], w_low, 1.0, lane), nz - 1, 1)
    c_high = pltpu.roll(coefficients(zpack[1], w_high, -1.0, lax.rem(lane + 1, nz)), 1, 1)
    cpack[...] = c_high

    pl.when(z_last)(zc.start)
    for f in range(3):
        ypack[0, f] = blk[f, inside, 0, :]
        ypack[1, f] = blk[f, inside, ny - 1, :]
    def wall_x(within, halo_plane, edge_plane):
        @pl.when(jnp.logical_not(within))
        def _():
            for f in range(1, 4):
                blk[f, halo_plane] = zero
            blk[0, halo_plane] = blk[0, edge_plane]

    wall_x(not_low_x, 0, 1)
    wall_x(not_high_x, nx + 1, nx)

    def wall_y(within, side):
        @pl.when(jnp.logical_not(within))
        def _():
            for f in range(1, 4):
                yhalo[side, f] = jnp.zeros((nx, nz), jnp.float32)
            yhalo[side, 0] = ypack[side, 0]

    wall_y(not_low_y, 0)
    wall_y(not_high_y, 1)

    def stencil(x, k):
        p = x + 1
        centre = [blk[1 + f, p] for f in range(3)]

        def pair(f, axis_no):
            if axis_no == 0:
                return blk[f, p - 1], blk[f, p + 1]
            field = blk[f, p]
            if axis_no == 1:
                return (jnp.where(row == 0, 0.0, pltpu.roll(field, 1, 0)),
                        jnp.where(row == ny - 1, 0.0, pltpu.roll(field, ny - 1, 0)))
            return (jnp.where(lane == 0, 0.0, pltpu.roll(field, 1, 1)),
                    jnp.where(lane == nz - 1, 0.0, pltpu.roll(field, nz - 1, 1)))

        advect = total = None
        for axis_no in range(3):
            low, high = pair(1 + k, axis_no)
            term = centre[axis_no] * (high - low)
            both = high + low
            advect = term if advect is None else advect + term
            total = both if total is None else total + both
        low, high = pair(0, k)
        forces = (viscosity * (total - 6.0 * centre[k])
                  - 0.5 * (advect + (high - low)))
        if k == 2:
            forces = forces + force
        value = ustar[k, x] + time_step * forces
        ustar[k, x] = value * inv[x]
        return value

    def upward_body(i, flow):
        for x in (1 + 2 * i, 2 + 2 * i):
            flow = flow + weight[x] * stencil(x, 2)
        return flow

    flow = lax.fori_loop(0, (nx - 2) // 2, upward_body, zero, unroll=3)

    start(y1_rest, not_high_y, not_low_y)
    start(x1_rest, not_high_x, not_low_x)

    low, high = pack_z(1, lambda f, x: vp[0, x])
    vzpack[0] = low
    vzpack[1] = high
    zv[0].start()
    pl.when(not_first)(zv[1].start)

    def along_y_coefficients(side, sign):
        w = weight[:, 0 if side == 0 else ny - 1, :]
        return w * (time_step * viscosity + (sign * 0.5 * time_step) * ypack[side, 2])

    cy_low, cy_high = along_y_coefficients(0, 1.0), along_y_coefficients(1, -1.0)

    def fold(value):
        value = jnp.sum(value, axis=0, keepdims=True)
        return value + pltpu.roll(value, nz // 2, 1)

    line = lax.broadcasted_iota(jnp.int32, (1, nz), 1)
    void_line = fold(void_total)

    def across_body(i, carry):
        for x in (1 + 2 * i, 2 + 2 * i):
            stencil(x, 0)
            stencil(x, 1)
        return carry

    lax.fori_loop(0, (nx - 2) // 2, across_body, 0, unroll=3)
    @pl.when(z_first)
    def _():
        pl.semaphore_wait(ready.at[3], 1)
        z1[1].start()
        zv[1].start()

    def sum_copy(which, src, dst, device):
        return pltpu.make_async_remote_copy(
            src, dst, sum_send.at[which], sum_recv.at[which], device_id=device, device_id_type=MESH)

    def all_in(which):
        _, count, _, me = members(which)

        @pl.when(me < count - 1)
        def _():
            pl.semaphore_wait(ready.at[4 + which], 1)

    def send_sum(which, value):
        axes, count, base, me = members(which)
        mine = slots.at[base + me]
        slots[base + me] = value
        for k in range(count - 1):
            other = jnp.where(k < me, k, k + 1)
            sum_copy(which, mine, mine, ring_device(axes, other)).start()

    def all_sums(which):
        axes, count, base, me = members(which)
        others = slots.at[pl.ds(base, count - 1)]
        return sum_copy(which, others, others, ring_device(axes, lax.rem(me + 1, count)))

    def recv_sum(which):
        axes, count, base, me = members(which)
        all_sums(which).wait_recv()
        return jnp.sum(slots[pl.ds(base, count)], axis=0)

    finish_x(blk.at[3, pl.ds(0, 2)], blk.at[3, 0], 0)
    flow = flow + weight[0] * stencil(0, 2) + weight[nx - 1] * stencil(nx - 1, 2)
    acc[...] = flow
    finish_y(yhalo.at[:, 3], yhalo.at[0, 3], 2)
    y_line = jnp.sum(cy_low * yhalo[0, 3] + cy_high * yhalo[1, 3], axis=0, keepdims=True)
    def across_edges():
        finish_x(blk.at[rest, pl.ds(0, 2)], blk.at[rest, 0], 1)
        for x in (0, nx - 1):
            stencil(x, 0)
            stencil(x, 1)

    pl.when(z_first)(across_edges)
    z1[0].wait_recv()
    acc[...] += c_low * zhalo[0]

    @pl.when(jnp.logical_not(z_last))
    def _():
        z1[1].wait_recv()
        acc[...] += c_high * zhalo[1]

    def sum_up():
        flow_line = jnp.sum(acc[...], axis=0, keepdims=True) + y_line
        flow_line = flow_line + pltpu.roll(flow_line, nz // 2, 1)
        send_sum(0, jnp.where(line < nz // 2, flow_line, void_line))

    for which in range(len(phases)):
        all_in(which)
    pl.when(jnp.logical_not(z_first))(sum_up)

    first_row = row == 0
    last_row = row == ny - 1
    first_lane = lane == 0
    last_lane = lane == nz - 1
    row_sign = jnp.where(first_row, 1.0, jnp.where(last_row, -1.0, 0.0))
    lane_sign = jnp.where(first_lane, 1.0, jnp.where(last_lane, -1.0, 0.0))
    row_sign, lane_sign = (s * (0.5 * time_step) for s in (row_sign, lane_sign))
    row_visc, lane_visc = (jnp.abs(s) * (2.0 * viscosity) for s in (row_sign, lane_sign))

    def interleave(low, high):
        even = lax.rem(lane, 2) == 0
        return jnp.where(even, low, high), jnp.where(even, high, low)

    def unpack(which, at):
        return pltpu.roll(which, lax.rem(2 * nz - at, nz), 1)

    def rows(f, x):
        return jnp.where(
            row < ny // 2,
            jnp.broadcast_to(yhalo[0, f, pl.ds(x, 1), :], (ny, nz)),
            jnp.broadcast_to(yhalo[1, f, pl.ds(x, 1), :], (ny, nz)))

    def correct(x, which, components, with_rows=True):
        by_row = row_visc + row_sign * blk[2, x + 1]
        by_lane = lane_visc + lane_sign * blk[3, x + 1]
        inverse, v = inv[x], vp[0, x]
        for k in components:
            value = by_lane * unpack(which, (1 + k) * nx + x)
            if with_rows:
                value = value + by_row * rows(1 + k, x)
            if k == 1:
                value = value + row_sign * rows(0, x)
            if k == 2:
                value = value + lane_sign * unpack(which, x)
            value = ustar[k, x] + value * inverse
            ustar[k, x] = value
            flux[k, x] = v * value

    def correct_all(pair, components, with_rows=True):
        def body(i, carry):
            correct(2 * i, pair[0], components, with_rows)
            correct(2 * i + 1, pair[1], components, with_rows)
            return carry

        lax.fori_loop(0, nx // 2, body, 0, unroll=4)

    x2 = exchange(flux.at[0, 0], flux.at[0, nx - 1], fxhalo.at[0], fxhalo.at[1], 0, (8,), "gx", up_x, down_x)
    y2 = exchange(ypack.at[0, 4], ypack.at[1, 4], fyhalo.at[0], fyhalo.at[1], 1, (9,), "gy", up_y, down_y)
    z2 = exchange(fzpack.at[0], fzpack.at[1], fzhalo.at[0], fzhalo.at[1], 2, (10,), "gz", z_up, z_down)

    def send_flux_z():
        low, high = pack_z(1, lambda f, x: flux[2, x])
        fzpack[0] = low
        fzpack[1] = high
        for copy in z2:
            copy.start()

    z_low = pltpu.roll(zhalo[0], 1, 1)
    @pl.when(z_last)
    def _():
        correct_all(interleave(z_low, zero), (2,))
        send_flux_z()

    pl.when(z_last)(z1[1].wait_recv)
    z_high = pltpu.roll(zhalo[1], nz - 1, 1)
    joined = interleave(z_low, z_high)
    pl.when(not_first)(across_edges)
    finish_y(yhalo.at[:, rest], yhalo.at[0, rest], 3)
    correct_all(joined, (0, 1))
    ypack[0, 4] = flux[1, :, 0, :]
    ypack[1, 4] = flux[1, :, ny - 1, :]
    start(y2, not_high_y, not_low_y)
    start(x2, not_high_x, not_low_x)

    @pl.when(z_first)
    def _():
        zc.wait_recv()
        product = chalo[...] * zpack[0]
        acc[...] += product
        sum_up()
        product = product + pltpu.roll(product, nz - 3 * nx, 1)
        edge[...] = jnp.where(lane < nx, product, 0.0)

    @pl.when(not_first)
    def _():
        edge[...] = zero

    @pl.when(z_last)
    def _():
        correct_all(interleave(zero, z_high), (2,), False)

    @pl.when(not_last)
    def _():
        correct_all(joined, (2,))
        send_flux_z()

    for within, side in ((not_low_x, 0), (not_high_x, 1)):
        @pl.when(jnp.logical_not(within))
        def _():
            fxhalo[side] = zero
    for within, side in ((not_low_y, 0), (not_high_y, 1)):
        @pl.when(jnp.logical_not(within))
        def _():
            fyhalo[side] = jnp.zeros((nx, nz), jnp.float32)

    copy_to(vzpack, vzhalo, 2, 6, "gz", z_up).wait_recv()
    v_joined = interleave(pltpu.roll(vzhalo[0], 1, 1), pltpu.roll(vzhalo[1], nz - 1, 1))

    def source_plane(x, odd, x_low, x_high):
        fy, fz, v = flux[1, x], flux[2, x], vp[0, x]
        y_low = jnp.where(first_row, 0.0, pltpu.roll(fy, 1, 0))
        y_high = jnp.where(last_row, 0.0, pltpu.roll(fy, ny - 1, 0))
        z_low = jnp.where(first_lane, 0.0, pltpu.roll(fz, 1, 1))
        z_high = jnp.where(last_lane, 0.0, pltpu.roll(fz, nz - 1, 1))
        v_halo = unpack(v_joined[odd], x)
        v_low = jnp.where(first_lane, v_halo, pltpu.roll(v, 1, 1))
        v_high = jnp.where(last_lane, v_halo, pltpu.roll(v, nz - 1, 1))
        div[x] = 0.5 * ((x_high - x_low) + (y_high - y_low) + (z_high - z_low))
        slope[x] = (0.5 * time_step) * (v_high - v_low)

    def source_body(i, carry):
        x = 2 * i + 1
        source_plane(x, 1, flux[0, x - 1], flux[0, x + 1])
        source_plane(x + 1, 0, flux[0, x], flux[0, x + 2])
        return carry

    lax.fori_loop(0, nx // 2 - 1, source_body, 0, unroll=3)
    phase = 0
    while phase < len(phases) - 1:
        total = recv_sum(phase)
        phase += 1
        send_sum(phase, total)
    finish_x(fxhalo, fxhalo.at[0], 8)
    source_plane(0, 0, fxhalo[0], flux[0, 1])
    source_plane(nx - 1, 1, flux[0, nx - 2], fxhalo[1])
    finish_y(fyhalo, fyhalo.at[0], 9)
    copy_to(fzpack, fzhalo, 2, 10, "gz", z_up).wait_recv()
    f_joined = interleave(pltpu.roll(fzhalo[0], 1, 1) + edge[...], pltpu.roll(fzhalo[1], nz - 1, 1))
    row_half, lane_half = row_sign / time_step, lane_sign / time_step

    def edge_plane(x, odd):
        y_halo = jnp.where(
            row < ny // 2,
            jnp.broadcast_to(fyhalo[0, pl.ds(x, 1), :], (ny, nz)),
            jnp.broadcast_to(fyhalo[1, pl.ds(x, 1), :], (ny, nz)))
        div[x] = div[x] - row_half * y_halo - lane_half * unpack(f_joined[odd], x)

    def edge_body(i, carry):
        edge_plane(2 * i, 0)
        edge_plane(2 * i + 1, 1)
        return carry

    lax.fori_loop(0, nx // 2, edge_body, 0, unroll=16)

    for which in range(len(phases)):
        all_sums(which).wait_send()
    sent = inv.at[pl.ds(0, 5)]
    settle(inv.at[pl.ds(0, 10)], sent, 0, 0, not_high_x, not_low_x, False)
    settle(ypack, ypack.at[0], 1, 2, not_high_y, not_low_y, False)
    sent = inv.at[pl.ds(0, 6)]
    copy_to(sent, sent, 2, 4, "gz", z_up).wait_send()
    pl.when(z_last)(zc.wait_send)

    total = recv_sum(phase)
    half = line < nz // 2
    flow_sum = jnp.sum(jnp.where(half, total, 0.0), axis=1, keepdims=True)
    void_sum = jnp.sum(jnp.where(half, 0.0, total), axis=1, keepdims=True)
    cells = float(nx * ny * nz * gx * gy * gz)
    step = (target[0] * cells - flow_sum) / (time_step * void_sum)
    lines[0] = jnp.broadcast_to(step, (1, nz)) + force
    lines[1] = jnp.broadcast_to(step, (1, nz))


def shift_kernel(ustar, div, slope, lines, vel_out, source_out, forcing_out, upward, source, sem):
    nx, ny, nz = div.shape
    half = nx // 2
    copies = [
        pltpu.make_async_copy(ustar.at[pl.ds(0, 2)], vel_out.at[pl.ds(0, 2)], sem.at[0]),
        pltpu.make_async_copy(lines.at[0], forcing_out, sem.at[1]),
    ]
    for copy in copies:
        copy.start()
    step = jnp.broadcast_to(lines[1], (ny, nz))
    for part in range(2):
        def body(i, carry):
            x = part * half + i
            upward[x] = ustar[2, x] + time_step * step
            source[x] = div[x] + step * slope[x]
            return carry

        lax.fori_loop(0, half, body, 0, unroll=8)
        planes = pl.ds(part * half, half)
        for copy in (
            pltpu.make_async_copy(upward.at[planes], vel_out.at[2, planes], sem.at[2 + 2 * part]),
            pltpu.make_async_copy(source.at[planes], source_out.at[planes], sem.at[3 + 2 * part]),
        ):
            copy.start()
            copies.append(copy)
    for copy in copies:
        copy.wait()


def local(velocity, pressure, voidage, particle_vel, forcing, target_flux):
    nx, ny, nz = voidage.shape
    sizes = tuple(lax.axis_size(a) for a in ("gx", "gy", "gz"))
    if math.prod(sizes) <= DIRECT_LIMIT:
        phases = (("gz", "gy", "gx"),)
    else:
        phases = (("gy", "gx"), ("gz",))
    slot_count = sum(math.prod(lax.axis_size(a) for a in axes) for axes in phases)
    f32 = jnp.float32
    vmem = pl.BlockSpec(memory_space=pltpu.VMEM)
    smem = pl.BlockSpec(memory_space=pltpu.SMEM)
    hbm = pl.BlockSpec(memory_space=pltpu.HBM)
    dma = pltpu.SemaphoreType.DMA
    faces = [pltpu.VMEM((2, ny, nz), f32), pltpu.VMEM((2, ny, nz), f32)]
    face = [pltpu.VMEM((ny, nz), f32)]
    results = pl.pallas_call(
        functools.partial(kernel, sizes, phases),
        out_shape=(
            pltpu.VMEM((3, nx, ny, nz), f32),
            pltpu.VMEM((nx, ny, nz), f32),
            pltpu.VMEM((nx, ny, nz), f32),
            pltpu.VMEM((2, 1, nz), f32),
        ),
        in_specs=[hbm] * 4 + [smem] * 2,
        out_specs=(vmem,) * 4,
        scratch_shapes=[
            pltpu.VMEM((4, nx + 2, ny, nz), f32),
            pltpu.VMEM((4, nx, ny, nz), f32),
            pltpu.VMEM((nx, ny, nz), f32),
            pltpu.VMEM((nx, ny, nz), f32),
            pltpu.VMEM((3, nx, ny, nz), f32),
        ] + face + face + [
            pltpu.VMEM((2, 5, nx, nz), f32),
            pltpu.VMEM((2, 4, nx, nz), f32),
        ] + faces + face + face + faces + [
            pltpu.VMEM((2, nx, nz), f32),
            pltpu.VMEM((2, ny, nz), f32),
        ] + faces + [
            pltpu.VMEM((slot_count, 1, nz), f32),
            dma((2,)), dma((4,)), dma((11,)),
            dma((len(phases),)), dma((len(phases),)),
            pltpu.SemaphoreType.REGULAR((4 + len(phases),)),
        ],
        compiler_params=pltpu.CompilerParams(collective_id=0, has_side_effects=True),
    )(velocity, pressure, voidage, particle_vel, forcing, target_flux)
    vel_new, source, forcing_new = pl.pallas_call(
        shift_kernel,
        out_shape=(
            jax.ShapeDtypeStruct((3, nx, ny, nz), f32),
            jax.ShapeDtypeStruct((nx, ny, nz), f32),
            jax.ShapeDtypeStruct((1, nz), f32),
        ),
        in_specs=[vmem] * 4,
        out_specs=(hbm,) * 3,
        scratch_shapes=[
            pltpu.VMEM((nx, ny, nz), f32),
            pltpu.VMEM((nx, ny, nz), f32),
            dma((6,)),
        ],
    )(*(pltpu.with_memory_space_constraint(a, pltpu.VMEM) for a in results))
    return vel_new, source, forcing_new[0, :1]


def solution(mesh):
    return jax.shard_map(
        local,
        mesh=mesh,
        in_specs=(
            P(None, "gx", "gy", "gz"),
            P("gx", "gy", "gz"),
            P("gx", "gy", "gz"),
            P(None, "gx", "gy", "gz"),
            P(),
            P(),
        ),
        out_specs=(P(None, "gx", "gy", "gz"), P("gx", "gy", "gz"), P()),
        check_vma=False,
    )
```

```python
import functools
import math

import jax
import jax.numpy as jnp
from jax import lax
from jax.experimental import pallas as pl
from jax.experimental.pallas import tpu as pltpu
from jax.sharding import PartitionSpec as P

time_step = 0.2
viscosity = 0.1
drag_scale = 1.0
MESH = pl.DeviceIdType.MESH
DIRECT_LIMIT = 64
TINY = 1.1754944e-38


def ring_index(axes):
    index = 0
    for axis in axes:
        index = index * lax.axis_size(axis) + lax.axis_index(axis)
    return index


def ring_device(axes, index):
    device = {}
    for axis in reversed(axes):
        size = lax.axis_size(axis)
        device[axis] = lax.rem(index, size)
        index = lax.div(index, size)
    return device


def kernel(
    sizes, phases,
    vel_hbm, pres_hbm, void_hbm, part_hbm, forcing, target,
    ustar, div, slope, lines,
    blk, vp, inv, weight, flux, acc, edge, ypack, yhalo, zpack, zhalo, wpack, whalo,
    vzpack, vzhalo, fyhalo, fxhalo, fzpack, fzhalo, slots,
    load_sem, send, recv, sum_send, sum_recv, ready,
):
    gx, gy, gz = sizes
    nx, ny, nz = div.shape
    x_at, y_at, z_at = (lax.axis_index(a) for a in ("gx", "gy", "gz"))
    not_low_x, not_high_x = x_at > 0, x_at < gx - 1
    not_low_y, not_high_y = y_at > 0, y_at < gy - 1
    z_up, z_down = lax.rem(z_at + 1, gz), lax.rem(z_at + gz - 1, gz)
    z_first, z_last = z_at == 0, z_at == gz - 1
    not_first, not_last = z_at > 0, z_at < gz - 1

    def signal(sem, device):
        pl.semaphore_signal(sem, inc=1, device_id=device, device_id_type=MESH)

    def members(which):
        axes = phases[which]
        count = math.prod(lax.axis_size(a) for a in axes)
        base = sum(math.prod(lax.axis_size(a) for a in phases[w]) for w in range(which))
        return axes, count, base, ring_index(axes)

    plane = gx * gy
    direct = len(phases) == 1
    if direct:
        near = ((1, gx, plane, plane * (gz - 1)),)
    else:
        near = ((1, gx), (1, gz - 1))
    barrier = pltpu.get_barrier_semaphore()
    pl.when(not_high_x)(lambda: signal(barrier, {"gx": x_at + 1}))
    pl.when(not_high_y)(lambda: signal(barrier, {"gy": y_at + 1}))
    pl.when(not_last)(lambda: signal(barrier, {"gz": z_at + 1}))
    pl.when(z_first)(lambda: signal(barrier, {"gz": gz - 1}))
    lower = sum(jnp.where(c, 1, 0) for c in (not_low_x, not_low_y, not_first, z_last))
    for which in range(len(phases)):
        axes, count, _, me = members(which)
        far = me < count - 1
        for d in near[which]:
            far = far & (me != count - 1 - d)
        pl.when(far)(lambda: signal(barrier, ring_device(axes, count - 1)))
        lower = lower + jnp.where(me == count - 1, count - 1 - len(near[which]), 0)

    inside = pl.ds(1, nx)
    for load in (
        pltpu.make_async_copy(vel_hbm, blk.at[pl.ds(1, 3), inside], load_sem.at[0]),
        pltpu.make_async_copy(pres_hbm, blk.at[0, inside], load_sem.at[0]),
        pltpu.make_async_copy(void_hbm, vp.at[0], load_sem.at[1]),
        pltpu.make_async_copy(part_hbm, vp.at[pl.ds(1, 3)], load_sem.at[1]),
    ):
        load.start()

    lane = lax.broadcasted_iota(jnp.int32, (ny, nz), 1)
    row = lax.broadcasted_iota(jnp.int32, (ny, nz), 0)
    zero = jnp.zeros((ny, nz), jnp.float32)

    even = lax.rem(lane, 2) == 0
    pairs = (lax.div(lax.rem(lane + 1, nz), 2), lax.div(lane, 2))

    def interleave(low, high):
        return jnp.where(even, low, high), jnp.where(even, high, low)

    def pack_z(fields, read, at=0):
        tiles = []
        for odd in range(2):
            total = None
            for f in range(fields):
                tile = zero
                for x in range(odd, nx, 2):
                    turned = read(f, x)
                    to = (at + f * nx + x) % nz
                    if to:
                        turned = pltpu.roll(turned, to, 1)
                    tile = jnp.where(pairs[odd] == to // 2, turned, tile)
                total = tile if total is None else total + tile
            tiles.append(total)
        return interleave(*tiles)

    def copy_to(src, dst, send_at, recv_at, axis, device):
        return pltpu.make_async_remote_copy(
            src, dst, send.at[send_at], recv.at[recv_at],
            device_id={axis: device}, device_id_type=MESH)

    def exchange(low, high, dst_low, dst_high, send_at, recvs, axis, up, down):
        return (copy_to(high, dst_low, send_at, recvs[0], axis, up),
                copy_to(low, dst_high, send_at, recvs[-1], axis, down))

    def start(pair, high, low):
        pl.when(high)(pair[0].start)
        pl.when(low)(pair[1].start)

    def settle(both, one, send_at, recv_at, high, low, received):
        def wait(ref):
            copy = copy_to(ref, ref, send_at, recv_at, "gz", z_up)
            return copy.wait_recv if received else copy.wait_send

        pl.when(high & low)(wait(both))
        pl.when(high ^ low)(wait(one))

    def finish_x(both, one, recv_at):
        settle(both, one, 0, recv_at, not_high_x, not_low_x, True)

    def finish_y(both, one, recv_at):
        settle(both, one, 1, recv_at, not_high_y, not_low_y, True)

    up_x, down_x = jnp.minimum(x_at + 1, gx - 1), jnp.maximum(x_at - 1, 0)
    up_y, down_y = jnp.minimum(y_at + 1, gy - 1), jnp.maximum(y_at - 1, 0)
    rest = pl.ds(0, 3)

    def along_x(fields, recvs):
        return exchange(blk.at[fields, 1], blk.at[fields, nx], blk.at[fields, 0], blk.at[fields, nx + 1],
                        0, recvs, "gx", up_x, down_x)

    def along_y(fields, recvs):
        return exchange(ypack.at[0, fields], ypack.at[1, fields], yhalo.at[0, fields], yhalo.at[1, fields],
                        1, recvs, "gy", up_y, down_y)

    x1, x1_rest = along_x(3, (0,)), along_x(rest, (1,))
    y1, y1_rest = along_y(3, (2,)), along_y(rest, (3,))
    z1 = exchange(zpack.at[0], zpack.at[1], zhalo.at[0], zhalo.at[1], 2, (4, 5), "gz", z_up, z_down)
    zv = exchange(vzpack.at[0], vzpack.at[1], vzhalo.at[0], vzhalo.at[1], 2, (6,), "gz", z_up, z_down)
    zc = copy_to(wpack, whalo, 3, 7, "gz", z_up)

    pl.when(lower > 0)(lambda: pl.semaphore_wait(barrier, lower))
    pl.when(not_low_y)(lambda: signal(ready.at[1], {"gy": down_y}))
    pl.when(not_low_x)(lambda: signal(ready.at[0], {"gx": down_x}))
    pl.when(not_first)(lambda: signal(ready.at[2], {"gz": z_down}))
    pl.when(z_last)(lambda: signal(ready.at[3], {"gz": z_up}))
    for which in range(len(phases)):
        axes, count, _, me = members(which)

        @pl.when(me == count - 1)
        def _():
            for k in range(count - 1):
                signal(ready.at[4 + which], ring_device(axes, k))
    pltpu.make_async_copy(blk.at[:, inside], blk.at[:, inside], load_sem.at[0]).wait()
    for side, y in ((0, 0), (1, ny - 1)):
        ypack[side, 3] = blk[3, inside, y, :]
    pl.when(not_low_y)(y1[1].start)
    pl.when(not_low_x)(x1[1].start)
    low, high = pack_z(4, lambda f, x: blk[f, x + 1])
    zpack[0] = low
    zpack[1] = high
    pl.when(not_first)(z1[1].start)
    pl.when(z_last)(z1[0].start)
    pltpu.make_async_copy(vp, vp, load_sem.at[1]).wait()
    force = forcing[0]

    def drag_plane(x):
        v = vp[0, x]
        c = [blk[1 + k, x + 1] for k in range(3)]
        q = [vp[1 + k, x] for k in range(3)]
        square = sum((c[k] - q[k]) ** 2 for k in range(3))
        slip = square * lax.rsqrt(jnp.maximum(square, TINY))
        drag = drag_scale * (1.0 - v) * jnp.exp(-2.65 * jnp.log(v)) * (1.0 + slip)
        step_drag = time_step * drag
        inverse = 1.0 / (1.0 + step_drag)
        w = v * inverse
        inv[x] = inverse
        weight[x] = w
        for k in range(3):
            ustar[k, x] = c[k] + step_drag * q[k]
        return w

    weights = [drag_plane(x) for x in range(nx)]
    w_low, w_high = pack_z(1, lambda f, x: weights[x], 3 * nx)
    wpack[...] = w_high
    pl.when(z_last)(zc.start)

    for higher, which, copy in ((not_high_x, 0, x1[0]), (not_high_y, 1, y1[0]), (not_last, 2, z1[0])):
        @pl.when(higher)
        def _():
            pl.semaphore_wait(ready.at[which], 1)
            copy.start()
    def coefficients(face, w, sign, at):
        upward = w * (time_step * viscosity + (sign * 0.5 * time_step) * face)
        pressed = (sign * 0.5 * time_step) * pltpu.roll(w, nz - 3 * nx, 1)
        return jnp.where(at < nx, pressed,
                         jnp.where((at >= 3 * nx) & (at < 4 * nx), upward, 0.0))

    c_low = pltpu.roll(coefficients(zpack[0], w_low, 1.0, lane), nz - 1, 1)
    c_high = pltpu.roll(coefficients(zpack[1], w_high, -1.0, lax.rem(lane + 1, nz)), 1, 1)
    for f in range(3):
        ypack[0, f] = blk[f, inside, 0, :]
        ypack[1, f] = blk[f, inside, ny - 1, :]
    def wall_x(within, halo_plane, edge_plane):
        @pl.when(jnp.logical_not(within))
        def _():
            for f in range(1, 4):
                blk[f, halo_plane] = zero
            blk[0, halo_plane] = blk[0, edge_plane]

    wall_x(not_low_x, 0, 1)
    wall_x(not_high_x, nx + 1, nx)

    def wall_y(within, side):
        @pl.when(jnp.logical_not(within))
        def _():
            for f in range(1, 4):
                yhalo[side, f] = jnp.zeros((nx, nz), jnp.float32)
            yhalo[side, 0] = ypack[side, 0]

    wall_y(not_low_y, 0)
    wall_y(not_high_y, 1)

    def stencil(x, k):
        p = x + 1
        centre = [blk[1 + f, p] for f in range(3)]

        def pair(f, axis_no):
            if axis_no == 0:
                return blk[f, p - 1], blk[f, p + 1]
            field = blk[f, p]
            if axis_no == 1:
                return (jnp.where(row == 0, 0.0, pltpu.roll(field, 1, 0)),
                        jnp.where(row == ny - 1, 0.0, pltpu.roll(field, ny - 1, 0)))
            return (jnp.where(lane == 0, 0.0, pltpu.roll(field, 1, 1)),
                    jnp.where(lane == nz - 1, 0.0, pltpu.roll(field, nz - 1, 1)))

        advect = total = None
        for axis_no in range(3):
            low, high = pair(1 + k, axis_no)
            term = centre[axis_no] * (high - low)
            both = high + low
            advect = term if advect is None else advect + term
            total = both if total is None else total + both
        low, high = pair(0, k)
        forces = (viscosity * (total - 6.0 * centre[k])
                  - 0.5 * (advect + (high - low)))
        if k == 2:
            forces = forces + force
        value = ustar[k, x] + time_step * forces
        ustar[k, x] = value * inv[x]
        return value

    def upward_body(i, flow):
        for x in (1 + 2 * i, 2 + 2 * i):
            flow = flow + weight[x] * stencil(x, 2)
        return flow

    flow = lax.fori_loop(0, (nx - 2) // 2, upward_body, zero, unroll=3)

    start(x1_rest, not_high_x, not_low_x)
    start(y1_rest, not_high_y, not_low_y)

    low, high = pack_z(1, lambda f, x: vp[0, x])
    vzpack[0] = low
    vzpack[1] = high
    zv[0].start()
    pl.when(not_first)(zv[1].start)

    def along_y_coefficients(side, sign):
        w = weight[:, 0 if side == 0 else ny - 1, :]
        return w * (time_step * viscosity + (sign * 0.5 * time_step) * ypack[side, 2])

    cy_low, cy_high = along_y_coefficients(0, 1.0), along_y_coefficients(1, -1.0)

    def fold(value):
        value = jnp.sum(value, axis=0, keepdims=True)
        return value + pltpu.roll(value, nz // 2, 1)

    line = lax.broadcasted_iota(jnp.int32, (1, nz), 1)
    void_line = fold(lax.fori_loop(0, nx, lambda x, total: total + vp[0, x], zero, unroll=8))

    def across_body(i, carry):
        for x in (1 + 2 * i, 2 + 2 * i):
            stencil(x, 0)
            stencil(x, 1)
        return carry

    lax.fori_loop(0, (nx - 2) // 2, across_body, 0, unroll=3)
    @pl.when(z_first)
    def _():
        pl.semaphore_wait(ready.at[3], 1)
        z1[1].start()
        zv[1].start()

    def sum_copy(which, src, dst, device):
        return pltpu.make_async_remote_copy(
            src, dst, sum_send.at[which], sum_recv.at[which], device_id=device, device_id_type=MESH)

    def all_in(which):
        _, count, _, me = members(which)

        @pl.when(me < count - 1)
        def _():
            pl.semaphore_wait(ready.at[4 + which], 1)

    def send_sum(which, value):
        axes, count, base, me = members(which)
        mine = slots.at[base + me]
        slots[base + me] = value
        for k in range(count - 1):
            other = jnp.where(k < me, k, k + 1)
            sum_copy(which, mine, mine, ring_device(axes, other)).start()

    def all_sums(which):
        axes, count, base, me = members(which)
        others = slots.at[pl.ds(base, count - 1)]
        return sum_copy(which, others, others, ring_device(axes, lax.rem(me + 1, count)))

    def recv_sum(which):
        axes, count, base, me = members(which)
        all_sums(which).wait_recv()
        return jnp.sum(slots[pl.ds(base, count)], axis=0)

    finish_x(blk.at[3, pl.ds(0, 2)], blk.at[3, 0], 0)
    flow = flow + weight[0] * stencil(0, 2) + weight[nx - 1] * stencil(nx - 1, 2)
    acc[...] = flow
    finish_y(yhalo.at[:, 3], yhalo.at[0, 3], 2)
    y_line = jnp.sum(cy_low * yhalo[0, 3] + cy_high * yhalo[1, 3], axis=0, keepdims=True)
    def across_edges():
        finish_x(blk.at[rest, pl.ds(0, 2)], blk.at[rest, 0], 1)
        for x in (0, nx - 1):
            stencil(x, 0)
            stencil(x, 1)

    pl.when(z_first)(across_edges)
    z1[0].wait_recv()
    acc[...] += c_low * zhalo[0]

    @pl.when(z_first)
    def _():
        face = pltpu.roll(zpack[0], nz - 1, 1)
        edge[...] = ((time_step * viscosity - (0.5 * time_step) * zhalo[0]) * face
                     - (0.5 * time_step) * pltpu.roll(face, 3 * nx, 1))

    @pl.when(jnp.logical_not(z_last))
    def _():
        z1[1].wait_recv()
        acc[...] += c_high * zhalo[1]

    def sum_up():
        flow_line = jnp.sum(acc[...], axis=0, keepdims=True) + y_line
        flow_line = flow_line + pltpu.roll(flow_line, nz // 2, 1)
        send_sum(0, jnp.where(line < nz // 2, flow_line, void_line))

    for which in range(len(phases)):
        all_in(which)
    pl.when(jnp.logical_not(z_first))(sum_up)

    first_row = row == 0
    last_row = row == ny - 1
    first_lane = lane == 0
    last_lane = lane == nz - 1
    row_sign = jnp.where(first_row, 1.0, jnp.where(last_row, -1.0, 0.0))
    lane_sign = jnp.where(first_lane, 1.0, jnp.where(last_lane, -1.0, 0.0))
    row_sign, lane_sign = (s * (0.5 * time_step) for s in (row_sign, lane_sign))
    row_visc, lane_visc = (jnp.abs(s) * (2.0 * viscosity) for s in (row_sign, lane_sign))

    def unpack(which, at):
        return pltpu.roll(which, lax.rem(2 * nz - at, nz), 1)

    def rows(f, x):
        return jnp.where(
            row < ny // 2,
            jnp.broadcast_to(yhalo[0, f, pl.ds(x, 1), :], (ny, nz)),
            jnp.broadcast_to(yhalo[1, f, pl.ds(x, 1), :], (ny, nz)))

    def correct(x, which, components, with_rows=True):
        by_row = row_visc + row_sign * blk[2, x + 1]
        by_lane = lane_visc + lane_sign * blk[3, x + 1]
        inverse, v = inv[x], vp[0, x]
        for k in components:
            value = by_lane * unpack(which, (1 + k) * nx + x)
            if with_rows:
                value = value + by_row * rows(1 + k, x)
            if k == 1:
                value = value + row_sign * rows(0, x)
            if k == 2:
                value = value + lane_sign * unpack(which, x)
            value = ustar[k, x] + value * inverse
            ustar[k, x] = value
            flux[k, x] = v * value

    def correct_all(pair, components, with_rows=True):
        def body(i, carry):
            correct(2 * i, pair[0], components, with_rows)
            correct(2 * i + 1, pair[1], components, with_rows)
            return carry

        lax.fori_loop(0, nx // 2, body, 0, unroll=4)

    x2 = exchange(flux.at[0, 0], flux.at[0, nx - 1], fxhalo.at[0], fxhalo.at[1], 0, (8,), "gx", up_x, down_x)
    y2 = exchange(ypack.at[0, 4], ypack.at[1, 4], fyhalo.at[0], fyhalo.at[1], 1, (9,), "gy", up_y, down_y)
    z2 = exchange(fzpack.at[0], fzpack.at[1], fzhalo.at[0], fzhalo.at[1], 2, (10,), "gz", z_up, z_down)

    def send_flux_z():
        low, high = pack_z(1, lambda f, x: flux[2, x])
        fzpack[0] = low
        fzpack[1] = high
        for copy in z2:
            copy.start()

    z_low = pltpu.roll(zhalo[0], 1, 1)
    @pl.when(z_last)
    def _():
        correct_all(interleave(z_low, zero), (2,))
        send_flux_z()

    pl.when(z_last)(z1[1].wait_recv)
    z_high = pltpu.roll(zhalo[1], nz - 1, 1)
    joined = interleave(z_low, z_high)
    pl.when(not_first)(across_edges)
    finish_y(yhalo.at[:, rest], yhalo.at[0, rest], 3)
    correct_all(joined, (0, 1))
    ypack[0, 4] = flux[1, :, 0, :]
    ypack[1, 4] = flux[1, :, ny - 1, :]
    start(y2, not_high_y, not_low_y)
    start(x2, not_high_x, not_low_x)

    @pl.when(z_first)
    def _():
        zc.wait_recv()
        product = whalo[...] * edge[...]
        acc[...] += product
        sum_up()
        edge[...] = jnp.where(lane < nx, pltpu.roll(product, nz - 3 * nx + 1, 1), 0.0)

    @pl.when(not_first)
    def _():
        edge[...] = zero

    @pl.when(z_last)
    def _():
        correct_all(interleave(zero, z_high), (2,), False)

    @pl.when(not_last)
    def _():
        correct_all(joined, (2,))
        send_flux_z()

    for within, side in ((not_low_x, 0), (not_high_x, 1)):
        @pl.when(jnp.logical_not(within))
        def _():
            fxhalo[side] = zero
    for within, side in ((not_low_y, 0), (not_high_y, 1)):
        @pl.when(jnp.logical_not(within))
        def _():
            fyhalo[side] = jnp.zeros((nx, nz), jnp.float32)

    copy_to(vzpack, vzhalo, 2, 6, "gz", z_up).wait_recv()
    v_joined = interleave(pltpu.roll(vzhalo[0], 1, 1), pltpu.roll(vzhalo[1], nz - 1, 1))

    def source_plane(x, odd, x_low, x_high):
        fy, fz, v = flux[1, x], flux[2, x], vp[0, x]
        y_low = jnp.where(first_row, 0.0, pltpu.roll(fy, 1, 0))
        y_high = jnp.where(last_row, 0.0, pltpu.roll(fy, ny - 1, 0))
        z_low = jnp.where(first_lane, 0.0, pltpu.roll(fz, 1, 1))
        z_high = jnp.where(last_lane, 0.0, pltpu.roll(fz, nz - 1, 1))
        v_halo = unpack(v_joined[odd], x)
        v_low = jnp.where(first_lane, v_halo, pltpu.roll(v, 1, 1))
        v_high = jnp.where(last_lane, v_halo, pltpu.roll(v, nz - 1, 1))
        div[x] = 0.5 * ((x_high - x_low) + (y_high - y_low) + (z_high - z_low))
        slope[x] = (0.5 * time_step) * (v_high - v_low)

    def source_body(i, carry):
        x = 2 * i + 1
        source_plane(x, 1, flux[0, x - 1], flux[0, x + 1])
        source_plane(x + 1, 0, flux[0, x], flux[0, x + 2])
        return carry

    lax.fori_loop(0, nx // 2 - 1, source_body, 0, unroll=3)
    phase = 0
    while phase < len(phases) - 1:
        total = recv_sum(phase)
        phase += 1
        send_sum(phase, total)
    finish_x(fxhalo, fxhalo.at[0], 8)
    source_plane(0, 0, fxhalo[0], flux[0, 1])
    source_plane(nx - 1, 1, flux[0, nx - 2], fxhalo[1])
    finish_y(fyhalo, fyhalo.at[0], 9)
    copy_to(fzpack, fzhalo, 2, 10, "gz", z_up).wait_recv()
    f_joined = interleave(pltpu.roll(fzhalo[0], 1, 1) + edge[...], pltpu.roll(fzhalo[1], nz - 1, 1))
    row_half, lane_half = row_sign / time_step, lane_sign / time_step

    def edge_plane(x, odd):
        y_halo = jnp.where(
            row < ny // 2,
            jnp.broadcast_to(fyhalo[0, pl.ds(x, 1), :], (ny, nz)),
            jnp.broadcast_to(fyhalo[1, pl.ds(x, 1), :], (ny, nz)))
        div[x] = div[x] - row_half * y_halo - lane_half * unpack(f_joined[odd], x)

    def edge_body(i, carry):
        edge_plane(2 * i, 0)
        edge_plane(2 * i + 1, 1)
        return carry

    lax.fori_loop(0, nx // 2, edge_body, 0, unroll=16)

    for which in range(len(phases)):
        all_sums(which).wait_send()
    sent = inv.at[pl.ds(0, 5)]
    settle(inv.at[pl.ds(0, 10)], sent, 0, 0, not_high_x, not_low_x, False)
    settle(ypack, ypack.at[0], 1, 2, not_high_y, not_low_y, False)
    sent = inv.at[pl.ds(0, 6)]
    copy_to(sent, sent, 2, 4, "gz", z_up).wait_send()
    pl.when(z_last)(zc.wait_send)

    total = recv_sum(phase)
    half = line < nz // 2
    flow_sum = jnp.sum(jnp.where(half, total, 0.0), axis=1, keepdims=True)
    void_sum = jnp.sum(jnp.where(half, 0.0, total), axis=1, keepdims=True)
    cells = float(nx * ny * nz * gx * gy * gz)
    step = (target[0] * cells - flow_sum) / (time_step * void_sum)
    lines[0] = jnp.broadcast_to(step, (1, nz)) + force
    lines[1] = jnp.broadcast_to(step, (1, nz))


def shift_kernel(ustar, div, slope, lines, vel_out, source_out, forcing_out, made, sem):
    nx, ny, nz = div.shape
    half = nx // 2
    across, line = pl.ds(0, 2), pltpu.make_async_copy(lines.at[0], forcing_out, sem.at[2])
    for k in range(2):
        for part in range(2):
            planes = pl.ds(part * half, half)
            pltpu.make_async_copy(ustar.at[k, planes], vel_out.at[k, planes], sem.at[0]).start()
    line.start()
    step = jnp.broadcast_to(lines[1], (ny, nz))
    for part in range(2):
        def body(i, carry):
            x = part * half + i
            made[0, x] = ustar[2, x] + time_step * step
            made[1, x] = div[x] + step * slope[x]
            return carry

        lax.fori_loop(0, half, body, 0, unroll=8)
        planes = pl.ds(part * half, half)
        pltpu.make_async_copy(made.at[0, planes], vel_out.at[2, planes], sem.at[1]).start()
        pltpu.make_async_copy(made.at[1, planes], source_out.at[planes], sem.at[1]).start()
    pltpu.make_async_copy(ustar.at[across], vel_out.at[across], sem.at[0]).wait()
    pltpu.make_async_copy(made, vel_out.at[across], sem.at[1]).wait()
    line.wait()


def local(velocity, pressure, voidage, particle_vel, forcing, target_flux):
    nx, ny, nz = voidage.shape
    sizes = tuple(lax.axis_size(a) for a in ("gx", "gy", "gz"))
    if math.prod(sizes) <= DIRECT_LIMIT:
        phases = (("gz", "gy", "gx"),)
    else:
        phases = (("gy", "gx"), ("gz",))
    slot_count = sum(math.prod(lax.axis_size(a) for a in axes) for axes in phases)
    f32 = jnp.float32
    vmem = pl.BlockSpec(memory_space=pltpu.VMEM)
    smem = pl.BlockSpec(memory_space=pltpu.SMEM)
    hbm = pl.BlockSpec(memory_space=pltpu.HBM)
    dma = pltpu.SemaphoreType.DMA
    faces = [pltpu.VMEM((2, ny, nz), f32), pltpu.VMEM((2, ny, nz), f32)]
    face = [pltpu.VMEM((ny, nz), f32)]
    results = pl.pallas_call(
        functools.partial(kernel, sizes, phases),
        out_shape=(
            pltpu.VMEM((3, nx, ny, nz), f32),
            pltpu.VMEM((nx, ny, nz), f32),
            pltpu.VMEM((nx, ny, nz), f32),
            pltpu.VMEM((2, 1, nz), f32),
        ),
        in_specs=[hbm] * 4 + [smem] * 2,
        out_specs=(vmem,) * 4,
        scratch_shapes=[
            pltpu.VMEM((4, nx + 2, ny, nz), f32),
            pltpu.VMEM((4, nx, ny, nz), f32),
            pltpu.VMEM((nx, ny, nz), f32),
            pltpu.VMEM((nx, ny, nz), f32),
            pltpu.VMEM((3, nx, ny, nz), f32),
        ] + face + face + [
            pltpu.VMEM((2, 5, nx, nz), f32),
            pltpu.VMEM((2, 4, nx, nz), f32),
        ] + faces + face + face + faces + [
            pltpu.VMEM((2, nx, nz), f32),
            pltpu.VMEM((2, ny, nz), f32),
        ] + faces + [
            pltpu.VMEM((slot_count, 1, nz), f32),
            dma((2,)), dma((4,)), dma((11,)),
            dma((len(phases),)), dma((len(phases),)),
            pltpu.SemaphoreType.REGULAR((4 + len(phases),)),
        ],
        compiler_params=pltpu.CompilerParams(collective_id=0, has_side_effects=True),
    )(velocity, pressure, voidage, particle_vel, forcing, target_flux)
    vel_new, source, forcing_new = pl.pallas_call(
        shift_kernel,
        out_shape=(
            jax.ShapeDtypeStruct((3, nx, ny, nz), f32),
            jax.ShapeDtypeStruct((nx, ny, nz), f32),
            jax.ShapeDtypeStruct((1, nz), f32),
        ),
        in_specs=[vmem] * 4,
        out_specs=(hbm,) * 3,
        scratch_shapes=[
            pltpu.VMEM((2, nx, ny, nz), f32),
            dma((3,)),
        ],
    )(*(pltpu.with_memory_space_constraint(a, pltpu.VMEM) for a in results))
    return vel_new, source, forcing_new[0, :1]


def solution(mesh):
    return jax.shard_map(
        local,
        mesh=mesh,
        in_specs=(
            P(None, "gx", "gy", "gz"),
            P("gx", "gy", "gz"),
            P("gx", "gy", "gz"),
            P(None, "gx", "gy", "gz"),
            P(),
            P(),
        ),
        out_specs=(P(None, "gx", "gy", "gz"), P("gx", "gy", "gz"), P()),
        check_vma=False,
    )
```

```python
import functools
import math

import jax
import jax.numpy as jnp
from jax import lax
from jax.experimental import pallas as pl
from jax.experimental.pallas import tpu as pltpu
from jax.sharding import PartitionSpec as P

time_step = 0.2
viscosity = 0.1
drag_scale = 1.0
MESH = pl.DeviceIdType.MESH
DIRECT_LIMIT = 64
TINY = 1.1754944e-38


def ring_index(axes):
    index = 0
    for axis in axes:
        index = index * lax.axis_size(axis) + lax.axis_index(axis)
    return index


def ring_device(axes, index):
    device = {}
    for axis in reversed(axes):
        size = lax.axis_size(axis)
        device[axis] = lax.rem(index, size)
        index = lax.div(index, size)
    return device


def kernel(
    sizes, phases,
    vel_hbm, pres_hbm, void_hbm, part_hbm, forcing, target,
    ustar, div, slope, lines,
    blk, vp, inv, weight, flux, acc, edge, ypack, yhalo, zpack, zhalo, wpack, whalo,
    vzpack, vzhalo, fyhalo, fxhalo, fzpack, fzhalo, slots,
    load_sem, send, recv, sum_send, sum_recv, ready,
):
    gx, gy, gz = sizes
    nx, ny, nz = div.shape
    x_at, y_at, z_at = (lax.axis_index(a) for a in ("gx", "gy", "gz"))
    not_low_x, not_high_x = x_at > 0, x_at < gx - 1
    not_low_y, not_high_y = y_at > 0, y_at < gy - 1
    z_up, z_down = lax.rem(z_at + 1, gz), lax.rem(z_at + gz - 1, gz)
    z_first, z_last = z_at == 0, z_at == gz - 1
    not_first, not_last = z_at > 0, z_at < gz - 1

    def signal(sem, device):
        pl.semaphore_signal(sem, inc=1, device_id=device, device_id_type=MESH)

    def members(which):
        axes = phases[which]
        count = math.prod(lax.axis_size(a) for a in axes)
        base = sum(math.prod(lax.axis_size(a) for a in phases[w]) for w in range(which))
        return axes, count, base, ring_index(axes)

    plane = gx * gy
    direct = len(phases) == 1
    if direct:
        near = ((1, gx, plane, plane * (gz - 1)),)
    else:
        near = ((1, gx), (1, gz - 1))
    barrier = pltpu.get_barrier_semaphore()
    pl.when(not_high_x)(lambda: signal(barrier, {"gx": x_at + 1}))
    pl.when(not_high_y)(lambda: signal(barrier, {"gy": y_at + 1}))
    pl.when(not_last)(lambda: signal(barrier, {"gz": z_at + 1}))
    pl.when(z_first)(lambda: signal(barrier, {"gz": gz - 1}))
    lower = sum(jnp.where(c, 1, 0) for c in (not_low_x, not_low_y, not_first, z_last))
    for which in range(len(phases)):
        axes, count, _, me = members(which)
        far = me < count - 1
        for d in near[which]:
            far = far & (me != count - 1 - d)
        pl.when(far)(lambda: signal(barrier, ring_device(axes, count - 1)))
        lower = lower + jnp.where(me == count - 1, count - 1 - len(near[which]), 0)

    inside = pl.ds(1, nx)
    for load in (
        pltpu.make_async_copy(vel_hbm, blk.at[pl.ds(1, 3), inside], load_sem.at[0]),
        pltpu.make_async_copy(pres_hbm, blk.at[0, inside], load_sem.at[0]),
        pltpu.make_async_copy(void_hbm, vp.at[0], load_sem.at[1]),
        pltpu.make_async_copy(part_hbm, vp.at[pl.ds(1, 3)], load_sem.at[1]),
    ):
        load.start()

    lane = lax.broadcasted_iota(jnp.int32, (ny, nz), 1)
    row = lax.broadcasted_iota(jnp.int32, (ny, nz), 0)
    zero = jnp.zeros((ny, nz), jnp.float32)

    even = lax.rem(lane, 2) == 0
    pairs = (lax.div(lax.rem(lane + 1, nz), 2), lax.div(lane, 2))

    def interleave(low, high):
        return jnp.where(even, low, high), jnp.where(even, high, low)

    def pack_z(fields, read, at=0):
        tiles = []
        for odd in range(2):
            total = None
            for f in range(fields):
                tile = zero
                for x in range(odd, nx, 2):
                    turned = read(f, x)
                    to = (at + f * nx + x) % nz
                    if to:
                        turned = pltpu.roll(turned, to, 1)
                    tile = jnp.where(pairs[odd] == to // 2, turned, tile)
                total = tile if total is None else total + tile
            tiles.append(total)
        return interleave(*tiles)

    def copy_to(src, dst, send_at, recv_at, axis, device):
        return pltpu.make_async_remote_copy(
            src, dst, send.at[send_at], recv.at[recv_at],
            device_id={axis: device}, device_id_type=MESH)

    def exchange(low, high, dst_low, dst_high, send_at, recvs, axis, up, down):
        return (copy_to(high, dst_low, send_at, recvs[0], axis, up),
                copy_to(low, dst_high, send_at, recvs[-1], axis, down))

    def start(pair, high, low):
        pl.when(high)(pair[0].start)
        pl.when(low)(pair[1].start)

    def settle(both, one, send_at, recv_at, high, low, received):
        def wait(ref):
            copy = copy_to(ref, ref, send_at, recv_at, "gz", z_up)
            return copy.wait_recv if received else copy.wait_send

        pl.when(high & low)(wait(both))
        pl.when(high ^ low)(wait(one))

    def finish_x(both, one, recv_at):
        settle(both, one, 0, recv_at, not_high_x, not_low_x, True)

    def finish_y(both, one, recv_at):
        settle(both, one, 1, recv_at, not_high_y, not_low_y, True)

    up_x, down_x = jnp.minimum(x_at + 1, gx - 1), jnp.maximum(x_at - 1, 0)
    up_y, down_y = jnp.minimum(y_at + 1, gy - 1), jnp.maximum(y_at - 1, 0)
    rest = pl.ds(0, 3)

    def along_x(fields, recvs):
        return exchange(blk.at[fields, 1], blk.at[fields, nx], blk.at[fields, 0], blk.at[fields, nx + 1],
                        0, recvs, "gx", up_x, down_x)

    def along_y(fields, recvs):
        return exchange(ypack.at[0, fields], ypack.at[1, fields], yhalo.at[0, fields], yhalo.at[1, fields],
                        1, recvs, "gy", up_y, down_y)

    x1, x1_rest = along_x(3, (0,)), along_x(rest, (1,))
    y1, y1_rest = along_y(3, (2,)), along_y(rest, (3,))
    z1 = exchange(zpack.at[0], zpack.at[1], zhalo.at[0], zhalo.at[1], 2, (4, 5), "gz", z_up, z_down)
    zv = exchange(vzpack.at[0], vzpack.at[1], vzhalo.at[0], vzhalo.at[1], 2, (6,), "gz", z_up, z_down)
    zc = copy_to(wpack, whalo, 3, 7, "gz", z_up)

    pl.when(lower > 0)(lambda: pl.semaphore_wait(barrier, lower))
    pl.when(not_low_y)(lambda: signal(ready.at[1], {"gy": down_y}))
    pl.when(not_low_x)(lambda: signal(ready.at[0], {"gx": down_x}))
    pl.when(not_first)(lambda: signal(ready.at[2], {"gz": z_down}))
    pl.when(z_last)(lambda: signal(ready.at[3], {"gz": z_up}))
    for which in range(len(phases)):
        axes, count, _, me = members(which)

        @pl.when(me == count - 1)
        def _():
            for k in range(count - 1):
                signal(ready.at[4 + which], ring_device(axes, k))
    pltpu.make_async_copy(blk.at[:, inside], blk.at[:, inside], load_sem.at[0]).wait()
    for side, y in ((0, 0), (1, ny - 1)):
        ypack[side, 3] = blk[3, inside, y, :]
    pl.when(not_low_y)(y1[1].start)
    pl.when(not_low_x)(x1[1].start)
    low, high = pack_z(4, lambda f, x: blk[f, x + 1])
    zpack[0] = low
    zpack[1] = high
    pl.when(not_first)(z1[1].start)
    pl.when(z_last)(z1[0].start)
    pltpu.make_async_copy(vp, vp, load_sem.at[1]).wait()
    force = forcing[0]

    def drag_plane(x):
        v = vp[0, x]
        c = [blk[1 + k, x + 1] for k in range(3)]
        q = [vp[1 + k, x] for k in range(3)]
        square = sum((c[k] - q[k]) ** 2 for k in range(3))
        slip = square * lax.rsqrt(jnp.maximum(square, TINY))
        drag = drag_scale * (1.0 - v) * jnp.exp(-2.65 * jnp.log(v)) * (1.0 + slip)
        step_drag = time_step * drag
        inverse = 1.0 / (1.0 + step_drag)
        w = v * inverse
        inv[x] = inverse
        weight[x] = w
        for k in range(3):
            ustar[k, x] = c[k] + step_drag * q[k]
        return w

    weights = [drag_plane(x) for x in range(nx)]
    w_low, w_high = pack_z(1, lambda f, x: weights[x], 3 * nx)
    wpack[...] = w_high
    pl.when(z_last)(zc.start)

    for higher, which, copy in ((not_high_x, 0, x1[0]), (not_high_y, 1, y1[0]), (not_last, 2, z1[0])):
        @pl.when(higher)
        def _():
            pl.semaphore_wait(ready.at[which], 1)
            copy.start()
    def coefficients(face, w, sign, at):
        upward = w * (time_step * viscosity + (sign * 0.5 * time_step) * face)
        pressed = (sign * 0.5 * time_step) * pltpu.roll(w, nz - 3 * nx, 1)
        return jnp.where(at < nx, pressed,
                         jnp.where((at >= 3 * nx) & (at < 4 * nx), upward, 0.0))

    c_low = pltpu.roll(coefficients(zpack[0], w_low, 1.0, lane), nz - 1, 1)
    c_high = pltpu.roll(coefficients(zpack[1], w_high, -1.0, lax.rem(lane + 1, nz)), 1, 1)
    for f in range(3):
        ypack[0, f] = blk[f, inside, 0, :]
        ypack[1, f] = blk[f, inside, ny - 1, :]
    def wall_x(within, halo_plane, edge_plane):
        @pl.when(jnp.logical_not(within))
        def _():
            for f in range(1, 4):
                blk[f, halo_plane] = zero
            blk[0, halo_plane] = blk[0, edge_plane]

    wall_x(not_low_x, 0, 1)
    wall_x(not_high_x, nx + 1, nx)

    def wall_y(within, side):
        @pl.when(jnp.logical_not(within))
        def _():
            for f in range(1, 4):
                yhalo[side, f] = jnp.zeros((nx, nz), jnp.float32)
            yhalo[side, 0] = ypack[side, 0]

    wall_y(not_low_y, 0)
    wall_y(not_high_y, 1)

    def stencil(x, k):
        p = x + 1
        centre = [blk[1 + f, p] for f in range(3)]

        def pair(f, axis_no):
            if axis_no == 0:
                return blk[f, p - 1], blk[f, p + 1]
            field = blk[f, p]
            if axis_no == 1:
                return (jnp.where(row == 0, 0.0, pltpu.roll(field, 1, 0)),
                        jnp.where(row == ny - 1, 0.0, pltpu.roll(field, ny - 1, 0)))
            return (jnp.where(lane == 0, 0.0, pltpu.roll(field, 1, 1)),
                    jnp.where(lane == nz - 1, 0.0, pltpu.roll(field, nz - 1, 1)))

        advect = total = None
        for axis_no in range(3):
            low, high = pair(1 + k, axis_no)
            term = centre[axis_no] * (high - low)
            both = high + low
            advect = term if advect is None else advect + term
            total = both if total is None else total + both
        low, high = pair(0, k)
        forces = (viscosity * (total - 6.0 * centre[k])
                  - 0.5 * (advect + (high - low)))
        if k == 2:
            forces = forces + force
        value = ustar[k, x] + time_step * forces
        ustar[k, x] = value * inv[x]
        return value

    def upward_body(i, flow):
        for x in (1 + 2 * i, 2 + 2 * i):
            flow = flow + weight[x] * stencil(x, 2)
        return flow

    flow = lax.fori_loop(0, (nx - 2) // 2, upward_body, zero, unroll=3)

    start(x1_rest, not_high_x, not_low_x)
    start(y1_rest, not_high_y, not_low_y)

    low, high = pack_z(1, lambda f, x: vp[0, x])
    vzpack[0] = low
    vzpack[1] = high
    zv[0].start()
    pl.when(not_first)(zv[1].start)

    def along_y_coefficients(side, sign):
        w = weight[:, 0 if side == 0 else ny - 1, :]
        return w * (time_step * viscosity + (sign * 0.5 * time_step) * ypack[side, 2])

    cy_low, cy_high = along_y_coefficients(0, 1.0), along_y_coefficients(1, -1.0)

    def fold(value):
        value = jnp.sum(value, axis=0, keepdims=True)
        return value + pltpu.roll(value, nz // 2, 1)

    line = lax.broadcasted_iota(jnp.int32, (1, nz), 1)
    void_line = fold(lax.fori_loop(0, nx, lambda x, total: total + vp[0, x], zero, unroll=8))

    def across_body(i, carry):
        for x in (1 + 2 * i, 2 + 2 * i):
            stencil(x, 0)
            stencil(x, 1)
        return carry

    lax.fori_loop(0, (nx - 2) // 2, across_body, 0, unroll=3)
    @pl.when(z_first)
    def _():
        pl.semaphore_wait(ready.at[3], 1)
        z1[1].start()
        zv[1].start()

    def sum_copy(which, src, dst, device):
        return pltpu.make_async_remote_copy(
            src, dst, sum_send.at[which], sum_recv.at[which], device_id=device, device_id_type=MESH)

    def all_in(which):
        _, count, _, me = members(which)

        @pl.when(me < count - 1)
        def _():
            pl.semaphore_wait(ready.at[4 + which], 1)

    def send_sums(which, first, last):
        axes, count, base, me = members(which)
        mine = slots.at[base + me]
        for k in range(first, min(last, count - 1)):
            other = jnp.where(k < me, k, k + 1)
            sum_copy(which, mine, mine, ring_device(axes, other)).start()

    def send_sum(which, value, last):
        _, _, base, me = members(which)
        slots[base + me] = value
        send_sums(which, 0, last)

    def all_sums(which):
        axes, count, base, me = members(which)
        others = slots.at[pl.ds(base, count - 1)]
        return sum_copy(which, others, others, ring_device(axes, lax.rem(me + 1, count)))

    def recv_sum(which):
        axes, count, base, me = members(which)
        all_sums(which).wait_recv()
        return jnp.sum(slots[pl.ds(base, count)], axis=0)

    finish_x(blk.at[3, pl.ds(0, 2)], blk.at[3, 0], 0)
    flow = flow + weight[0] * stencil(0, 2) + weight[nx - 1] * stencil(nx - 1, 2)
    acc[...] = flow
    finish_y(yhalo.at[:, 3], yhalo.at[0, 3], 2)
    y_line = jnp.sum(cy_low * yhalo[0, 3] + cy_high * yhalo[1, 3], axis=0, keepdims=True)
    def across_edges():
        finish_x(blk.at[rest, pl.ds(0, 2)], blk.at[rest, 0], 1)
        for x in (0, nx - 1):
            stencil(x, 0)
            stencil(x, 1)

    pl.when(z_first)(across_edges)
    z1[0].wait_recv()
    acc[...] += c_low * zhalo[0]

    @pl.when(z_first)
    def _():
        face = pltpu.roll(zpack[0], nz - 1, 1)
        edge[...] = ((time_step * viscosity - (0.5 * time_step) * zhalo[0]) * face
                     - (0.5 * time_step) * pltpu.roll(face, 3 * nx, 1))

    @pl.when(jnp.logical_not(z_last))
    def _():
        z1[1].wait_recv()
        acc[...] += c_high * zhalo[1]

    devices = gx * gy * gz

    def sum_up(last=devices):
        flow_line = jnp.sum(acc[...], axis=0, keepdims=True) + y_line
        flow_line = flow_line + pltpu.roll(flow_line, nz // 2, 1)
        send_sum(0, jnp.where(line < nz // 2, flow_line, void_line), last)

    for which in range(len(phases)):
        all_in(which)
    pl.when(jnp.logical_not(z_first))(sum_up)

    first_row = row == 0
    last_row = row == ny - 1
    first_lane = lane == 0
    last_lane = lane == nz - 1
    row_sign = jnp.where(first_row, 1.0, jnp.where(last_row, -1.0, 0.0))
    lane_sign = jnp.where(first_lane, 1.0, jnp.where(last_lane, -1.0, 0.0))
    row_sign, lane_sign = (s * (0.5 * time_step) for s in (row_sign, lane_sign))
    row_visc, lane_visc = (jnp.abs(s) * (2.0 * viscosity) for s in (row_sign, lane_sign))

    def unpack(which, at):
        return pltpu.roll(which, lax.rem(2 * nz - at, nz), 1)

    def rows(f, x):
        return jnp.where(
            row < ny // 2,
            jnp.broadcast_to(yhalo[0, f, pl.ds(x, 1), :], (ny, nz)),
            jnp.broadcast_to(yhalo[1, f, pl.ds(x, 1), :], (ny, nz)))

    def correct(x, which, components, with_rows=True):
        by_row = row_visc + row_sign * blk[2, x + 1]
        by_lane = lane_visc + lane_sign * blk[3, x + 1]
        inverse, v = inv[x], vp[0, x]
        for k in components:
            value = by_lane * unpack(which, (1 + k) * nx + x)
            if with_rows:
                value = value + by_row * rows(1 + k, x)
            if k == 1:
                value = value + row_sign * rows(0, x)
            if k == 2:
                value = value + lane_sign * unpack(which, x)
            value = ustar[k, x] + value * inverse
            ustar[k, x] = value
            flux[k, x] = v * value

    def correct_all(pair, components, with_rows=True):
        def body(i, carry):
            correct(2 * i, pair[0], components, with_rows)
            correct(2 * i + 1, pair[1], components, with_rows)
            return carry

        lax.fori_loop(0, nx // 2, body, 0, unroll=4)

    x2 = exchange(flux.at[0, 0], flux.at[0, nx - 1], fxhalo.at[0], fxhalo.at[1], 0, (8,), "gx", up_x, down_x)
    y2 = exchange(ypack.at[0, 4], ypack.at[1, 4], fyhalo.at[0], fyhalo.at[1], 1, (9,), "gy", up_y, down_y)
    z2 = exchange(fzpack.at[0], fzpack.at[1], fzhalo.at[0], fzhalo.at[1], 2, (10,), "gz", z_up, z_down)

    def send_flux_z():
        low, high = pack_z(1, lambda f, x: flux[2, x])
        fzpack[0] = low
        fzpack[1] = high
        for copy in z2:
            copy.start()

    z_low = pltpu.roll(zhalo[0], 1, 1)
    @pl.when(z_first)
    def _():
        zc.wait_recv()
    @pl.when(z_first)
    def _():
        product = whalo[...] * edge[...]
        acc[...] += product
        sum_up(plane - 1)
        edge[...] = jnp.where(lane < nx, pltpu.roll(product, nz - 3 * nx + 1, 1), 0.0)

    @pl.when(z_last)
    def _():
        correct_all(interleave(z_low, zero), (2,))
        send_flux_z()

    pl.when(z_last)(z1[1].wait_recv)
    z_high = pltpu.roll(zhalo[1], nz - 1, 1)
    joined = interleave(z_low, z_high)
    pl.when(not_first)(across_edges)
    finish_y(yhalo.at[:, rest], yhalo.at[0, rest], 3)
    correct_all(joined, (0, 1))
    ypack[0, 4] = flux[1, :, 0, :]
    ypack[1, 4] = flux[1, :, ny - 1, :]
    start(y2, not_high_y, not_low_y)
    start(x2, not_high_x, not_low_x)

    pl.when(z_first)(lambda: send_sums(0, plane - 1, devices))
    @pl.when(not_first)
    def _():
        edge[...] = zero

    @pl.when(z_last)
    def _():
        correct_all(interleave(zero, z_high), (2,), False)

    @pl.when(not_last)
    def _():
        correct_all(joined, (2,))
        send_flux_z()

    for within, side in ((not_low_x, 0), (not_high_x, 1)):
        @pl.when(jnp.logical_not(within))
        def _():
            fxhalo[side] = zero
    for within, side in ((not_low_y, 0), (not_high_y, 1)):
        @pl.when(jnp.logical_not(within))
        def _():
            fyhalo[side] = jnp.zeros((nx, nz), jnp.float32)

    copy_to(vzpack, vzhalo, 2, 6, "gz", z_up).wait_recv()
    v_joined = interleave(pltpu.roll(vzhalo[0], 1, 1), pltpu.roll(vzhalo[1], nz - 1, 1))

    def source_plane(x, odd, x_low, x_high):
        fy, fz, v = flux[1, x], flux[2, x], vp[0, x]
        y_low = jnp.where(first_row, 0.0, pltpu.roll(fy, 1, 0))
        y_high = jnp.where(last_row, 0.0, pltpu.roll(fy, ny - 1, 0))
        z_low = jnp.where(first_lane, 0.0, pltpu.roll(fz, 1, 1))
        z_high = jnp.where(last_lane, 0.0, pltpu.roll(fz, nz - 1, 1))
        v_halo = unpack(v_joined[odd], x)
        v_low = jnp.where(first_lane, v_halo, pltpu.roll(v, 1, 1))
        v_high = jnp.where(last_lane, v_halo, pltpu.roll(v, nz - 1, 1))
        div[x] = 0.5 * ((x_high - x_low) + (y_high - y_low) + (z_high - z_low))
        slope[x] = (0.5 * time_step) * (v_high - v_low)

    def source_body(i, carry):
        x = 2 * i + 1
        source_plane(x, 1, flux[0, x - 1], flux[0, x + 1])
        source_plane(x + 1, 0, flux[0, x], flux[0, x + 2])
        return carry

    lax.fori_loop(0, nx // 2 - 1, source_body, 0, unroll=3)
    phase = 0
    while phase < len(phases) - 1:
        total = recv_sum(phase)
        phase += 1
        send_sum(phase, total, devices)
    finish_x(fxhalo, fxhalo.at[0], 8)
    source_plane(0, 0, fxhalo[0], flux[0, 1])
    source_plane(nx - 1, 1, flux[0, nx - 2], fxhalo[1])
    finish_y(fyhalo, fyhalo.at[0], 9)
    copy_to(fzpack, fzhalo, 2, 10, "gz", z_up).wait_recv()
    f_joined = interleave(pltpu.roll(fzhalo[0], 1, 1) + edge[...], pltpu.roll(fzhalo[1], nz - 1, 1))
    row_half, lane_half = row_sign / time_step, lane_sign / time_step

    def edge_plane(x, odd):
        y_halo = jnp.where(
            row < ny // 2,
            jnp.broadcast_to(fyhalo[0, pl.ds(x, 1), :], (ny, nz)),
            jnp.broadcast_to(fyhalo[1, pl.ds(x, 1), :], (ny, nz)))
        div[x] = div[x] - row_half * y_halo - lane_half * unpack(f_joined[odd], x)

    def edge_body(i, carry):
        edge_plane(2 * i, 0)
        edge_plane(2 * i + 1, 1)
        return carry

    lax.fori_loop(0, nx // 2, edge_body, 0, unroll=16)

    for which in range(len(phases)):
        all_sums(which).wait_send()
    sent = inv.at[pl.ds(0, 5)]
    settle(inv.at[pl.ds(0, 10)], sent, 0, 0, not_high_x, not_low_x, False)
    settle(ypack, ypack.at[0], 1, 2, not_high_y, not_low_y, False)
    sent = inv.at[pl.ds(0, 6)]
    copy_to(sent, sent, 2, 4, "gz", z_up).wait_send()
    pl.when(z_last)(zc.wait_send)

    total = recv_sum(phase)
    half = line < nz // 2
    flow_sum = jnp.sum(jnp.where(half, total, 0.0), axis=1, keepdims=True)
    void_sum = jnp.sum(jnp.where(half, 0.0, total), axis=1, keepdims=True)
    cells = float(nx * ny * nz * gx * gy * gz)
    step = (target[0] * cells - flow_sum) / (time_step * void_sum)
    lines[0] = jnp.broadcast_to(step, (1, nz)) + force
    lines[1] = jnp.broadcast_to(step, (1, nz))


def shift_kernel(ustar, div, slope, lines, vel_out, source_out, forcing_out, made, sem):
    nx, ny, nz = div.shape
    half = nx // 2
    across, line = pl.ds(0, 2), pltpu.make_async_copy(lines.at[0], forcing_out, sem.at[2])
    for k in range(2):
        for part in range(2):
            planes = pl.ds(part * half, half)
            pltpu.make_async_copy(ustar.at[k, planes], vel_out.at[k, planes], sem.at[0]).start()
    line.start()
    step = jnp.broadcast_to(lines[1], (ny, nz))
    for part in range(2):
        def body(i, carry):
            x = part * half + i
            made[0, x] = ustar[2, x] + time_step * step
            made[1, x] = div[x] + step * slope[x]
            return carry

        lax.fori_loop(0, half, body, 0, unroll=8)
        planes = pl.ds(part * half, half)
        pltpu.make_async_copy(made.at[0, planes], vel_out.at[2, planes], sem.at[1]).start()
        pltpu.make_async_copy(made.at[1, planes], source_out.at[planes], sem.at[1]).start()
    pltpu.make_async_copy(ustar.at[across], vel_out.at[across], sem.at[0]).wait()
    pltpu.make_async_copy(made, vel_out.at[across], sem.at[1]).wait()
    line.wait()


def local(velocity, pressure, voidage, particle_vel, forcing, target_flux):
    nx, ny, nz = voidage.shape
    sizes = tuple(lax.axis_size(a) for a in ("gx", "gy", "gz"))
    if math.prod(sizes) <= DIRECT_LIMIT:
        phases = (("gz", "gy", "gx"),)
    else:
        phases = (("gy", "gx"), ("gz",))
    slot_count = sum(math.prod(lax.axis_size(a) for a in axes) for axes in phases)
    f32 = jnp.float32
    vmem = pl.BlockSpec(memory_space=pltpu.VMEM)
    smem = pl.BlockSpec(memory_space=pltpu.SMEM)
    hbm = pl.BlockSpec(memory_space=pltpu.HBM)
    dma = pltpu.SemaphoreType.DMA
    faces = [pltpu.VMEM((2, ny, nz), f32), pltpu.VMEM((2, ny, nz), f32)]
    face = [pltpu.VMEM((ny, nz), f32)]
    results = pl.pallas_call(
        functools.partial(kernel, sizes, phases),
        out_shape=(
            pltpu.VMEM((3, nx, ny, nz), f32),
            pltpu.VMEM((nx, ny, nz), f32),
            pltpu.VMEM((nx, ny, nz), f32),
            pltpu.VMEM((2, 1, nz), f32),
        ),
        in_specs=[hbm] * 4 + [smem] * 2,
        out_specs=(vmem,) * 4,
        scratch_shapes=[
            pltpu.VMEM((4, nx + 2, ny, nz), f32),
            pltpu.VMEM((4, nx, ny, nz), f32),
            pltpu.VMEM((nx, ny, nz), f32),
            pltpu.VMEM((nx, ny, nz), f32),
            pltpu.VMEM((3, nx, ny, nz), f32),
        ] + face + face + [
            pltpu.VMEM((2, 5, nx, nz), f32),
            pltpu.VMEM((2, 4, nx, nz), f32),
        ] + faces + face + face + faces + [
            pltpu.VMEM((2, nx, nz), f32),
            pltpu.VMEM((2, ny, nz), f32),
        ] + faces + [
            pltpu.VMEM((slot_count, 1, nz), f32),
            dma((2,)), dma((4,)), dma((11,)),
            dma((len(phases),)), dma((len(phases),)),
            pltpu.SemaphoreType.REGULAR((4 + len(phases),)),
        ],
        compiler_params=pltpu.CompilerParams(collective_id=0, has_side_effects=True),
    )(velocity, pressure, voidage, particle_vel, forcing, target_flux)
    vel_new, source, forcing_new = pl.pallas_call(
        shift_kernel,
        out_shape=(
            jax.ShapeDtypeStruct((3, nx, ny, nz), f32),
            jax.ShapeDtypeStruct((nx, ny, nz), f32),
            jax.ShapeDtypeStruct((1, nz), f32),
        ),
        in_specs=[vmem] * 4,
        out_specs=(hbm,) * 3,
        scratch_shapes=[
            pltpu.VMEM((2, nx, ny, nz), f32),
            dma((3,)),
        ],
    )(*(pltpu.with_memory_space_constraint(a, pltpu.VMEM) for a in results))
    return vel_new, source, forcing_new[0, :1]


def solution(mesh):
    return jax.shard_map(
        local,
        mesh=mesh,
        in_specs=(
            P(None, "gx", "gy", "gz"),
            P("gx", "gy", "gz"),
            P("gx", "gy", "gz"),
            P(None, "gx", "gy", "gz"),
            P(),
            P(),
        ),
        out_specs=(P(None, "gx", "gy", "gz"), P("gx", "gy", "gz"), P()),
        check_vma=False,
    )
```

```python
import functools
import math

import jax
import jax.numpy as jnp
from jax import lax
from jax.experimental import pallas as pl
from jax.experimental.pallas import tpu as pltpu
from jax.sharding import PartitionSpec as P

time_step = 0.2
viscosity = 0.1
drag_scale = 1.0
MESH = pl.DeviceIdType.MESH
DIRECT_LIMIT = 64
TINY = 1.1754944e-38


def ring_index(axes):
    index = 0
    for axis in axes:
        index = index * lax.axis_size(axis) + lax.axis_index(axis)
    return index


def ring_device(axes, index):
    device = {}
    for axis in reversed(axes):
        size = lax.axis_size(axis)
        device[axis] = lax.rem(index, size)
        index = lax.div(index, size)
    return device


def kernel(
    sizes, phases,
    vel_hbm, pres_hbm, void_hbm, part_hbm, forcing, target,
    ustar, div, slope, lines,
    blk, vp, inv, weight, flux, acc, edge, ypack, yhalo, zpack, zhalo, wpack, whalo,
    vzpack, vzhalo, fyhalo, fxhalo, fzpack, fzhalo, slots,
    load_sem, send, recv, sum_send, sum_recv, ready,
):
    gx, gy, gz = sizes
    nx, ny, nz = div.shape
    x_at, y_at, z_at = (lax.axis_index(a) for a in ("gx", "gy", "gz"))
    not_low_x, not_high_x = x_at > 0, x_at < gx - 1
    not_low_y, not_high_y = y_at > 0, y_at < gy - 1
    z_up, z_down = lax.rem(z_at + 1, gz), lax.rem(z_at + gz - 1, gz)
    z_first, z_last = z_at == 0, z_at == gz - 1
    not_first, not_last = z_at > 0, z_at < gz - 1

    def signal(sem, device):
        pl.semaphore_signal(sem, inc=1, device_id=device, device_id_type=MESH)

    def members(which):
        axes = phases[which]
        count = math.prod(lax.axis_size(a) for a in axes)
        base = sum(math.prod(lax.axis_size(a) for a in phases[w]) for w in range(which))
        return axes, count, base, ring_index(axes)

    plane = gx * gy
    direct = len(phases) == 1
    if direct:
        near = ((1, gx, plane, plane * (gz - 1)),)
    else:
        near = ((1, gx), (1, gz - 1))
    barrier = pltpu.get_barrier_semaphore()
    pl.when(not_high_x)(lambda: signal(barrier, {"gx": x_at + 1}))
    pl.when(not_high_y)(lambda: signal(barrier, {"gy": y_at + 1}))
    pl.when(not_last)(lambda: signal(barrier, {"gz": z_at + 1}))
    pl.when(z_first)(lambda: signal(barrier, {"gz": gz - 1}))
    lower = sum(jnp.where(c, 1, 0) for c in (not_low_x, not_low_y, not_first, z_last))
    for which in range(len(phases)):
        axes, count, _, me = members(which)
        far = me < count - 1
        for d in near[which]:
            far = far & (me != count - 1 - d)
        pl.when(far)(lambda: signal(barrier, ring_device(axes, count - 1)))
        lower = lower + jnp.where(me == count - 1, count - 1 - len(near[which]), 0)

    inside = pl.ds(1, nx)
    for load in (
        pltpu.make_async_copy(vel_hbm, blk.at[pl.ds(1, 3), inside], load_sem.at[0]),
        pltpu.make_async_copy(pres_hbm, blk.at[0, inside], load_sem.at[0]),
        pltpu.make_async_copy(void_hbm, vp.at[0], load_sem.at[1]),
        pltpu.make_async_copy(part_hbm, vp.at[pl.ds(1, 3)], load_sem.at[1]),
    ):
        load.start()

    lane = lax.broadcasted_iota(jnp.int32, (ny, nz), 1)
    row = lax.broadcasted_iota(jnp.int32, (ny, nz), 0)
    zero = jnp.zeros((ny, nz), jnp.float32)

    even = lax.rem(lane, 2) == 0
    pairs = (lax.div(lax.rem(lane + 1, nz), 2), lax.div(lane, 2))

    def interleave(low, high):
        return jnp.where(even, low, high), jnp.where(even, high, low)

    def pack_z(fields, read, at=0):
        tiles = []
        for odd in range(2):
            total = None
            for f in range(fields):
                tile = zero
                for x in range(odd, nx, 2):
                    turned = read(f, x)
                    to = (at + f * nx + x) % nz
                    if to:
                        turned = pltpu.roll(turned, to, 1)
                    tile = jnp.where(pairs[odd] == to // 2, turned, tile)
                total = tile if total is None else total + tile
            tiles.append(total)
        return interleave(*tiles)

    def copy_to(src, dst, send_at, recv_at, axis, device):
        return pltpu.make_async_remote_copy(
            src, dst, send.at[send_at], recv.at[recv_at],
            device_id={axis: device}, device_id_type=MESH)

    def exchange(low, high, dst_low, dst_high, send_at, recvs, axis, up, down):
        return (copy_to(high, dst_low, send_at, recvs[0], axis, up),
                copy_to(low, dst_high, send_at, recvs[-1], axis, down))

    def start(pair, high, low):
        pl.when(high)(pair[0].start)
        pl.when(low)(pair[1].start)

    def settle(both, one, send_at, recv_at, high, low, received):
        def wait(ref):
            copy = copy_to(ref, ref, send_at, recv_at, "gz", z_up)
            return copy.wait_recv if received else copy.wait_send

        pl.when(high & low)(wait(both))
        pl.when(high ^ low)(wait(one))

    def finish_x(both, one, recv_at):
        settle(both, one, 0, recv_at, not_high_x, not_low_x, True)

    def finish_y(both, one, recv_at):
        settle(both, one, 1, recv_at, not_high_y, not_low_y, True)

    up_x, down_x = jnp.minimum(x_at + 1, gx - 1), jnp.maximum(x_at - 1, 0)
    up_y, down_y = jnp.minimum(y_at + 1, gy - 1), jnp.maximum(y_at - 1, 0)
    rest = pl.ds(0, 3)

    def along_x(fields, recvs):
        return exchange(blk.at[fields, 1], blk.at[fields, nx], blk.at[fields, 0], blk.at[fields, nx + 1],
                        0, recvs, "gx", up_x, down_x)

    def along_y(fields, recvs):
        return exchange(ypack.at[0, fields], ypack.at[1, fields], yhalo.at[0, fields], yhalo.at[1, fields],
                        1, recvs, "gy", up_y, down_y)

    x1, x1_rest = along_x(3, (0,)), along_x(rest, (1,))
    y1, y1_rest = along_y(3, (2,)), along_y(rest, (3,))
    z1 = exchange(zpack.at[0], zpack.at[1], zhalo.at[0], zhalo.at[1], 2, (4, 5), "gz", z_up, z_down)
    zv = exchange(vzpack.at[0], vzpack.at[1], vzhalo.at[0], vzhalo.at[1], 2, (6,), "gz", z_up, z_down)
    zc = copy_to(wpack, whalo, 3, 7, "gz", z_up)

    pl.when(lower > 0)(lambda: pl.semaphore_wait(barrier, lower))
    pl.when(not_low_y)(lambda: signal(ready.at[1], {"gy": down_y}))
    pl.when(not_low_x)(lambda: signal(ready.at[0], {"gx": down_x}))
    pl.when(not_first)(lambda: signal(ready.at[2], {"gz": z_down}))
    pl.when(z_last)(lambda: signal(ready.at[3], {"gz": z_up}))
    for which in range(len(phases)):
        axes, count, _, me = members(which)

        @pl.when(me == count - 1)
        def _():
            for k in range(count - 1):
                signal(ready.at[4 + which], ring_device(axes, k))
    pltpu.make_async_copy(blk.at[:, inside], blk.at[:, inside], load_sem.at[0]).wait()
    for side, y in ((0, 0), (1, ny - 1)):
        ypack[side, 3] = blk[3, inside, y, :]
    pl.when(not_low_y)(y1[1].start)
    pl.when(not_low_x)(x1[1].start)
    low, high = pack_z(4, lambda f, x: blk[f, x + 1])
    zpack[0] = low
    zpack[1] = high
    pl.when(z_last)(z1[0].start)
    pl.when(not_first)(z1[1].start)
    pltpu.make_async_copy(vp, vp, load_sem.at[1]).wait()
    force = forcing[0]

    def drag_plane(x):
        v = vp[0, x]
        c = [blk[1 + k, x + 1] for k in range(3)]
        q = [vp[1 + k, x] for k in range(3)]
        square = sum((c[k] - q[k]) ** 2 for k in range(3))
        slip = square * lax.rsqrt(jnp.maximum(square, TINY))
        drag = drag_scale * (1.0 - v) * jnp.exp(-2.65 * jnp.log(v)) * (1.0 + slip)
        step_drag = time_step * drag
        inverse = 1.0 / (1.0 + step_drag)
        w = v * inverse
        inv[x] = inverse
        weight[x] = w
        for k in range(3):
            ustar[k, x] = c[k] + step_drag * q[k]
        return w

    weights = [drag_plane(x) for x in range(nx)]
    w_low, w_high = pack_z(1, lambda f, x: weights[x], 3 * nx)
    wpack[...] = w_high
    pl.when(z_last)(zc.start)

    for higher, which, copy in ((not_high_x, 0, x1[0]), (not_high_y, 1, y1[0]), (not_last, 2, z1[0])):
        @pl.when(higher)
        def _():
            pl.semaphore_wait(ready.at[which], 1)
            copy.start()
    def coefficients(face, w, sign, at):
        upward = w * (time_step * viscosity + (sign * 0.5 * time_step) * face)
        pressed = (sign * 0.5 * time_step) * pltpu.roll(w, nz - 3 * nx, 1)
        return jnp.where(at < nx, pressed,
                         jnp.where((at >= 3 * nx) & (at < 4 * nx), upward, 0.0))

    c_low = pltpu.roll(coefficients(zpack[0], w_low, 1.0, lane), nz - 1, 1)
    c_high = pltpu.roll(coefficients(zpack[1], w_high, -1.0, lax.rem(lane + 1, nz)), 1, 1)
    for f in range(3):
        ypack[0, f] = blk[f, inside, 0, :]
        ypack[1, f] = blk[f, inside, ny - 1, :]
    def wall_x(within, halo_plane, edge_plane):
        @pl.when(jnp.logical_not(within))
        def _():
            for f in range(1, 4):
                blk[f, halo_plane] = zero
            blk[0, halo_plane] = blk[0, edge_plane]

    wall_x(not_low_x, 0, 1)
    wall_x(not_high_x, nx + 1, nx)

    def wall_y(within, side):
        @pl.when(jnp.logical_not(within))
        def _():
            for f in range(1, 4):
                yhalo[side, f] = jnp.zeros((nx, nz), jnp.float32)
            yhalo[side, 0] = ypack[side, 0]

    wall_y(not_low_y, 0)
    wall_y(not_high_y, 1)

    def stencil(x, k):
        p = x + 1
        centre = [blk[1 + f, p] for f in range(3)]

        def pair(f, axis_no):
            if axis_no == 0:
                return blk[f, p - 1], blk[f, p + 1]
            field = blk[f, p]
            if axis_no == 1:
                return (jnp.where(row == 0, 0.0, pltpu.roll(field, 1, 0)),
                        jnp.where(row == ny - 1, 0.0, pltpu.roll(field, ny - 1, 0)))
            return (jnp.where(lane == 0, 0.0, pltpu.roll(field, 1, 1)),
                    jnp.where(lane == nz - 1, 0.0, pltpu.roll(field, nz - 1, 1)))

        advect = total = None
        for axis_no in range(3):
            low, high = pair(1 + k, axis_no)
            term = centre[axis_no] * (high - low)
            both = high + low
            advect = term if advect is None else advect + term
            total = both if total is None else total + both
        low, high = pair(0, k)
        forces = (viscosity * (total - 6.0 * centre[k])
                  - 0.5 * (advect + (high - low)))
        if k == 2:
            forces = forces + force
        value = ustar[k, x] + time_step * forces
        ustar[k, x] = value * inv[x]
        return value

    def upward_body(i, flow):
        for x in (1 + 2 * i, 2 + 2 * i):
            flow = flow + weight[x] * stencil(x, 2)
        return flow

    flow = lax.fori_loop(0, (nx - 2) // 2, upward_body, zero, unroll=3)

    start(x1_rest, not_high_x, not_low_x)
    start(y1_rest, not_high_y, not_low_y)

    low, high = pack_z(1, lambda f, x: vp[0, x])
    vzpack[0] = low
    vzpack[1] = high
    zv[0].start()
    pl.when(not_first)(zv[1].start)

    def along_y_coefficients(side, sign):
        w = weight[:, 0 if side == 0 else ny - 1, :]
        return w * (time_step * viscosity + (sign * 0.5 * time_step) * ypack[side, 2])

    cy_low, cy_high = along_y_coefficients(0, 1.0), along_y_coefficients(1, -1.0)

    void_total = lax.fori_loop(0, nx, lambda x, total: total + vp[0, x], zero, unroll=8)
    void_line = jnp.sum(void_total, axis=0, keepdims=True)

    def across_body(i, carry):
        for x in (1 + 2 * i, 2 + 2 * i):
            stencil(x, 0)
            stencil(x, 1)
        return carry

    lax.fori_loop(0, (nx - 2) // 2, across_body, 0, unroll=3)
    @pl.when(z_first)
    def _():
        pl.semaphore_wait(ready.at[3], 1)
        z1[1].start()
        zv[1].start()

    def sum_copy(which, src, dst, device):
        return pltpu.make_async_remote_copy(
            src, dst, sum_send.at[which], sum_recv.at[which], device_id=device, device_id_type=MESH)

    def all_in(which):
        _, count, _, me = members(which)

        @pl.when(me < count - 1)
        def _():
            pl.semaphore_wait(ready.at[4 + which], 1)

    def send_sums(which, first, last):
        axes, count, base, me = members(which)
        mine = slots.at[base + me]
        for k in range(first, min(last, count - 1)):
            other = jnp.where(k < me, k, k + 1)
            sum_copy(which, mine, mine, ring_device(axes, other)).start()

    def send_sum(which, value, last):
        _, _, base, me = members(which)
        for at in range(2):
            slots[base + me, at] = value[at][0]
        send_sums(which, 0, last)

    def all_sums(which):
        axes, count, base, me = members(which)
        others = slots.at[pl.ds(base, count - 1)]
        return sum_copy(which, others, others, ring_device(axes, lax.rem(me + 1, count)))

    def recv_sum(which):
        axes, count, base, me = members(which)
        all_sums(which).wait_recv()
        return [jnp.sum(slots[pl.ds(base, count), at], axis=0, keepdims=True) for at in range(2)]

    finish_x(blk.at[3, pl.ds(0, 2)], blk.at[3, 0], 0)
    flow = flow + weight[0] * stencil(0, 2) + weight[nx - 1] * stencil(nx - 1, 2)
    acc[...] = flow
    finish_y(yhalo.at[:, 3], yhalo.at[0, 3], 2)
    y_line = jnp.sum(cy_low * yhalo[0, 3] + cy_high * yhalo[1, 3], axis=0, keepdims=True)
    def across_edges():
        finish_x(blk.at[rest, pl.ds(0, 2)], blk.at[rest, 0], 1)
        for x in (0, nx - 1):
            stencil(x, 0)
            stencil(x, 1)

    pl.when(z_first)(across_edges)
    z1[0].wait_recv()
    acc[...] += c_low * zhalo[0]

    @pl.when(z_first)
    def _():
        face = pltpu.roll(zpack[0], nz - 1, 1)
        edge[...] = ((time_step * viscosity - (0.5 * time_step) * zhalo[0]) * face
                     - (0.5 * time_step) * pltpu.roll(face, 3 * nx, 1))

    @pl.when(jnp.logical_not(z_last))
    def _():
        z1[1].wait_recv()
        acc[...] += c_high * zhalo[1]

    devices = gx * gy * gz

    def sum_up(last=devices):
        send_sum(0, (jnp.sum(acc[...], axis=0, keepdims=True) + y_line, void_line), last)

    for which in range(len(phases)):
        all_in(which)
    pl.when(jnp.logical_not(z_first))(sum_up)

    first_row = row == 0
    last_row = row == ny - 1
    first_lane = lane == 0
    last_lane = lane == nz - 1
    row_sign = jnp.where(first_row, 1.0, jnp.where(last_row, -1.0, 0.0))
    lane_sign = jnp.where(first_lane, 1.0, jnp.where(last_lane, -1.0, 0.0))
    row_sign, lane_sign = (s * (0.5 * time_step) for s in (row_sign, lane_sign))
    row_visc, lane_visc = (jnp.abs(s) * (2.0 * viscosity) for s in (row_sign, lane_sign))

    def unpack(which, at):
        return pltpu.roll(which, lax.rem(2 * nz - at, nz), 1)

    def rows(f, x):
        return jnp.where(
            row < ny // 2,
            jnp.broadcast_to(yhalo[0, f, pl.ds(x, 1), :], (ny, nz)),
            jnp.broadcast_to(yhalo[1, f, pl.ds(x, 1), :], (ny, nz)))

    def correct(x, which, components, with_rows=True):
        by_row = row_visc + row_sign * blk[2, x + 1]
        by_lane = lane_visc + lane_sign * blk[3, x + 1]
        inverse, v = inv[x], vp[0, x]
        for k in components:
            value = by_lane * unpack(which, (1 + k) * nx + x)
            if with_rows:
                value = value + by_row * rows(1 + k, x)
            if k == 1:
                value = value + row_sign * rows(0, x)
            if k == 2:
                value = value + lane_sign * unpack(which, x)
            value = ustar[k, x] + value * inverse
            ustar[k, x] = value
            flux[k, x] = v * value

    def correct_all(pair, components, with_rows=True):
        def body(i, carry):
            correct(2 * i, pair[0], components, with_rows)
            correct(2 * i + 1, pair[1], components, with_rows)
            return carry

        lax.fori_loop(0, nx // 2, body, 0, unroll=8)

    x2 = exchange(flux.at[0, 0], flux.at[0, nx - 1], fxhalo.at[0], fxhalo.at[1], 0, (8,), "gx", up_x, down_x)
    y2 = exchange(ypack.at[0, 4], ypack.at[1, 4], fyhalo.at[0], fyhalo.at[1], 1, (9,), "gy", up_y, down_y)
    z2 = exchange(fzpack.at[0], fzpack.at[1], fzhalo.at[0], fzhalo.at[1], 2, (10,), "gz", z_up, z_down)

    def send_flux_z():
        low, high = pack_z(1, lambda f, x: flux[2, x])
        fzpack[0] = low
        fzpack[1] = high
        for copy in z2:
            copy.start()

    z_low = pltpu.roll(zhalo[0], 1, 1)
    @pl.when(z_first)
    def _():
        zc.wait_recv()
    @pl.when(z_first)
    def _():
        product = whalo[...] * edge[...]
        acc[...] += product
        sum_up(plane - 1)
        edge[...] = jnp.where(lane < nx, pltpu.roll(product, nz - 3 * nx + 1, 1), 0.0)

    @pl.when(z_last)
    def _():
        correct_all(interleave(z_low, zero), (2,))
        send_flux_z()

    pl.when(z_last)(z1[1].wait_recv)
    z_high = pltpu.roll(zhalo[1], nz - 1, 1)
    joined = interleave(z_low, z_high)
    pl.when(not_first)(across_edges)
    finish_y(yhalo.at[:, rest], yhalo.at[0, rest], 3)
    correct_all(joined, (0, 1))
    ypack[0, 4] = flux[1, :, 0, :]
    ypack[1, 4] = flux[1, :, ny - 1, :]
    start(y2, not_high_y, not_low_y)
    start(x2, not_high_x, not_low_x)

    pl.when(z_first)(lambda: send_sums(0, plane - 1, devices))
    @pl.when(not_first)
    def _():
        edge[...] = zero

    @pl.when(z_last)
    def _():
        correct_all(interleave(zero, z_high), (2,), False)

    @pl.when(not_last)
    def _():
        correct_all(joined, (2,))
        send_flux_z()

    for within, side in ((not_low_x, 0), (not_high_x, 1)):
        @pl.when(jnp.logical_not(within))
        def _():
            fxhalo[side] = zero
    for within, side in ((not_low_y, 0), (not_high_y, 1)):
        @pl.when(jnp.logical_not(within))
        def _():
            fyhalo[side] = jnp.zeros((nx, nz), jnp.float32)

    copy_to(vzpack, vzhalo, 2, 6, "gz", z_up).wait_recv()
    v_joined = interleave(pltpu.roll(vzhalo[0], 1, 1), pltpu.roll(vzhalo[1], nz - 1, 1))

    def source_plane(x, odd, x_low, x_high):
        fy, fz, v = flux[1, x], flux[2, x], vp[0, x]
        y_low = jnp.where(first_row, 0.0, pltpu.roll(fy, 1, 0))
        y_high = jnp.where(last_row, 0.0, pltpu.roll(fy, ny - 1, 0))
        z_low = jnp.where(first_lane, 0.0, pltpu.roll(fz, 1, 1))
        z_high = jnp.where(last_lane, 0.0, pltpu.roll(fz, nz - 1, 1))
        v_halo = unpack(v_joined[odd], x)
        v_low = jnp.where(first_lane, v_halo, pltpu.roll(v, 1, 1))
        v_high = jnp.where(last_lane, v_halo, pltpu.roll(v, nz - 1, 1))
        div[x] = 0.5 * ((x_high - x_low) + (y_high - y_low) + (z_high - z_low))
        slope[x] = (0.5 * time_step) * (v_high - v_low)

    def source_body(i, carry):
        x = 2 * i + 1
        source_plane(x, 1, flux[0, x - 1], flux[0, x + 1])
        source_plane(x + 1, 0, flux[0, x], flux[0, x + 2])
        return carry

    lax.fori_loop(0, nx // 2 - 1, source_body, 0, unroll=3)
    phase = 0
    while phase < len(phases) - 1:
        total = recv_sum(phase)
        phase += 1
        send_sum(phase, total, devices)
    finish_x(fxhalo, fxhalo.at[0], 8)
    source_plane(0, 0, fxhalo[0], flux[0, 1])
    source_plane(nx - 1, 1, flux[0, nx - 2], fxhalo[1])
    finish_y(fyhalo, fyhalo.at[0], 9)
    copy_to(fzpack, fzhalo, 2, 10, "gz", z_up).wait_recv()
    f_joined = interleave(pltpu.roll(fzhalo[0], 1, 1) + edge[...], pltpu.roll(fzhalo[1], nz - 1, 1))
    row_half, lane_half = row_sign / time_step, lane_sign / time_step

    def edge_plane(x, odd):
        y_halo = jnp.where(
            row < ny // 2,
            jnp.broadcast_to(fyhalo[0, pl.ds(x, 1), :], (ny, nz)),
            jnp.broadcast_to(fyhalo[1, pl.ds(x, 1), :], (ny, nz)))
        div[x] = div[x] - row_half * y_halo - lane_half * unpack(f_joined[odd], x)

    def edge_body(i, carry):
        edge_plane(2 * i, 0)
        edge_plane(2 * i + 1, 1)
        return carry

    lax.fori_loop(0, nx // 2, edge_body, 0, unroll=16)

    for which in range(len(phases)):
        all_sums(which).wait_send()
    sent = inv.at[pl.ds(0, 5)]
    settle(inv.at[pl.ds(0, 10)], sent, 0, 0, not_high_x, not_low_x, False)
    settle(ypack, ypack.at[0], 1, 2, not_high_y, not_low_y, False)
    sent = inv.at[pl.ds(0, 6)]
    copy_to(sent, sent, 2, 4, "gz", z_up).wait_send()
    pl.when(z_last)(zc.wait_send)

    total = recv_sum(phase)
    flow_sum, void_sum = (jnp.sum(t, axis=1, keepdims=True) for t in total)
    cells = float(nx * ny * nz * gx * gy * gz)
    step = (target[0] * cells - flow_sum) / (time_step * void_sum)
    lines[0] = jnp.broadcast_to(step, (1, nz)) + force
    lines[1] = jnp.broadcast_to(step, (1, nz))


def shift_kernel(ustar, div, slope, lines, vel_out, source_out, forcing_out, made, sem):
    nx, ny, nz = div.shape
    half = nx // 2
    across, line = pl.ds(0, 2), pltpu.make_async_copy(lines.at[0], forcing_out, sem.at[2])
    for k in range(2):
        for part in range(2):
            planes = pl.ds(part * half, half)
            pltpu.make_async_copy(ustar.at[k, planes], vel_out.at[k, planes], sem.at[0]).start()
    line.start()
    step = jnp.broadcast_to(lines[1], (ny, nz))
    for part in range(2):
        def body(i, carry):
            x = part * half + i
            made[0, x] = ustar[2, x] + time_step * step
            made[1, x] = div[x] + step * slope[x]
            return carry

        lax.fori_loop(0, half, body, 0, unroll=8)
        planes = pl.ds(part * half, half)
        pltpu.make_async_copy(made.at[0, planes], vel_out.at[2, planes], sem.at[1]).start()
        pltpu.make_async_copy(made.at[1, planes], source_out.at[planes], sem.at[1]).start()
    pltpu.make_async_copy(ustar.at[across], vel_out.at[across], sem.at[0]).wait()
    pltpu.make_async_copy(made, vel_out.at[across], sem.at[1]).wait()
    line.wait()


def local(velocity, pressure, voidage, particle_vel, forcing, target_flux):
    nx, ny, nz = voidage.shape
    sizes = tuple(lax.axis_size(a) for a in ("gx", "gy", "gz"))
    if math.prod(sizes) <= DIRECT_LIMIT:
        phases = (("gz", "gy", "gx"),)
    else:
        phases = (("gy", "gx"), ("gz",))
    slot_count = sum(math.prod(lax.axis_size(a) for a in axes) for axes in phases)
    f32 = jnp.float32
    vmem = pl.BlockSpec(memory_space=pltpu.VMEM)
    smem = pl.BlockSpec(memory_space=pltpu.SMEM)
    hbm = pl.BlockSpec(memory_space=pltpu.HBM)
    dma = pltpu.SemaphoreType.DMA
    faces = [pltpu.VMEM((2, ny, nz), f32), pltpu.VMEM((2, ny, nz), f32)]
    face = [pltpu.VMEM((ny, nz), f32)]
    results = pl.pallas_call(
        functools.partial(kernel, sizes, phases),
        out_shape=(
            pltpu.VMEM((3, nx, ny, nz), f32),
            pltpu.VMEM((nx, ny, nz), f32),
            pltpu.VMEM((nx, ny, nz), f32),
            pltpu.VMEM((2, 1, nz), f32),
        ),
        in_specs=[hbm] * 4 + [smem] * 2,
        out_specs=(vmem,) * 4,
        scratch_shapes=[
            pltpu.VMEM((4, nx + 2, ny, nz), f32),
            pltpu.VMEM((4, nx, ny, nz), f32),
            pltpu.VMEM((nx, ny, nz), f32),
            pltpu.VMEM((nx, ny, nz), f32),
            pltpu.VMEM((3, nx, ny, nz), f32),
        ] + face + face + [
            pltpu.VMEM((2, 5, nx, nz), f32),
            pltpu.VMEM((2, 4, nx, nz), f32),
        ] + faces + face + face + faces + [
            pltpu.VMEM((2, nx, nz), f32),
            pltpu.VMEM((2, ny, nz), f32),
        ] + faces + [
            pltpu.VMEM((slot_count, 2, nz), f32),
            dma((2,)), dma((4,)), dma((11,)),
            dma((len(phases),)), dma((len(phases),)),
            pltpu.SemaphoreType.REGULAR((4 + len(phases),)),
        ],
        compiler_params=pltpu.CompilerParams(collective_id=0, has_side_effects=True),
    )(velocity, pressure, voidage, particle_vel, forcing, target_flux)
    vel_new, source, forcing_new = pl.pallas_call(
        shift_kernel,
        out_shape=(
            jax.ShapeDtypeStruct((3, nx, ny, nz), f32),
            jax.ShapeDtypeStruct((nx, ny, nz), f32),
            jax.ShapeDtypeStruct((1, nz), f32),
        ),
        in_specs=[vmem] * 4,
        out_specs=(hbm,) * 3,
        scratch_shapes=[
            pltpu.VMEM((2, nx, ny, nz), f32),
            dma((3,)),
        ],
    )(*(pltpu.with_memory_space_constraint(a, pltpu.VMEM) for a in results))
    return vel_new, source, forcing_new[0, :1]


def solution(mesh):
    return jax.shard_map(
        local,
        mesh=mesh,
        in_specs=(
            P(None, "gx", "gy", "gz"),
            P("gx", "gy", "gz"),
            P("gx", "gy", "gz"),
            P(None, "gx", "gy", "gz"),
            P(),
            P(),
        ),
        out_specs=(P(None, "gx", "gy", "gz"), P("gx", "gy", "gz"), P()),
        check_vma=False,
    )
```

```python
import functools
import math

import jax
import jax.numpy as jnp
from jax import lax
from jax.experimental import pallas as pl
from jax.experimental.pallas import tpu as pltpu
from jax.sharding import PartitionSpec as P

time_step = 0.2
viscosity = 0.1
drag_scale = 1.0
MESH = pl.DeviceIdType.MESH
DIRECT_LIMIT = 64
TINY = 1.1754944e-38


def ring_index(axes):
    index = 0
    for axis in axes:
        index = index * lax.axis_size(axis) + lax.axis_index(axis)
    return index


def ring_device(axes, index):
    device = {}
    for axis in reversed(axes):
        size = lax.axis_size(axis)
        device[axis] = lax.rem(index, size)
        index = lax.div(index, size)
    return device


def kernel(
    sizes, phases,
    vel_hbm, pres_hbm, void_hbm, part_hbm, forcing, target,
    ustar, div, slope, lines,
    blk, vp, inv, weight, flux, acc, edge, ypack, yhalo, zpack, zhalo, wpack, whalo,
    vzpack, vzhalo, fyhalo, fxhalo, fzpack, fzhalo, slots,
    load_sem, send, recv, sum_send, sum_recv, ready,
):
    gx, gy, gz = sizes
    nx, ny, nz = div.shape
    x_at, y_at, z_at = (lax.axis_index(a) for a in ("gx", "gy", "gz"))
    not_low_x, not_high_x = x_at > 0, x_at < gx - 1
    not_low_y, not_high_y = y_at > 0, y_at < gy - 1
    z_up, z_down = lax.rem(z_at + 1, gz), lax.rem(z_at + gz - 1, gz)
    z_first, z_last = z_at == 0, z_at == gz - 1
    not_first, not_last = z_at > 0, z_at < gz - 1

    def signal(sem, device):
        pl.semaphore_signal(sem, inc=1, device_id=device, device_id_type=MESH)

    def members(which):
        axes = phases[which]
        count = math.prod(lax.axis_size(a) for a in axes)
        base = sum(math.prod(lax.axis_size(a) for a in phases[w]) for w in range(which))
        return axes, count, base, ring_index(axes)

    plane = gx * gy
    direct = len(phases) == 1
    if direct:
        near = ((1, gx, plane, plane * (gz - 1)),)
    else:
        near = ((1, gx), (1, gz - 1))
    barrier = pltpu.get_barrier_semaphore()
    peers = jnp.where(z_last, 1, 0)
    for there, axis, at in ((not_high_y, "gy", y_at + 1), (not_last, "gz", z_at + 1), (not_high_x, "gx", x_at + 1),
                            (not_low_y, "gy", y_at - 1), (not_first, "gz", z_at - 1), (not_low_x, "gx", x_at - 1)):
        pl.when(there)(lambda: signal(barrier, {axis: at}))
        peers = peers + jnp.where(there, 1, 0)
    pl.when(z_first)(lambda: signal(barrier, {"gz": gz - 1}))
    for which in range(len(phases)):
        axes, count, _, me = members(which)
        far = me < count - 1
        for d in near[which]:
            far = far & (me != count - 1 - d)
        pl.when(far)(lambda: signal(barrier, ring_device(axes, count - 1)))
        peers = peers + jnp.where(me == count - 1, count - 1 - len(near[which]), 0)

    inside = pl.ds(1, nx)
    for load in (
        pltpu.make_async_copy(vel_hbm, blk.at[pl.ds(1, 3), inside], load_sem.at[0]),
        pltpu.make_async_copy(pres_hbm, blk.at[0, inside], load_sem.at[0]),
        pltpu.make_async_copy(void_hbm, vp.at[0], load_sem.at[1]),
        pltpu.make_async_copy(part_hbm, vp.at[pl.ds(1, 3)], load_sem.at[1]),
    ):
        load.start()

    lane = lax.broadcasted_iota(jnp.int32, (ny, nz), 1)
    row = lax.broadcasted_iota(jnp.int32, (ny, nz), 0)
    zero = jnp.zeros((ny, nz), jnp.float32)

    even = lax.rem(lane, 2) == 0
    pairs = (lax.div(lax.rem(lane + 1, nz), 2), lax.div(lane, 2))

    def interleave(low, high):
        return jnp.where(even, low, high), jnp.where(even, high, low)

    def pack_z(fields, read, at=0):
        tiles = []
        for odd in range(2):
            total = None
            for f in range(fields):
                tile = zero
                for x in range(odd, nx, 2):
                    turned = read(f, x)
                    to = (at + f * nx + x) % nz
                    if to:
                        turned = pltpu.roll(turned, to, 1)
                    tile = jnp.where(pairs[odd] == to // 2, turned, tile)
                total = tile if total is None else total + tile
            tiles.append(total)
        return interleave(*tiles)

    def copy_to(src, dst, send_at, recv_at, axis, device):
        return pltpu.make_async_remote_copy(
            src, dst, send.at[send_at], recv.at[recv_at],
            device_id={axis: device}, device_id_type=MESH)

    def exchange(low, high, dst_low, dst_high, send_at, recvs, axis, up, down):
        return (copy_to(high, dst_low, send_at, recvs[0], axis, up),
                copy_to(low, dst_high, send_at, recvs[-1], axis, down))

    def start(pair, high, low):
        pl.when(high)(pair[0].start)
        pl.when(low)(pair[1].start)

    def settle(both, one, send_at, recv_at, high, low, received):
        def wait(ref):
            copy = copy_to(ref, ref, send_at, recv_at, "gz", z_up)
            return copy.wait_recv if received else copy.wait_send

        pl.when(high & low)(wait(both))
        pl.when(high ^ low)(wait(one))

    def finish_x(both, one, recv_at):
        settle(both, one, 0, recv_at, not_high_x, not_low_x, True)

    def finish_y(both, one, recv_at):
        settle(both, one, 1, recv_at, not_high_y, not_low_y, True)

    up_x, down_x = jnp.minimum(x_at + 1, gx - 1), jnp.maximum(x_at - 1, 0)
    up_y, down_y = jnp.minimum(y_at + 1, gy - 1), jnp.maximum(y_at - 1, 0)
    rest = pl.ds(0, 3)

    def along_x(fields, recvs):
        return exchange(blk.at[fields, 1], blk.at[fields, nx], blk.at[fields, 0], blk.at[fields, nx + 1],
                        0, recvs, "gx", up_x, down_x)

    def along_y(fields, recvs):
        return exchange(ypack.at[0, fields], ypack.at[1, fields], yhalo.at[0, fields], yhalo.at[1, fields],
                        1, recvs, "gy", up_y, down_y)

    x1, x1_rest = along_x(3, (0,)), along_x(rest, (1,))
    y1, y1_rest = along_y(3, (2,)), along_y(rest, (3,))
    z1 = exchange(zpack.at[0], zpack.at[1], zhalo.at[0], zhalo.at[1], 2, (4, 5), "gz", z_up, z_down)
    zv = exchange(vzpack.at[0], vzpack.at[1], vzhalo.at[0], vzhalo.at[1], 2, (6,), "gz", z_up, z_down)
    zc = copy_to(wpack, whalo, 3, 7, "gz", z_up)

    pltpu.make_async_copy(blk.at[:, inside], blk.at[:, inside], load_sem.at[0]).wait()
    for side, y in ((0, 0), (1, ny - 1)):
        ypack[side, 3] = blk[3, inside, y, :]
    low, high = pack_z(4, lambda f, x: blk[f, x + 1])
    zpack[0] = low
    zpack[1] = high
    pl.when(peers > 0)(lambda: pl.semaphore_wait(barrier, peers))
    pl.when(z_last)(z1[0].start)
    start(y1, not_high_y, not_low_y)
    start(x1, not_high_x, not_low_x)
    pl.when(not_first)(z1[1].start)
    pl.when(not_last)(z1[0].start)
    pl.when(z_last)(lambda: signal(ready.at[0], {"gz": z_up}))
    for which in range(len(phases)):
        axes, count, _, me = members(which)

        @pl.when(me == count - 1)
        def _():
            for k in range(count - 1):
                signal(ready.at[1 + which], ring_device(axes, k))
    pltpu.make_async_copy(vp, vp, load_sem.at[1]).wait()
    force = forcing[0]

    def drag_plane(x):
        v = vp[0, x]
        c = [blk[1 + k, x + 1] for k in range(3)]
        q = [vp[1 + k, x] for k in range(3)]
        square = sum((c[k] - q[k]) ** 2 for k in range(3))
        slip = square * lax.rsqrt(jnp.maximum(square, TINY))
        drag = drag_scale * (1.0 - v) * jnp.exp(-2.65 * jnp.log(v)) * (1.0 + slip)
        step_drag = time_step * drag
        inverse = 1.0 / (1.0 + step_drag)
        w = v * inverse
        inv[x] = inverse
        weight[x] = w
        for k in range(3):
            ustar[k, x] = c[k] + step_drag * q[k]
        return w

    weights = [drag_plane(x) for x in range(nx)]
    w_low, w_high = pack_z(1, lambda f, x: weights[x], 3 * nx)
    wpack[...] = w_high
    pl.when(z_last)(zc.start)

    def coefficients(face, w, sign, at):
        upward = w * (time_step * viscosity + (sign * 0.5 * time_step) * face)
        pressed = (sign * 0.5 * time_step) * pltpu.roll(w, nz - 3 * nx, 1)
        return jnp.where(at < nx, pressed,
                         jnp.where((at >= 3 * nx) & (at < 4 * nx), upward, 0.0))

    c_low = pltpu.roll(coefficients(zpack[0], w_low, 1.0, lane), nz - 1, 1)
    c_high = pltpu.roll(coefficients(zpack[1], w_high, -1.0, lax.rem(lane + 1, nz)), 1, 1)
    for f in range(3):
        ypack[0, f] = blk[f, inside, 0, :]
        ypack[1, f] = blk[f, inside, ny - 1, :]
    def wall_x(within, halo_plane, edge_plane):
        @pl.when(jnp.logical_not(within))
        def _():
            for f in range(1, 4):
                blk[f, halo_plane] = zero
            blk[0, halo_plane] = blk[0, edge_plane]

    wall_x(not_low_x, 0, 1)
    wall_x(not_high_x, nx + 1, nx)

    def wall_y(within, side):
        @pl.when(jnp.logical_not(within))
        def _():
            for f in range(1, 4):
                yhalo[side, f] = jnp.zeros((nx, nz), jnp.float32)
            yhalo[side, 0] = ypack[side, 0]

    wall_y(not_low_y, 0)
    wall_y(not_high_y, 1)

    def stencil(x, k):
        p = x + 1
        centre = [blk[1 + f, p] for f in range(3)]

        def pair(f, axis_no):
            if axis_no == 0:
                return blk[f, p - 1], blk[f, p + 1]
            field = blk[f, p]
            if axis_no == 1:
                return (jnp.where(row == 0, 0.0, pltpu.roll(field, 1, 0)),
                        jnp.where(row == ny - 1, 0.0, pltpu.roll(field, ny - 1, 0)))
            return (jnp.where(lane == 0, 0.0, pltpu.roll(field, 1, 1)),
                    jnp.where(lane == nz - 1, 0.0, pltpu.roll(field, nz - 1, 1)))

        advect = total = None
        for axis_no in range(3):
            low, high = pair(1 + k, axis_no)
            term = centre[axis_no] * (high - low)
            both = high + low
            advect = term if advect is None else advect + term
            total = both if total is None else total + both
        low, high = pair(0, k)
        forces = (viscosity * (total - 6.0 * centre[k])
                  - 0.5 * (advect + (high - low)))
        if k == 2:
            forces = forces + force
        value = ustar[k, x] + time_step * forces
        ustar[k, x] = value * inv[x]
        return value

    def upward_body(i, flow):
        for x in (1 + 2 * i, 2 + 2 * i):
            flow = flow + weight[x] * stencil(x, 2)
        return flow

    flow = lax.fori_loop(0, (nx - 2) // 2, upward_body, zero, unroll=3)

    start(x1_rest, not_high_x, not_low_x)
    start(y1_rest, not_high_y, not_low_y)

    low, high = pack_z(1, lambda f, x: vp[0, x])
    vzpack[0] = low
    vzpack[1] = high
    zv[0].start()
    pl.when(not_first)(zv[1].start)

    def along_y_coefficients(side, sign):
        w = weight[:, 0 if side == 0 else ny - 1, :]
        return w * (time_step * viscosity + (sign * 0.5 * time_step) * ypack[side, 2])

    cy_low, cy_high = along_y_coefficients(0, 1.0), along_y_coefficients(1, -1.0)

    void_total = lax.fori_loop(0, nx, lambda x, total: total + vp[0, x], zero, unroll=8)
    void_line = jnp.sum(void_total, axis=0, keepdims=True)

    def across_body(i, carry):
        for x in (1 + 2 * i, 2 + 2 * i):
            stencil(x, 0)
            stencil(x, 1)
        return carry

    lax.fori_loop(0, (nx - 2) // 2, across_body, 0, unroll=3)
    @pl.when(z_first)
    def _():
        pl.semaphore_wait(ready.at[0], 1)
        z1[1].start()
        zv[1].start()

    def sum_copy(which, src, dst, device):
        return pltpu.make_async_remote_copy(
            src, dst, sum_send.at[which], sum_recv.at[which], device_id=device, device_id_type=MESH)

    def all_in(which):
        _, count, _, me = members(which)

        @pl.when(me < count - 1)
        def _():
            pl.semaphore_wait(ready.at[1 + which], 1)

    def send_sums(which, first, last):
        axes, count, base, me = members(which)
        mine = slots.at[base + me]
        for k in range(first, min(last, count - 1)):
            other = jnp.where(k < me, k, k + 1)
            sum_copy(which, mine, mine, ring_device(axes, other)).start()

    def send_sum(which, value, last):
        _, _, base, me = members(which)
        for at in range(2):
            slots[base + me, at] = value[at][0]
        send_sums(which, 0, last)

    def all_sums(which):
        axes, count, base, me = members(which)
        others = slots.at[pl.ds(base, count - 1)]
        return sum_copy(which, others, others, ring_device(axes, lax.rem(me + 1, count)))

    def recv_sum(which):
        axes, count, base, me = members(which)
        all_sums(which).wait_recv()
        return [jnp.sum(slots[pl.ds(base, count), at], axis=0, keepdims=True) for at in range(2)]

    finish_x(blk.at[3, pl.ds(0, 2)], blk.at[3, 0], 0)
    flow = flow + weight[0] * stencil(0, 2) + weight[nx - 1] * stencil(nx - 1, 2)
    acc[...] = flow
    finish_y(yhalo.at[:, 3], yhalo.at[0, 3], 2)
    y_line = jnp.sum(cy_low * yhalo[0, 3] + cy_high * yhalo[1, 3], axis=0, keepdims=True)
    def across_edges():
        finish_x(blk.at[rest, pl.ds(0, 2)], blk.at[rest, 0], 1)
        for x in (0, nx - 1):
            stencil(x, 0)
            stencil(x, 1)

    pl.when(z_first)(across_edges)
    z1[0].wait_recv()
    acc[...] += c_low * zhalo[0]

    @pl.when(z_first)
    def _():
        face = pltpu.roll(zpack[0], nz - 1, 1)
        edge[...] = ((time_step * viscosity - (0.5 * time_step) * zhalo[0]) * face
                     - (0.5 * time_step) * pltpu.roll(face, 3 * nx, 1))

    @pl.when(jnp.logical_not(z_last))
    def _():
        z1[1].wait_recv()
        acc[...] += c_high * zhalo[1]

    devices = gx * gy * gz

    def sum_up(last=devices):
        send_sum(0, (jnp.sum(acc[...], axis=0, keepdims=True) + y_line, void_line), last)

    for which in range(len(phases)):
        all_in(which)
    pl.when(jnp.logical_not(z_first))(sum_up)

    first_row = row == 0
    last_row = row == ny - 1
    first_lane = lane == 0
    last_lane = lane == nz - 1
    row_sign = jnp.where(first_row, 1.0, jnp.where(last_row, -1.0, 0.0))
    lane_sign = jnp.where(first_lane, 1.0, jnp.where(last_lane, -1.0, 0.0))
    row_sign, lane_sign = (s * (0.5 * time_step) for s in (row_sign, lane_sign))
    row_visc, lane_visc = (jnp.abs(s) * (2.0 * viscosity) for s in (row_sign, lane_sign))

    def unpack(which, at):
        return pltpu.roll(which, lax.rem(2 * nz - at, nz), 1)

    def rows(f, x):
        return jnp.where(
            row < ny // 2,
            jnp.broadcast_to(yhalo[0, f, pl.ds(x, 1), :], (ny, nz)),
            jnp.broadcast_to(yhalo[1, f, pl.ds(x, 1), :], (ny, nz)))

    def correct(x, which, components, with_rows=True):
        by_row = row_visc + row_sign * blk[2, x + 1]
        by_lane = lane_visc + lane_sign * blk[3, x + 1]
        inverse, v = inv[x], vp[0, x]
        for k in components:
            value = by_lane * unpack(which, (1 + k) * nx + x)
            if with_rows:
                value = value + by_row * rows(1 + k, x)
            if k == 1:
                value = value + row_sign * rows(0, x)
            if k == 2:
                value = value + lane_sign * unpack(which, x)
            value = ustar[k, x] + value * inverse
            ustar[k, x] = value
            flux[k, x] = v * value

    def correct_all(pair, components, with_rows=True):
        def body(i, carry):
            correct(2 * i, pair[0], components, with_rows)
            correct(2 * i + 1, pair[1], components, with_rows)
            return carry

        lax.fori_loop(0, nx // 2, body, 0, unroll=8)

    x2 = exchange(flux.at[0, 0], flux.at[0, nx - 1], fxhalo.at[0], fxhalo.at[1], 0, (8,), "gx", up_x, down_x)
    y2 = exchange(ypack.at[0, 4], ypack.at[1, 4], fyhalo.at[0], fyhalo.at[1], 1, (9,), "gy", up_y, down_y)
    z2 = exchange(fzpack.at[0], fzpack.at[1], fzhalo.at[0], fzhalo.at[1], 2, (10,), "gz", z_up, z_down)

    def send_flux_z():
        low, high = pack_z(1, lambda f, x: flux[2, x])
        fzpack[0] = low
        fzpack[1] = high
        for copy in z2:
            copy.start()

    z_low = pltpu.roll(zhalo[0], 1, 1)
    @pl.when(z_first)
    def _():
        zc.wait_recv()
    @pl.when(z_first)
    def _():
        product = whalo[...] * edge[...]
        acc[...] += product
        sum_up(plane - 1)
        edge[...] = jnp.where(lane < nx, pltpu.roll(product, nz - 3 * nx + 1, 1), 0.0)

    @pl.when(z_last)
    def _():
        correct_all(interleave(z_low, zero), (2,))
        send_flux_z()

    pl.when(z_last)(z1[1].wait_recv)
    z_high = pltpu.roll(zhalo[1], nz - 1, 1)
    joined = interleave(z_low, z_high)
    pl.when(not_first)(across_edges)
    finish_y(yhalo.at[:, rest], yhalo.at[0, rest], 3)
    correct_all(joined, (0, 1))
    ypack[0, 4] = flux[1, :, 0, :]
    ypack[1, 4] = flux[1, :, ny - 1, :]
    start(y2, not_high_y, not_low_y)
    start(x2, not_high_x, not_low_x)

    pl.when(z_first)(lambda: send_sums(0, plane - 1, devices))
    @pl.when(not_first)
    def _():
        edge[...] = zero

    @pl.when(z_last)
    def _():
        correct_all(interleave(zero, z_high), (2,), False)

    @pl.when(not_last)
    def _():
        correct_all(joined, (2,))
        send_flux_z()

    for within, side in ((not_low_x, 0), (not_high_x, 1)):
        @pl.when(jnp.logical_not(within))
        def _():
            fxhalo[side] = zero
    for within, side in ((not_low_y, 0), (not_high_y, 1)):
        @pl.when(jnp.logical_not(within))
        def _():
            fyhalo[side] = jnp.zeros((nx, nz), jnp.float32)

    copy_to(vzpack, vzhalo, 2, 6, "gz", z_up).wait_recv()
    v_joined = interleave(pltpu.roll(vzhalo[0], 1, 1), pltpu.roll(vzhalo[1], nz - 1, 1))

    def source_plane(x, odd, x_low, x_high):
        fy, fz, v = flux[1, x], flux[2, x], vp[0, x]
        y_low = jnp.where(first_row, 0.0, pltpu.roll(fy, 1, 0))
        y_high = jnp.where(last_row, 0.0, pltpu.roll(fy, ny - 1, 0))
        z_low = jnp.where(first_lane, 0.0, pltpu.roll(fz, 1, 1))
        z_high = jnp.where(last_lane, 0.0, pltpu.roll(fz, nz - 1, 1))
        v_halo = unpack(v_joined[odd], x)
        v_low = jnp.where(first_lane, v_halo, pltpu.roll(v, 1, 1))
        v_high = jnp.where(last_lane, v_halo, pltpu.roll(v, nz - 1, 1))
        div[x] = 0.5 * ((x_high - x_low) + (y_high - y_low) + (z_high - z_low))
        slope[x] = (0.5 * time_step) * (v_high - v_low)

    def source_body(i, carry):
        x = 2 * i + 1
        source_plane(x, 1, flux[0, x - 1], flux[0, x + 1])
        source_plane(x + 1, 0, flux[0, x], flux[0, x + 2])
        return carry

    lax.fori_loop(0, nx // 2 - 1, source_body, 0, unroll=3)
    phase = 0
    while phase < len(phases) - 1:
        total = recv_sum(phase)
        phase += 1
        send_sum(phase, total, devices)
    finish_x(fxhalo, fxhalo.at[0], 8)
    source_plane(0, 0, fxhalo[0], flux[0, 1])
    source_plane(nx - 1, 1, flux[0, nx - 2], fxhalo[1])
    finish_y(fyhalo, fyhalo.at[0], 9)
    copy_to(fzpack, fzhalo, 2, 10, "gz", z_up).wait_recv()
    f_joined = interleave(pltpu.roll(fzhalo[0], 1, 1) + edge[...], pltpu.roll(fzhalo[1], nz - 1, 1))
    row_half, lane_half = row_sign / time_step, lane_sign / time_step

    def edge_plane(x, odd):
        y_halo = jnp.where(
            row < ny // 2,
            jnp.broadcast_to(fyhalo[0, pl.ds(x, 1), :], (ny, nz)),
            jnp.broadcast_to(fyhalo[1, pl.ds(x, 1), :], (ny, nz)))
        div[x] = div[x] - row_half * y_halo - lane_half * unpack(f_joined[odd], x)

    def edge_body(i, carry):
        edge_plane(2 * i, 0)
        edge_plane(2 * i + 1, 1)
        return carry

    lax.fori_loop(0, nx // 2, edge_body, 0, unroll=16)

    for which in range(len(phases)):
        all_sums(which).wait_send()
    sent = inv.at[pl.ds(0, 5)]
    settle(inv.at[pl.ds(0, 10)], sent, 0, 0, not_high_x, not_low_x, False)
    settle(ypack, ypack.at[0], 1, 2, not_high_y, not_low_y, False)
    sent = inv.at[pl.ds(0, 6)]
    copy_to(sent, sent, 2, 4, "gz", z_up).wait_send()
    pl.when(z_last)(zc.wait_send)

    total = recv_sum(phase)
    flow_sum, void_sum = (jnp.sum(t, axis=1, keepdims=True) for t in total)
    cells = float(nx * ny * nz * gx * gy * gz)
    step = (target[0] * cells - flow_sum) / (time_step * void_sum)
    lines[0] = jnp.broadcast_to(step, (1, nz)) + force
    lines[1] = jnp.broadcast_to(step, (1, nz))


def shift_kernel(ustar, div, slope, lines, vel_out, source_out, forcing_out, made, sem):
    nx, ny, nz = div.shape
    half = nx // 2
    across, line = pl.ds(0, 2), pltpu.make_async_copy(lines.at[0], forcing_out, sem.at[2])
    for k in range(2):
        for part in range(2):
            planes = pl.ds(part * half, half)
            pltpu.make_async_copy(ustar.at[k, planes], vel_out.at[k, planes], sem.at[0]).start()
    line.start()
    step = jnp.broadcast_to(lines[1], (ny, nz))
    for part in range(2):
        def body(i, carry):
            x = part * half + i
            made[0, x] = ustar[2, x] + time_step * step
            made[1, x] = div[x] + step * slope[x]
            return carry

        lax.fori_loop(0, half, body, 0, unroll=8)
        planes = pl.ds(part * half, half)
        pltpu.make_async_copy(made.at[0, planes], vel_out.at[2, planes], sem.at[1]).start()
        pltpu.make_async_copy(made.at[1, planes], source_out.at[planes], sem.at[1]).start()
    pltpu.make_async_copy(ustar.at[across], vel_out.at[across], sem.at[0]).wait()
    pltpu.make_async_copy(made, vel_out.at[across], sem.at[1]).wait()
    line.wait()


def local(velocity, pressure, voidage, particle_vel, forcing, target_flux):
    nx, ny, nz = voidage.shape
    sizes = tuple(lax.axis_size(a) for a in ("gx", "gy", "gz"))
    if math.prod(sizes) <= DIRECT_LIMIT:
        phases = (("gz", "gy", "gx"),)
    else:
        phases = (("gy", "gx"), ("gz",))
    slot_count = sum(math.prod(lax.axis_size(a) for a in axes) for axes in phases)
    f32 = jnp.float32
    vmem = pl.BlockSpec(memory_space=pltpu.VMEM)
    smem = pl.BlockSpec(memory_space=pltpu.SMEM)
    hbm = pl.BlockSpec(memory_space=pltpu.HBM)
    dma = pltpu.SemaphoreType.DMA
    faces = [pltpu.VMEM((2, ny, nz), f32), pltpu.VMEM((2, ny, nz), f32)]
    face = [pltpu.VMEM((ny, nz), f32)]
    results = pl.pallas_call(
        functools.partial(kernel, sizes, phases),
        out_shape=(
            pltpu.VMEM((3, nx, ny, nz), f32),
            pltpu.VMEM((nx, ny, nz), f32),
            pltpu.VMEM((nx, ny, nz), f32),
            pltpu.VMEM((2, 1, nz), f32),
        ),
        in_specs=[hbm] * 4 + [smem] * 2,
        out_specs=(vmem,) * 4,
        scratch_shapes=[
            pltpu.VMEM((4, nx + 2, ny, nz), f32),
            pltpu.VMEM((4, nx, ny, nz), f32),
            pltpu.VMEM((nx, ny, nz), f32),
            pltpu.VMEM((nx, ny, nz), f32),
            pltpu.VMEM((3, nx, ny, nz), f32),
        ] + face + face + [
            pltpu.VMEM((2, 5, nx, nz), f32),
            pltpu.VMEM((2, 4, nx, nz), f32),
        ] + faces + face + face + faces + [
            pltpu.VMEM((2, nx, nz), f32),
            pltpu.VMEM((2, ny, nz), f32),
        ] + faces + [
            pltpu.VMEM((slot_count, 2, nz), f32),
            dma((2,)), dma((4,)), dma((11,)),
            dma((len(phases),)), dma((len(phases),)),
            pltpu.SemaphoreType.REGULAR((1 + len(phases),)),
        ],
        compiler_params=pltpu.CompilerParams(collective_id=0, has_side_effects=True),
    )(velocity, pressure, voidage, particle_vel, forcing, target_flux)
    vel_new, source, forcing_new = pl.pallas_call(
        shift_kernel,
        out_shape=(
            jax.ShapeDtypeStruct((3, nx, ny, nz), f32),
            jax.ShapeDtypeStruct((nx, ny, nz), f32),
            jax.ShapeDtypeStruct((1, nz), f32),
        ),
        in_specs=[vmem] * 4,
        out_specs=(hbm,) * 3,
        scratch_shapes=[
            pltpu.VMEM((2, nx, ny, nz), f32),
            dma((3,)),
        ],
    )(*(pltpu.with_memory_space_constraint(a, pltpu.VMEM) for a in results))
    return vel_new, source, forcing_new[0, :1]


def solution(mesh):
    return jax.shard_map(
        local,
        mesh=mesh,
        in_specs=(
            P(None, "gx", "gy", "gz"),
            P("gx", "gy", "gz"),
            P("gx", "gy", "gz"),
            P(None, "gx", "gy", "gz"),
            P(),
            P(),
        ),
        out_specs=(P(None, "gx", "gy", "gz"), P("gx", "gy", "gz"), P()),
        check_vma=False,
    )
```

```python
import functools
import math

import jax
import jax.numpy as jnp
from jax import lax
from jax.experimental import pallas as pl
from jax.experimental.pallas import tpu as pltpu
from jax.sharding import PartitionSpec as P

time_step = 0.2
viscosity = 0.1
drag_scale = 1.0
MESH = pl.DeviceIdType.MESH
DIRECT_LIMIT = 64
TINY = 1.1754944e-38


def ring_index(axes):
    index = 0
    for axis in axes:
        index = index * lax.axis_size(axis) + lax.axis_index(axis)
    return index


def ring_device(axes, index):
    device = {}
    for axis in reversed(axes):
        size = lax.axis_size(axis)
        device[axis] = lax.rem(index, size)
        index = lax.div(index, size)
    return device


def kernel(
    sizes, phases,
    vel_hbm, pres_hbm, void_hbm, part_hbm, forcing, target,
    ustar, div, slope, lines,
    blk, vp, inv, weight, flux, acc, edge, pair, ypack, yhalo, zpack, zhalo, wpack, whalo,
    vzpack, vzhalo, fyhalo, fxhalo, fzpack, fzhalo, slots,
    load_sem, send, recv, sum_send, sum_recv, ready,
):
    gx, gy, gz = sizes
    nx, ny, nz = div.shape
    x_at, y_at, z_at = (lax.axis_index(a) for a in ("gx", "gy", "gz"))
    not_low_x, not_high_x = x_at > 0, x_at < gx - 1
    not_low_y, not_high_y = y_at > 0, y_at < gy - 1
    z_up, z_down = lax.rem(z_at + 1, gz), lax.rem(z_at + gz - 1, gz)
    z_first, z_last = z_at == 0, z_at == gz - 1
    not_first, not_last = z_at > 0, z_at < gz - 1

    def signal(sem, device):
        pl.semaphore_signal(sem, inc=1, device_id=device, device_id_type=MESH)

    def members(which):
        axes = phases[which]
        count = math.prod(lax.axis_size(a) for a in axes)
        base = sum(math.prod(lax.axis_size(a) for a in phases[w]) for w in range(which))
        return axes, count, base, ring_index(axes)

    plane = gx * gy
    direct = len(phases) == 1
    if direct:
        near = ((1, gx, plane, plane * (gz - 1)),)
    else:
        near = ((1, gx), (1, gz - 1))
    barrier = pltpu.get_barrier_semaphore()
    peers = jnp.where(z_last, 1, 0)
    for there, axis, at in ((not_high_y, "gy", y_at + 1), (not_last, "gz", z_at + 1), (not_high_x, "gx", x_at + 1),
                            (not_low_y, "gy", y_at - 1), (not_first, "gz", z_at - 1), (not_low_x, "gx", x_at - 1)):
        pl.when(there)(lambda: signal(barrier, {axis: at}))
        peers = peers + jnp.where(there, 1, 0)
    pl.when(z_first)(lambda: signal(barrier, {"gz": gz - 1}))
    for which in range(len(phases)):
        axes, count, _, me = members(which)
        far = me < count - 1
        for d in near[which]:
            far = far & (me != count - 1 - d)
        pl.when(far)(lambda: signal(barrier, ring_device(axes, count - 1)))
        peers = peers + jnp.where(me == count - 1, count - 1 - len(near[which]), 0)

    inside = pl.ds(1, nx)
    for load in (
        pltpu.make_async_copy(vel_hbm, blk.at[pl.ds(1, 3), inside], load_sem.at[0]),
        pltpu.make_async_copy(pres_hbm, blk.at[0, inside], load_sem.at[0]),
        pltpu.make_async_copy(void_hbm, vp.at[0], load_sem.at[1]),
        pltpu.make_async_copy(part_hbm, vp.at[pl.ds(1, 3)], load_sem.at[1]),
    ):
        load.start()

    lane = lax.broadcasted_iota(jnp.int32, (ny, nz), 1)
    row = lax.broadcasted_iota(jnp.int32, (ny, nz), 0)
    zero = jnp.zeros((ny, nz), jnp.float32)

    even = lax.rem(lane, 2) == 0
    pairs = (lax.div(lax.rem(lane + 1, nz), 2), lax.div(lane, 2))

    def interleave(low, high):
        return jnp.where(even, low, high), jnp.where(even, high, low)

    def pack_z(fields, read, at=0):
        tiles = []
        for odd in range(2):
            total = None
            for f in range(fields):
                tile = zero
                for x in range(odd, nx, 2):
                    turned = read(f, x)
                    to = (at + f * nx + x) % nz
                    if to:
                        turned = pltpu.roll(turned, to, 1)
                    tile = jnp.where(pairs[odd] == to // 2, turned, tile)
                total = tile if total is None else total + tile
            tiles.append(total)
        return interleave(*tiles)

    def copy_to(src, dst, send_at, recv_at, axis, device):
        return pltpu.make_async_remote_copy(
            src, dst, send.at[send_at], recv.at[recv_at],
            device_id={axis: device}, device_id_type=MESH)

    def exchange(low, high, dst_low, dst_high, send_at, recvs, axis, up, down):
        return (copy_to(high, dst_low, send_at, recvs[0], axis, up),
                copy_to(low, dst_high, send_at, recvs[-1], axis, down))

    def start(pair, high, low):
        pl.when(high)(pair[0].start)
        pl.when(low)(pair[1].start)

    def settle(both, one, send_at, recv_at, high, low, received):
        def wait(ref):
            copy = copy_to(ref, ref, send_at, recv_at, "gz", z_up)
            return copy.wait_recv if received else copy.wait_send

        pl.when(high & low)(wait(both))
        pl.when(high ^ low)(wait(one))

    def finish_x(both, one, recv_at):
        settle(both, one, 0, recv_at, not_high_x, not_low_x, True)

    def finish_y(both, one, recv_at):
        settle(both, one, 1, recv_at, not_high_y, not_low_y, True)

    up_x, down_x = jnp.minimum(x_at + 1, gx - 1), jnp.maximum(x_at - 1, 0)
    up_y, down_y = jnp.minimum(y_at + 1, gy - 1), jnp.maximum(y_at - 1, 0)
    rest = pl.ds(0, 3)

    def along_x(fields, recvs):
        return exchange(blk.at[fields, 1], blk.at[fields, nx], blk.at[fields, 0], blk.at[fields, nx + 1],
                        0, recvs, "gx", up_x, down_x)

    def along_y(fields, recvs):
        return exchange(ypack.at[0, fields], ypack.at[1, fields], yhalo.at[0, fields], yhalo.at[1, fields],
                        1, recvs, "gy", up_y, down_y)

    x1, x1_rest = along_x(3, (0,)), along_x(rest, (1,))
    y1, y1_rest = along_y(3, (2,)), along_y(rest, (3,))
    z1 = exchange(zpack.at[0], zpack.at[1], zhalo.at[0], zhalo.at[1], 2, (4, 5), "gz", z_up, z_down)
    zv = exchange(vzpack.at[0], vzpack.at[1], vzhalo.at[0], vzhalo.at[1], 2, (6,), "gz", z_up, z_down)
    zc = copy_to(wpack, whalo, 3, 7, "gz", z_up)

    pltpu.make_async_copy(blk.at[:, inside], blk.at[:, inside], load_sem.at[0]).wait()
    for side, y in ((0, 0), (1, ny - 1)):
        ypack[side, 3] = blk[3, inside, y, :]
    low, high = pack_z(4, lambda f, x: blk[f, x + 1])
    zpack[0] = low
    zpack[1] = high
    pl.when(peers > 0)(lambda: pl.semaphore_wait(barrier, peers))
    pl.when(z_last)(z1[0].start)
    start(y1, not_high_y, not_low_y)
    start(x1, not_high_x, not_low_x)
    pl.when(not_first)(z1[1].start)
    pl.when(not_last)(z1[0].start)
    pl.when(z_last)(lambda: signal(ready.at[0], {"gz": z_up}))
    for which in range(len(phases)):
        axes, count, _, me = members(which)

        @pl.when(me == count - 1)
        def _():
            for k in range(count - 1):
                signal(ready.at[1 + which], ring_device(axes, k))
    pltpu.make_async_copy(vp, vp, load_sem.at[1]).wait()
    force = forcing[0]

    def drag_plane(x):
        v = vp[0, x]
        c = [blk[1 + k, x + 1] for k in range(3)]
        q = [vp[1 + k, x] for k in range(3)]
        square = sum((c[k] - q[k]) ** 2 for k in range(3))
        slip = square * lax.rsqrt(jnp.maximum(square, TINY))
        drag = drag_scale * (1.0 - v) * jnp.exp(-2.65 * jnp.log(v)) * (1.0 + slip)
        step_drag = time_step * drag
        inverse = 1.0 / (1.0 + step_drag)
        w = v * inverse
        inv[x] = inverse
        weight[x] = w
        for k in range(3):
            ustar[k, x] = c[k] + step_drag * q[k]
        return w

    weights = [drag_plane(x) for x in range(nx)]
    w_low, w_high = pack_z(1, lambda f, x: weights[x], 3 * nx)
    wpack[...] = w_high
    pl.when(z_last)(zc.start)

    def coefficients(face, w, sign, at):
        upward = w * (time_step * viscosity + (sign * 0.5 * time_step) * face)
        pressed = (sign * 0.5 * time_step) * pltpu.roll(w, nz - 3 * nx, 1)
        return jnp.where(at < nx, pressed,
                         jnp.where((at >= 3 * nx) & (at < 4 * nx), upward, 0.0))

    c_low = pltpu.roll(coefficients(zpack[0], w_low, 1.0, lane), nz - 1, 1)
    c_high = pltpu.roll(coefficients(zpack[1], w_high, -1.0, lax.rem(lane + 1, nz)), 1, 1)
    for f in range(3):
        ypack[0, f] = blk[f, inside, 0, :]
        ypack[1, f] = blk[f, inside, ny - 1, :]
    def wall_x(within, halo_plane, edge_plane):
        @pl.when(jnp.logical_not(within))
        def _():
            for f in range(1, 4):
                blk[f, halo_plane] = zero
            blk[0, halo_plane] = blk[0, edge_plane]

    wall_x(not_low_x, 0, 1)
    wall_x(not_high_x, nx + 1, nx)

    def wall_y(within, side):
        @pl.when(jnp.logical_not(within))
        def _():
            for f in range(1, 4):
                yhalo[side, f] = jnp.zeros((nx, nz), jnp.float32)
            yhalo[side, 0] = ypack[side, 0]

    wall_y(not_low_y, 0)
    wall_y(not_high_y, 1)

    def stencil(x, k):
        p = x + 1
        centre = [blk[1 + f, p] for f in range(3)]

        def pair(f, axis_no):
            if axis_no == 0:
                return blk[f, p - 1], blk[f, p + 1]
            field = blk[f, p]
            if axis_no == 1:
                return (jnp.where(row == 0, 0.0, pltpu.roll(field, 1, 0)),
                        jnp.where(row == ny - 1, 0.0, pltpu.roll(field, ny - 1, 0)))
            return (jnp.where(lane == 0, 0.0, pltpu.roll(field, 1, 1)),
                    jnp.where(lane == nz - 1, 0.0, pltpu.roll(field, nz - 1, 1)))

        advect = total = None
        for axis_no in range(3):
            low, high = pair(1 + k, axis_no)
            term = centre[axis_no] * (high - low)
            both = high + low
            advect = term if advect is None else advect + term
            total = both if total is None else total + both
        low, high = pair(0, k)
        forces = (viscosity * (total - 6.0 * centre[k])
                  - 0.5 * (advect + (high - low)))
        if k == 2:
            forces = forces + force
        value = ustar[k, x] + time_step * forces
        ustar[k, x] = value * inv[x]
        return value

    def upward_body(i, flow):
        for x in (1 + 2 * i, 2 + 2 * i):
            flow = flow + weight[x] * stencil(x, 2)
        return flow

    flow = lax.fori_loop(0, (nx - 2) // 2, upward_body, zero, unroll=3)

    start(x1_rest, not_high_x, not_low_x)
    start(y1_rest, not_high_y, not_low_y)

    low, high = pack_z(1, lambda f, x: vp[0, x])
    vzpack[0] = low
    vzpack[1] = high
    zv[0].start()
    pl.when(not_first)(zv[1].start)

    def along_y_coefficients(side, sign):
        w = weight[:, 0 if side == 0 else ny - 1, :]
        return w * (time_step * viscosity + (sign * 0.5 * time_step) * ypack[side, 2])

    cy_low, cy_high = along_y_coefficients(0, 1.0), along_y_coefficients(1, -1.0)

    void_total = lax.fori_loop(0, nx, lambda x, total: total + vp[0, x], zero, unroll=8)
    void_line = jnp.sum(void_total, axis=0, keepdims=True)

    def across_body(i, carry):
        for x in (1 + 2 * i, 2 + 2 * i):
            stencil(x, 0)
            stencil(x, 1)
        return carry

    lax.fori_loop(0, (nx - 2) // 2, across_body, 0, unroll=3)
    @pl.when(z_first)
    def _():
        pl.semaphore_wait(ready.at[0], 1)
        z1[1].start()
        zv[1].start()

    def sum_copy(which, src, dst, device):
        return pltpu.make_async_remote_copy(
            src, dst, sum_send.at[which], sum_recv.at[which], device_id=device, device_id_type=MESH)

    def all_in(which):
        _, count, _, me = members(which)

        @pl.when(me < count - 1)
        def _():
            pl.semaphore_wait(ready.at[1 + which], 1)

    def send_sums(which, first, last):
        axes, count, base, me = members(which)
        mine = slots.at[base + me]
        for k in range(first, min(last, count - 1)):
            other = jnp.where(k < me, k, k + 1)
            sum_copy(which, mine, mine, ring_device(axes, other)).start()

    def send_sum(which, value, last):
        _, _, base, me = members(which)
        for at in range(2):
            slots[base + me, at] = value[at][0]
        send_sums(which, 0, last)

    def all_sums(which):
        axes, count, base, me = members(which)
        others = slots.at[pl.ds(base, count - 1)]
        return sum_copy(which, others, others, ring_device(axes, lax.rem(me + 1, count)))

    def recv_sum(which):
        axes, count, base, me = members(which)
        all_sums(which).wait_recv()
        return [jnp.sum(slots[pl.ds(base, count), at], axis=0, keepdims=True) for at in range(2)]

    finish_x(blk.at[3, pl.ds(0, 2)], blk.at[3, 0], 0)
    flow = flow + weight[0] * stencil(0, 2) + weight[nx - 1] * stencil(nx - 1, 2)
    acc[...] = flow
    finish_y(yhalo.at[:, 3], yhalo.at[0, 3], 2)
    y_line = jnp.sum(cy_low * yhalo[0, 3] + cy_high * yhalo[1, 3], axis=0, keepdims=True)
    def across_edges():
        finish_x(blk.at[rest, pl.ds(0, 2)], blk.at[rest, 0], 1)
        for x in (0, nx - 1):
            stencil(x, 0)
            stencil(x, 1)

    pl.when(z_first)(across_edges)

    @pl.when(z_first)
    def _():
        face = pltpu.roll(zpack[0], nz - 1, 1)
        wpack[...] = face
        edge[...] = (time_step * viscosity) * face - (0.5 * time_step) * pltpu.roll(face, 3 * nx, 1)

    z1[0].wait_recv()
    acc[...] += c_low * zhalo[0]

    @pl.when(jnp.logical_not(z_last))
    def _():
        z1[1].wait_recv()
        acc[...] += c_high * zhalo[1]

    devices = gx * gy * gz

    def sum_up(last=devices):
        send_sum(0, (jnp.sum(acc[...], axis=0, keepdims=True) + y_line, void_line), last)

    for which in range(len(phases)):
        all_in(which)
    pl.when(jnp.logical_not(z_first))(sum_up)

    first_row = row == 0
    last_row = row == ny - 1
    first_lane = lane == 0
    last_lane = lane == nz - 1
    row_sign = jnp.where(first_row, 1.0, jnp.where(last_row, -1.0, 0.0))
    lane_sign = jnp.where(first_lane, 1.0, jnp.where(last_lane, -1.0, 0.0))
    row_sign, lane_sign = (s * (0.5 * time_step) for s in (row_sign, lane_sign))
    row_visc, lane_visc = (jnp.abs(s) * (2.0 * viscosity) for s in (row_sign, lane_sign))

    def unpack(which, at):
        return pltpu.roll(which, lax.rem(2 * nz - at, nz), 1)

    def rows(f, x):
        return jnp.where(
            row < ny // 2,
            jnp.broadcast_to(yhalo[0, f, pl.ds(x, 1), :], (ny, nz)),
            jnp.broadcast_to(yhalo[1, f, pl.ds(x, 1), :], (ny, nz)))

    def correct(x, which, components, with_rows=True):
        by_row = row_visc + row_sign * blk[2, x + 1]
        by_lane = lane_visc + lane_sign * blk[3, x + 1]
        inverse, v = inv[x], vp[0, x]
        for k in components:
            value = by_lane * unpack(which, (1 + k) * nx + x)
            if with_rows:
                value = value + by_row * rows(1 + k, x)
            if k == 1:
                value = value + row_sign * rows(0, x)
            if k == 2:
                value = value + lane_sign * unpack(which, x)
            value = ustar[k, x] + value * inverse
            ustar[k, x] = value
            flux[k, x] = v * value

    def correct_all(pair, components, with_rows=True, first=0, last=nx // 2):
        def body(i, carry):
            correct(2 * i, pair[0], components, with_rows)
            correct(2 * i + 1, pair[1], components, with_rows)
            return carry

        lax.fori_loop(first, last, body, 0, unroll=8)

    x2 = exchange(flux.at[0, 0], flux.at[0, nx - 1], fxhalo.at[0], fxhalo.at[1], 0, (8,), "gx", up_x, down_x)
    y2 = exchange(ypack.at[0, 4], ypack.at[1, 4], fyhalo.at[0], fyhalo.at[1], 1, (9,), "gy", up_y, down_y)
    z2 = exchange(fzpack.at[0], fzpack.at[1], fzhalo.at[0], fzhalo.at[1], 2, (10,), "gz", z_up, z_down)

    def send_flux_z():
        low, high = pack_z(1, lambda f, x: flux[2, x])
        fzpack[0] = low
        fzpack[1] = high
        for copy in z2:
            copy.start()

    def join():
        pair[0], pair[1] = interleave(pltpu.roll(zhalo[0], 1, 1), pltpu.roll(zhalo[1], nz - 1, 1))

    def correct_first():
        finish_y(yhalo.at[:, rest], yhalo.at[0, rest], 3)
        correct_all((pair[0], pair[1]), (0, 1), last=nx // 4)

    @pl.when(z_first)
    def _():
        join()
        correct_first()

    @pl.when(z_first)
    def _():
        zc.wait_recv()
    @pl.when(z_first)
    def _():
        product = whalo[...] * (edge[...] - (0.5 * time_step) * zhalo[0] * wpack[...])
        acc[...] += product
        sum_up(plane - 1)
        edge[...] = jnp.where(lane < nx, pltpu.roll(product, nz - 3 * nx + 1, 1), 0.0)

    @pl.when(z_last)
    def _():
        correct_all(interleave(pltpu.roll(zhalo[0], 1, 1), zero), (2,))
        send_flux_z()

    pl.when(z_last)(z1[1].wait_recv)
    pl.when(not_first)(join)
    pl.when(not_first)(across_edges)
    pl.when(not_first)(correct_first)
    joined = pair[0], pair[1]
    correct_all(joined, (0, 1), first=nx // 4)
    ypack[0, 4] = flux[1, :, 0, :]
    ypack[1, 4] = flux[1, :, ny - 1, :]
    start(y2, not_high_y, not_low_y)
    start(x2, not_high_x, not_low_x)

    pl.when(z_first)(lambda: send_sums(0, plane - 1, devices))
    @pl.when(not_first)
    def _():
        edge[...] = zero

    @pl.when(z_last)
    def _():
        correct_all(interleave(zero, pltpu.roll(zhalo[1], nz - 1, 1)), (2,), False)

    @pl.when(not_last)
    def _():
        correct_all(joined, (2,))
        send_flux_z()

    for within, side in ((not_low_x, 0), (not_high_x, 1)):
        @pl.when(jnp.logical_not(within))
        def _():
            fxhalo[side] = zero
    for within, side in ((not_low_y, 0), (not_high_y, 1)):
        @pl.when(jnp.logical_not(within))
        def _():
            fyhalo[side] = jnp.zeros((nx, nz), jnp.float32)

    copy_to(vzpack, vzhalo, 2, 6, "gz", z_up).wait_recv()
    v_joined = interleave(pltpu.roll(vzhalo[0], 1, 1), pltpu.roll(vzhalo[1], nz - 1, 1))

    def source_plane(x, odd, x_low, x_high):
        fy, fz, v = flux[1, x], flux[2, x], vp[0, x]
        y_low = jnp.where(first_row, 0.0, pltpu.roll(fy, 1, 0))
        y_high = jnp.where(last_row, 0.0, pltpu.roll(fy, ny - 1, 0))
        z_low = jnp.where(first_lane, 0.0, pltpu.roll(fz, 1, 1))
        z_high = jnp.where(last_lane, 0.0, pltpu.roll(fz, nz - 1, 1))
        v_halo = unpack(v_joined[odd], x)
        v_low = jnp.where(first_lane, v_halo, pltpu.roll(v, 1, 1))
        v_high = jnp.where(last_lane, v_halo, pltpu.roll(v, nz - 1, 1))
        div[x] = 0.5 * ((x_high - x_low) + (y_high - y_low) + (z_high - z_low))
        slope[x] = (0.5 * time_step) * (v_high - v_low)

    def source_body(i, carry):
        x = 2 * i + 1
        source_plane(x, 1, flux[0, x - 1], flux[0, x + 1])
        source_plane(x + 1, 0, flux[0, x], flux[0, x + 2])
        return carry

    lax.fori_loop(0, nx // 2 - 1, source_body, 0, unroll=3)
    phase = 0
    while phase < len(phases) - 1:
        total = recv_sum(phase)
        phase += 1
        send_sum(phase, total, devices)
    finish_x(fxhalo, fxhalo.at[0], 8)
    source_plane(0, 0, fxhalo[0], flux[0, 1])
    source_plane(nx - 1, 1, flux[0, nx - 2], fxhalo[1])
    finish_y(fyhalo, fyhalo.at[0], 9)
    copy_to(fzpack, fzhalo, 2, 10, "gz", z_up).wait_recv()
    f_joined = interleave(pltpu.roll(fzhalo[0], 1, 1) + edge[...], pltpu.roll(fzhalo[1], nz - 1, 1))
    row_half, lane_half = row_sign / time_step, lane_sign / time_step

    def edge_plane(x, odd):
        y_halo = jnp.where(
            row < ny // 2,
            jnp.broadcast_to(fyhalo[0, pl.ds(x, 1), :], (ny, nz)),
            jnp.broadcast_to(fyhalo[1, pl.ds(x, 1), :], (ny, nz)))
        div[x] = div[x] - row_half * y_halo - lane_half * unpack(f_joined[odd], x)

    def edge_body(i, carry):
        edge_plane(2 * i, 0)
        edge_plane(2 * i + 1, 1)
        return carry

    lax.fori_loop(0, nx // 2, edge_body, 0, unroll=16)

    for which in range(len(phases)):
        all_sums(which).wait_send()
    sent = inv.at[pl.ds(0, 5)]
    settle(inv.at[pl.ds(0, 10)], sent, 0, 0, not_high_x, not_low_x, False)
    settle(ypack, ypack.at[0], 1, 2, not_high_y, not_low_y, False)
    sent = inv.at[pl.ds(0, 6)]
    copy_to(sent, sent, 2, 4, "gz", z_up).wait_send()
    pl.when(z_last)(zc.wait_send)

    total = recv_sum(phase)
    flow_sum, void_sum = (jnp.sum(t, axis=1, keepdims=True) for t in total)
    cells = float(nx * ny * nz * gx * gy * gz)
    step = (target[0] * cells - flow_sum) / (time_step * void_sum)
    lines[0] = jnp.broadcast_to(step, (1, nz)) + force
    lines[1] = jnp.broadcast_to(step, (1, nz))


def shift_kernel(ustar, div, slope, lines, vel_out, source_out, forcing_out, made, sem):
    nx, ny, nz = div.shape
    half = nx // 2
    across, line = pl.ds(0, 2), pltpu.make_async_copy(lines.at[0], forcing_out, sem.at[2])
    for k in range(2):
        for part in range(2):
            planes = pl.ds(part * half, half)
            pltpu.make_async_copy(ustar.at[k, planes], vel_out.at[k, planes], sem.at[0]).start()
    line.start()
    step = jnp.broadcast_to(lines[1], (ny, nz))
    for part in range(2):
        def body(i, carry):
            x = part * half + i
            made[0, x] = ustar[2, x] + time_step * step
            made[1, x] = div[x] + step * slope[x]
            return carry

        lax.fori_loop(0, half, body, 0, unroll=8)
        planes = pl.ds(part * half, half)
        pltpu.make_async_copy(made.at[0, planes], vel_out.at[2, planes], sem.at[1]).start()
        pltpu.make_async_copy(made.at[1, planes], source_out.at[planes], sem.at[1]).start()
    pltpu.make_async_copy(ustar.at[across], vel_out.at[across], sem.at[0]).wait()
    pltpu.make_async_copy(made, vel_out.at[across], sem.at[1]).wait()
    line.wait()


def local(velocity, pressure, voidage, particle_vel, forcing, target_flux):
    nx, ny, nz = voidage.shape
    sizes = tuple(lax.axis_size(a) for a in ("gx", "gy", "gz"))
    if math.prod(sizes) <= DIRECT_LIMIT:
        phases = (("gz", "gy", "gx"),)
    else:
        phases = (("gy", "gx"), ("gz",))
    slot_count = sum(math.prod(lax.axis_size(a) for a in axes) for axes in phases)
    f32 = jnp.float32
    vmem = pl.BlockSpec(memory_space=pltpu.VMEM)
    smem = pl.BlockSpec(memory_space=pltpu.SMEM)
    hbm = pl.BlockSpec(memory_space=pltpu.HBM)
    dma = pltpu.SemaphoreType.DMA
    faces = [pltpu.VMEM((2, ny, nz), f32), pltpu.VMEM((2, ny, nz), f32)]
    face = [pltpu.VMEM((ny, nz), f32)]
    results = pl.pallas_call(
        functools.partial(kernel, sizes, phases),
        out_shape=(
            pltpu.VMEM((3, nx, ny, nz), f32),
            pltpu.VMEM((nx, ny, nz), f32),
            pltpu.VMEM((nx, ny, nz), f32),
            pltpu.VMEM((2, 1, nz), f32),
        ),
        in_specs=[hbm] * 4 + [smem] * 2,
        out_specs=(vmem,) * 4,
        scratch_shapes=[
            pltpu.VMEM((4, nx + 2, ny, nz), f32),
            pltpu.VMEM((4, nx, ny, nz), f32),
            pltpu.VMEM((nx, ny, nz), f32),
            pltpu.VMEM((nx, ny, nz), f32),
            pltpu.VMEM((3, nx, ny, nz), f32),
        ] + face + face + faces[:1] + [
            pltpu.VMEM((2, 5, nx, nz), f32),
            pltpu.VMEM((2, 4, nx, nz), f32),
        ] + faces + face + face + faces + [
            pltpu.VMEM((2, nx, nz), f32),
            pltpu.VMEM((2, ny, nz), f32),
        ] + faces + [
            pltpu.VMEM((slot_count, 2, nz), f32),
            dma((2,)), dma((4,)), dma((11,)),
            dma((len(phases),)), dma((len(phases),)),
            pltpu.SemaphoreType.REGULAR((1 + len(phases),)),
        ],
        compiler_params=pltpu.CompilerParams(collective_id=0, has_side_effects=True),
    )(velocity, pressure, voidage, particle_vel, forcing, target_flux)
    vel_new, source, forcing_new = pl.pallas_call(
        shift_kernel,
        out_shape=(
            jax.ShapeDtypeStruct((3, nx, ny, nz), f32),
            jax.ShapeDtypeStruct((nx, ny, nz), f32),
            jax.ShapeDtypeStruct((1, nz), f32),
        ),
        in_specs=[vmem] * 4,
        out_specs=(hbm,) * 3,
        scratch_shapes=[
            pltpu.VMEM((2, nx, ny, nz), f32),
            dma((3,)),
        ],
    )(*(pltpu.with_memory_space_constraint(a, pltpu.VMEM) for a in results))
    return vel_new, source, forcing_new[0, :1]


def solution(mesh):
    return jax.shard_map(
        local,
        mesh=mesh,
        in_specs=(
            P(None, "gx", "gy", "gz"),
            P("gx", "gy", "gz"),
            P("gx", "gy", "gz"),
            P(None, "gx", "gy", "gz"),
            P(),
            P(),
        ),
        out_specs=(P(None, "gx", "gy", "gz"), P("gx", "gy", "gz"), P()),
        check_vma=False,
    )
```

```python
import functools
import math

import jax
import jax.numpy as jnp
from jax import lax
from jax.experimental import pallas as pl
from jax.experimental.pallas import tpu as pltpu
from jax.sharding import PartitionSpec as P

time_step = 0.2
viscosity = 0.1
drag_scale = 1.0
MESH = pl.DeviceIdType.MESH
DIRECT_LIMIT = 64
TINY = 1.1754944e-38


def ring_index(axes):
    index = 0
    for axis in axes:
        index = index * lax.axis_size(axis) + lax.axis_index(axis)
    return index


def ring_device(axes, index):
    device = {}
    for axis in reversed(axes):
        size = lax.axis_size(axis)
        device[axis] = lax.rem(index, size)
        index = lax.div(index, size)
    return device


def kernel(
    sizes, phases,
    vel_hbm, pres_hbm, void_hbm, part_hbm, forcing, target,
    ustar, div, slope, lines,
    blk, vp, inv, weight, flux, acc, edge, pair, ypack, yhalo, zpack, zhalo, wpack, whalo,
    vzpack, vzhalo, fyhalo, fxhalo, fzpack, fzhalo, slots,
    load_sem, send, recv, sum_send, sum_recv, ready,
):
    gx, gy, gz = sizes
    nx, ny, nz = div.shape
    x_at, y_at, z_at = (lax.axis_index(a) for a in ("gx", "gy", "gz"))
    not_low_x, not_high_x = x_at > 0, x_at < gx - 1
    not_low_y, not_high_y = y_at > 0, y_at < gy - 1
    z_up, z_down = lax.rem(z_at + 1, gz), lax.rem(z_at + gz - 1, gz)
    z_first, z_last = z_at == 0, z_at == gz - 1
    not_first, not_last = z_at > 0, z_at < gz - 1

    def signal(sem, device):
        pl.semaphore_signal(sem, inc=1, device_id=device, device_id_type=MESH)

    def members(which):
        axes = phases[which]
        count = math.prod(lax.axis_size(a) for a in axes)
        base = sum(math.prod(lax.axis_size(a) for a in phases[w]) for w in range(which))
        return axes, count, base, ring_index(axes)

    plane = gx * gy
    direct = len(phases) == 1
    if direct:
        near = ((1, gx, plane, plane * (gz - 1)),)
    else:
        near = ((1, gx), (1, gz - 1))
    barrier = pltpu.get_barrier_semaphore()
    peers = jnp.where(z_last, 1, 0)
    for there, axis, at in ((not_high_y, "gy", y_at + 1), (not_last, "gz", z_at + 1), (not_high_x, "gx", x_at + 1),
                            (not_low_y, "gy", y_at - 1), (not_first, "gz", z_at - 1), (not_low_x, "gx", x_at - 1)):
        pl.when(there)(lambda: signal(barrier, {axis: at}))
        peers = peers + jnp.where(there, 1, 0)
    pl.when(z_first)(lambda: signal(barrier, {"gz": gz - 1}))
    for which in range(len(phases)):
        axes, count, _, me = members(which)
        far = me < count - 1
        for d in near[which]:
            far = far & (me != count - 1 - d)
        pl.when(far)(lambda: signal(barrier, ring_device(axes, count - 1)))
        peers = peers + jnp.where(me == count - 1, count - 1 - len(near[which]), 0)

    inside = pl.ds(1, nx)
    for load in (
        pltpu.make_async_copy(vel_hbm, blk.at[pl.ds(1, 3), inside], load_sem.at[0]),
        pltpu.make_async_copy(pres_hbm, blk.at[0, inside], load_sem.at[0]),
        pltpu.make_async_copy(void_hbm, vp.at[0], load_sem.at[1]),
        pltpu.make_async_copy(part_hbm, vp.at[pl.ds(1, 3)], load_sem.at[1]),
    ):
        load.start()

    lane = lax.broadcasted_iota(jnp.int32, (ny, nz), 1)
    row = lax.broadcasted_iota(jnp.int32, (ny, nz), 0)
    zero = jnp.zeros((ny, nz), jnp.float32)

    even = lax.rem(lane, 2) == 0
    pairs = (lax.div(lax.rem(lane + 1, nz), 2), lax.div(lane, 2))

    def interleave(low, high):
        return jnp.where(even, low, high), jnp.where(even, high, low)

    def pack_z(fields, read, at=0):
        tiles = []
        for odd in range(2):
            total = None
            for f in range(fields):
                tile = zero
                for x in range(odd, nx, 2):
                    turned = read(f, x)
                    to = (at + f * nx + x) % nz
                    if to:
                        turned = pltpu.roll(turned, to, 1)
                    tile = jnp.where(pairs[odd] == to // 2, turned, tile)
                total = tile if total is None else total + tile
            tiles.append(total)
        return interleave(*tiles)

    def copy_to(src, dst, send_at, recv_at, axis, device):
        return pltpu.make_async_remote_copy(
            src, dst, send.at[send_at], recv.at[recv_at],
            device_id={axis: device}, device_id_type=MESH)

    def exchange(low, high, dst_low, dst_high, send_at, recvs, axis, up, down):
        return (copy_to(high, dst_low, send_at, recvs[0], axis, up),
                copy_to(low, dst_high, send_at, recvs[-1], axis, down))

    def start(pair, high, low):
        pl.when(high)(pair[0].start)
        pl.when(low)(pair[1].start)

    def settle(both, one, send_at, recv_at, high, low, received):
        def wait(ref):
            copy = copy_to(ref, ref, send_at, recv_at, "gz", z_up)
            return copy.wait_recv if received else copy.wait_send

        pl.when(high & low)(wait(both))
        pl.when(high ^ low)(wait(one))

    def finish_x(both, one, recv_at):
        settle(both, one, 0, recv_at, not_high_x, not_low_x, True)

    def finish_y(both, one, recv_at):
        settle(both, one, 1, recv_at, not_high_y, not_low_y, True)

    up_x, down_x = jnp.minimum(x_at + 1, gx - 1), jnp.maximum(x_at - 1, 0)
    up_y, down_y = jnp.minimum(y_at + 1, gy - 1), jnp.maximum(y_at - 1, 0)
    rest = pl.ds(0, 3)

    def along_x(fields, recvs):
        return exchange(blk.at[fields, 1], blk.at[fields, nx], blk.at[fields, 0], blk.at[fields, nx + 1],
                        0, recvs, "gx", up_x, down_x)

    def along_y(fields, recvs):
        return exchange(ypack.at[0, fields], ypack.at[1, fields], yhalo.at[0, fields], yhalo.at[1, fields],
                        1, recvs, "gy", up_y, down_y)

    x1, x1_rest = along_x(3, (0,)), along_x(rest, (1,))
    y1, y1_rest = along_y(3, (2,)), along_y(rest, (3,))
    z1 = exchange(zpack.at[0], zpack.at[1], zhalo.at[0], zhalo.at[1], 2, (4, 5), "gz", z_up, z_down)
    zv = exchange(vzpack.at[0], vzpack.at[1], vzhalo.at[0], vzhalo.at[1], 2, (6,), "gz", z_up, z_down)
    zc = copy_to(wpack, whalo, 3, 7, "gz", z_up)

    pltpu.make_async_copy(blk.at[:, inside], blk.at[:, inside], load_sem.at[0]).wait()
    for side, y in ((0, 0), (1, ny - 1)):
        ypack[side, 3] = blk[3, inside, y, :]
    low, high = pack_z(4, lambda f, x: blk[f, x + 1])
    zpack[0] = low
    zpack[1] = high
    pl.when(peers > 0)(lambda: pl.semaphore_wait(barrier, peers))
    pl.when(z_last)(z1[0].start)
    start(y1, not_high_y, not_low_y)
    start(x1, not_high_x, not_low_x)
    pl.when(not_first)(z1[1].start)
    pl.when(not_last)(z1[0].start)
    pl.when(z_last)(lambda: signal(ready.at[0], {"gz": z_up}))
    for which in range(len(phases)):
        axes, count, _, me = members(which)

        @pl.when(me == count - 1)
        def _():
            for k in range(count - 1):
                signal(ready.at[1 + which], ring_device(axes, k))
    pltpu.make_async_copy(vp, vp, load_sem.at[1]).wait()
    force = forcing[0]

    def drag_plane(x):
        v = vp[0, x]
        c = [blk[1 + k, x + 1] for k in range(3)]
        q = [vp[1 + k, x] for k in range(3)]
        square = sum((c[k] - q[k]) ** 2 for k in range(3))
        slip = square * lax.rsqrt(jnp.maximum(square, TINY))
        drag = drag_scale * (1.0 - v) * jnp.exp(-2.65 * jnp.log(v)) * (1.0 + slip)
        step_drag = time_step * drag
        inverse = 1.0 / (1.0 + step_drag)
        w = v * inverse
        inv[x] = inverse
        weight[x] = w
        for k in range(3):
            ustar[k, x] = c[k] + step_drag * q[k]
        return w

    weights = [drag_plane(x) for x in range(nx)]
    w_low, w_high = pack_z(1, lambda f, x: weights[x], 3 * nx)
    wpack[...] = w_high
    pl.when(z_last)(zc.start)

    def coefficients(face, w, sign, at):
        upward = w * (time_step * viscosity + (sign * 0.5 * time_step) * face)
        pressed = (sign * 0.5 * time_step) * pltpu.roll(w, nz - 3 * nx, 1)
        return jnp.where(at < nx, pressed,
                         jnp.where((at >= 3 * nx) & (at < 4 * nx), upward, 0.0))

    c_low = pltpu.roll(coefficients(zpack[0], w_low, 1.0, lane), nz - 1, 1)
    c_high = pltpu.roll(coefficients(zpack[1], w_high, -1.0, lax.rem(lane + 1, nz)), 1, 1)
    for f in range(3):
        ypack[0, f] = blk[f, inside, 0, :]
        ypack[1, f] = blk[f, inside, ny - 1, :]
    def wall_x(within, halo_plane, edge_plane):
        @pl.when(jnp.logical_not(within))
        def _():
            for f in range(1, 4):
                blk[f, halo_plane] = zero
            blk[0, halo_plane] = blk[0, edge_plane]

    wall_x(not_low_x, 0, 1)
    wall_x(not_high_x, nx + 1, nx)

    def wall_y(within, side):
        @pl.when(jnp.logical_not(within))
        def _():
            for f in range(1, 4):
                yhalo[side, f] = jnp.zeros((nx, nz), jnp.float32)
            yhalo[side, 0] = ypack[side, 0]

    wall_y(not_low_y, 0)
    wall_y(not_high_y, 1)

    def stencil(x, k):
        p = x + 1
        centre = [blk[1 + f, p] for f in range(3)]

        def pair(f, axis_no):
            if axis_no == 0:
                return blk[f, p - 1], blk[f, p + 1]
            field = blk[f, p]
            if axis_no == 1:
                return (jnp.where(row == 0, 0.0, pltpu.roll(field, 1, 0)),
                        jnp.where(row == ny - 1, 0.0, pltpu.roll(field, ny - 1, 0)))
            return (jnp.where(lane == 0, 0.0, pltpu.roll(field, 1, 1)),
                    jnp.where(lane == nz - 1, 0.0, pltpu.roll(field, nz - 1, 1)))

        advect = total = None
        for axis_no in range(3):
            low, high = pair(1 + k, axis_no)
            term = centre[axis_no] * (high - low)
            both = high + low
            advect = term if advect is None else advect + term
            total = both if total is None else total + both
        low, high = pair(0, k)
        forces = (viscosity * (total - 6.0 * centre[k])
                  - 0.5 * (advect + (high - low)))
        if k == 2:
            forces = forces + force
        value = ustar[k, x] + time_step * forces
        ustar[k, x] = value * inv[x]
        return value

    def upward_body(i, flow):
        for x in (1 + 2 * i, 2 + 2 * i):
            flow = flow + weight[x] * stencil(x, 2)
        return flow

    flow = lax.fori_loop(0, (nx - 2) // 2, upward_body, zero, unroll=3)

    start(x1_rest, not_high_x, not_low_x)
    start(y1_rest, not_high_y, not_low_y)

    low, high = pack_z(1, lambda f, x: vp[0, x])
    vzpack[0] = low
    vzpack[1] = high
    zv[0].start()
    pl.when(not_first)(zv[1].start)

    def along_y_coefficients(side, sign):
        w = weight[:, 0 if side == 0 else ny - 1, :]
        return w * (time_step * viscosity + (sign * 0.5 * time_step) * ypack[side, 2])

    cy_low, cy_high = along_y_coefficients(0, 1.0), along_y_coefficients(1, -1.0)

    void_total = lax.fori_loop(0, nx, lambda x, total: total + vp[0, x], zero, unroll=8)
    void_line = jnp.sum(void_total, axis=0, keepdims=True)

    def across_body(i, carry):
        for x in (1 + 2 * i, 2 + 2 * i):
            stencil(x, 0)
            stencil(x, 1)
        return carry

    lax.fori_loop(0, (nx - 2) // 2, across_body, 0, unroll=3)
    @pl.when(z_first)
    def _():
        pl.semaphore_wait(ready.at[0], 1)
        z1[1].start()
        zv[1].start()

    def sum_copy(which, src, dst, device):
        return pltpu.make_async_remote_copy(
            src, dst, sum_send.at[which], sum_recv.at[which], device_id=device, device_id_type=MESH)

    def all_in(which):
        _, count, _, me = members(which)

        @pl.when(me < count - 1)
        def _():
            pl.semaphore_wait(ready.at[1 + which], 1)

    def send_sums(which, first, last):
        axes, count, base, me = members(which)
        mine = slots.at[base + me]
        for k in range(first, min(last, count - 1)):
            other = jnp.where(k < me, k, k + 1)
            sum_copy(which, mine, mine, ring_device(axes, other)).start()

    def send_sum(which, value, last):
        _, _, base, me = members(which)
        for at in range(2):
            slots[base + me, at] = value[at][0]
        send_sums(which, 0, last)

    def all_sums(which):
        axes, count, base, me = members(which)
        others = slots.at[pl.ds(base, count - 1)]
        return sum_copy(which, others, others, ring_device(axes, lax.rem(me + 1, count)))

    def recv_sum(which):
        axes, count, base, me = members(which)
        all_sums(which).wait_recv()
        return [jnp.sum(slots[pl.ds(base, count), at], axis=0, keepdims=True) for at in range(2)]

    finish_x(blk.at[3, pl.ds(0, 2)], blk.at[3, 0], 0)
    flow = flow + weight[0] * stencil(0, 2) + weight[nx - 1] * stencil(nx - 1, 2)
    acc[...] = flow
    finish_y(yhalo.at[:, 3], yhalo.at[0, 3], 2)
    y_line = jnp.sum(cy_low * yhalo[0, 3] + cy_high * yhalo[1, 3], axis=0, keepdims=True)
    def across_edges():
        finish_x(blk.at[rest, pl.ds(0, 2)], blk.at[rest, 0], 1)
        for x in (0, nx - 1):
            stencil(x, 0)
            stencil(x, 1)

    pl.when(z_first)(across_edges)

    @pl.when(z_first)
    def _():
        face = pltpu.roll(zpack[0], nz - 1, 1)
        wpack[...] = face
        edge[...] = (time_step * viscosity) * face - (0.5 * time_step) * pltpu.roll(face, 3 * nx, 1)

    z1[0].wait_recv()
    acc[...] += c_low * zhalo[0]

    @pl.when(jnp.logical_not(z_last))
    def _():
        z1[1].wait_recv()
        acc[...] += c_high * zhalo[1]

    devices = gx * gy * gz

    def sum_up(last=devices):
        send_sum(0, (jnp.sum(acc[...], axis=0, keepdims=True) + y_line, void_line), last)

    for which in range(len(phases)):
        all_in(which)
    pl.when(jnp.logical_not(z_first))(sum_up)

    first_row = row == 0
    last_row = row == ny - 1
    first_lane = lane == 0
    last_lane = lane == nz - 1
    row_sign = jnp.where(first_row, 1.0, jnp.where(last_row, -1.0, 0.0))
    lane_sign = jnp.where(first_lane, 1.0, jnp.where(last_lane, -1.0, 0.0))
    row_sign, lane_sign = (s * (0.5 * time_step) for s in (row_sign, lane_sign))
    row_visc, lane_visc = (jnp.abs(s) * (2.0 * viscosity) for s in (row_sign, lane_sign))

    def unpack(which, at):
        return pltpu.roll(which, lax.rem(2 * nz - at, nz), 1)

    def rows(f, x):
        return jnp.where(
            row < ny // 2,
            jnp.broadcast_to(yhalo[0, f, pl.ds(x, 1), :], (ny, nz)),
            jnp.broadcast_to(yhalo[1, f, pl.ds(x, 1), :], (ny, nz)))

    def correct(x, which, components, with_rows=True):
        by_row = row_visc + row_sign * blk[2, x + 1]
        by_lane = lane_visc + lane_sign * blk[3, x + 1]
        inverse, v = inv[x], vp[0, x]
        for k in components:
            value = by_lane * unpack(which, (1 + k) * nx + x)
            if with_rows:
                value = value + by_row * rows(1 + k, x)
            if k == 1:
                value = value + row_sign * rows(0, x)
            if k == 2:
                value = value + lane_sign * unpack(which, x)
            value = ustar[k, x] + value * inverse
            ustar[k, x] = value
            flux[k, x] = v * value

    def correct_all(pair, components, with_rows=True, first=0, last=nx // 2, unroll=8):
        def body(i, carry):
            correct(2 * i, pair[0], components, with_rows)
            correct(2 * i + 1, pair[1], components, with_rows)
            return carry

        lax.fori_loop(first, last, body, 0, unroll=unroll)

    x2 = exchange(flux.at[0, 0], flux.at[0, nx - 1], fxhalo.at[0], fxhalo.at[1], 0, (8,), "gx", up_x, down_x)
    y2 = exchange(ypack.at[0, 4], ypack.at[1, 4], fyhalo.at[0], fyhalo.at[1], 1, (9,), "gy", up_y, down_y)
    z2 = exchange(fzpack.at[0], fzpack.at[1], fzhalo.at[0], fzhalo.at[1], 2, (10,), "gz", z_up, z_down)

    def send_flux_z():
        low, high = pack_z(1, lambda f, x: flux[2, x])
        fzpack[0] = low
        fzpack[1] = high
        for copy in z2:
            copy.start()

    def join():
        pair[0], pair[1] = interleave(pltpu.roll(zhalo[0], 1, 1), pltpu.roll(zhalo[1], nz - 1, 1))

    def correct_first():
        finish_y(yhalo.at[:, rest], yhalo.at[0, rest], 3)
        correct_all((pair[0], pair[1]), (0, 1), last=3 * (nx // 8), unroll=6)

    @pl.when(z_first)
    def _():
        edge[...] -= (0.5 * time_step) * zhalo[0] * wpack[...]
        join()
        correct_first()

    @pl.when(z_first)
    def _():
        zc.wait_recv()
    @pl.when(z_first)
    def _():
        product = whalo[...] * edge[...]
        acc[...] += product
        sum_up(plane - 1)
        edge[...] = jnp.where(lane < nx, pltpu.roll(product, nz - 3 * nx + 1, 1), 0.0)

    @pl.when(z_last)
    def _():
        correct_all(interleave(pltpu.roll(zhalo[0], 1, 1), zero), (2,))
        send_flux_z()

    pl.when(z_last)(z1[1].wait_recv)
    pl.when(not_first)(join)
    pl.when(not_first)(across_edges)
    pl.when(not_first)(correct_first)
    joined = pair[0], pair[1]
    correct_all(joined, (0, 1), first=3 * (nx // 8), unroll=4)
    ypack[0, 4] = flux[1, :, 0, :]
    ypack[1, 4] = flux[1, :, ny - 1, :]
    start(y2, not_high_y, not_low_y)
    start(x2, not_high_x, not_low_x)

    pl.when(z_first)(lambda: send_sums(0, plane - 1, devices))
    @pl.when(not_first)
    def _():
        edge[...] = zero

    @pl.when(z_last)
    def _():
        correct_all(interleave(zero, pltpu.roll(zhalo[1], nz - 1, 1)), (2,), False)

    @pl.when(not_last)
    def _():
        correct_all(joined, (2,))
        send_flux_z()

    for within, side in ((not_low_x, 0), (not_high_x, 1)):
        @pl.when(jnp.logical_not(within))
        def _():
            fxhalo[side] = zero
    for within, side in ((not_low_y, 0), (not_high_y, 1)):
        @pl.when(jnp.logical_not(within))
        def _():
            fyhalo[side] = jnp.zeros((nx, nz), jnp.float32)

    copy_to(vzpack, vzhalo, 2, 6, "gz", z_up).wait_recv()
    v_joined = interleave(pltpu.roll(vzhalo[0], 1, 1), pltpu.roll(vzhalo[1], nz - 1, 1))

    def source_plane(x, odd, x_low, x_high):
        fy, fz, v = flux[1, x], flux[2, x], vp[0, x]
        y_low = jnp.where(first_row, 0.0, pltpu.roll(fy, 1, 0))
        y_high = jnp.where(last_row, 0.0, pltpu.roll(fy, ny - 1, 0))
        z_low = jnp.where(first_lane, 0.0, pltpu.roll(fz, 1, 1))
        z_high = jnp.where(last_lane, 0.0, pltpu.roll(fz, nz - 1, 1))
        v_halo = unpack(v_joined[odd], x)
        v_low = jnp.where(first_lane, v_halo, pltpu.roll(v, 1, 1))
        v_high = jnp.where(last_lane, v_halo, pltpu.roll(v, nz - 1, 1))
        div[x] = 0.5 * ((x_high - x_low) + (y_high - y_low) + (z_high - z_low))
        slope[x] = (0.5 * time_step) * (v_high - v_low)

    def source_body(i, carry):
        x = 2 * i + 1
        source_plane(x, 1, flux[0, x - 1], flux[0, x + 1])
        source_plane(x + 1, 0, flux[0, x], flux[0, x + 2])
        return carry

    lax.fori_loop(0, nx // 2 - 1, source_body, 0, unroll=3)
    phase = 0
    while phase < len(phases) - 1:
        total = recv_sum(phase)
        phase += 1
        send_sum(phase, total, devices)
    finish_x(fxhalo, fxhalo.at[0], 8)
    source_plane(0, 0, fxhalo[0], flux[0, 1])
    source_plane(nx - 1, 1, flux[0, nx - 2], fxhalo[1])
    finish_y(fyhalo, fyhalo.at[0], 9)
    copy_to(fzpack, fzhalo, 2, 10, "gz", z_up).wait_recv()
    f_joined = interleave(pltpu.roll(fzhalo[0], 1, 1) + edge[...], pltpu.roll(fzhalo[1], nz - 1, 1))
    row_half, lane_half = row_sign / time_step, lane_sign / time_step

    def edge_plane(x, odd):
        y_halo = jnp.where(
            row < ny // 2,
            jnp.broadcast_to(fyhalo[0, pl.ds(x, 1), :], (ny, nz)),
            jnp.broadcast_to(fyhalo[1, pl.ds(x, 1), :], (ny, nz)))
        div[x] = div[x] - row_half * y_halo - lane_half * unpack(f_joined[odd], x)

    def edge_body(i, carry):
        edge_plane(2 * i, 0)
        edge_plane(2 * i + 1, 1)
        return carry

    lax.fori_loop(0, nx // 2, edge_body, 0, unroll=16)

    for which in range(len(phases)):
        all_sums(which).wait_send()
    sent = inv.at[pl.ds(0, 5)]
    settle(inv.at[pl.ds(0, 10)], sent, 0, 0, not_high_x, not_low_x, False)
    settle(ypack, ypack.at[0], 1, 2, not_high_y, not_low_y, False)
    sent = inv.at[pl.ds(0, 6)]
    copy_to(sent, sent, 2, 4, "gz", z_up).wait_send()
    pl.when(z_last)(zc.wait_send)

    total = recv_sum(phase)
    flow_sum, void_sum = (jnp.sum(t, axis=1, keepdims=True) for t in total)
    cells = float(nx * ny * nz * gx * gy * gz)
    step = (target[0] * cells - flow_sum) / (time_step * void_sum)
    lines[0] = jnp.broadcast_to(step, (1, nz)) + force
    lines[1] = jnp.broadcast_to(step, (1, nz))


def shift_kernel(ustar, div, slope, lines, vel_out, source_out, forcing_out, made, sem):
    nx, ny, nz = div.shape
    half = nx // 2
    across, line = pl.ds(0, 2), pltpu.make_async_copy(lines.at[0], forcing_out, sem.at[2])
    for k in range(2):
        for part in range(2):
            planes = pl.ds(part * half, half)
            pltpu.make_async_copy(ustar.at[k, planes], vel_out.at[k, planes], sem.at[0]).start()
    line.start()
    step = jnp.broadcast_to(lines[1], (ny, nz))
    for part in range(2):
        def body(i, carry):
            x = part * half + i
            made[0, x] = ustar[2, x] + time_step * step
            made[1, x] = div[x] + step * slope[x]
            return carry

        lax.fori_loop(0, half, body, 0, unroll=8)
        planes = pl.ds(part * half, half)
        pltpu.make_async_copy(made.at[0, planes], vel_out.at[2, planes], sem.at[1]).start()
        pltpu.make_async_copy(made.at[1, planes], source_out.at[planes], sem.at[1]).start()
    pltpu.make_async_copy(ustar.at[across], vel_out.at[across], sem.at[0]).wait()
    pltpu.make_async_copy(made, vel_out.at[across], sem.at[1]).wait()
    line.wait()


def local(velocity, pressure, voidage, particle_vel, forcing, target_flux):
    nx, ny, nz = voidage.shape
    sizes = tuple(lax.axis_size(a) for a in ("gx", "gy", "gz"))
    if math.prod(sizes) <= DIRECT_LIMIT:
        phases = (("gz", "gy", "gx"),)
    else:
        phases = (("gy", "gx"), ("gz",))
    slot_count = sum(math.prod(lax.axis_size(a) for a in axes) for axes in phases)
    f32 = jnp.float32
    vmem = pl.BlockSpec(memory_space=pltpu.VMEM)
    smem = pl.BlockSpec(memory_space=pltpu.SMEM)
    hbm = pl.BlockSpec(memory_space=pltpu.HBM)
    dma = pltpu.SemaphoreType.DMA
    faces = [pltpu.VMEM((2, ny, nz), f32), pltpu.VMEM((2, ny, nz), f32)]
    face = [pltpu.VMEM((ny, nz), f32)]
    results = pl.pallas_call(
        functools.partial(kernel, sizes, phases),
        out_shape=(
            pltpu.VMEM((3, nx, ny, nz), f32),
            pltpu.VMEM((nx, ny, nz), f32),
            pltpu.VMEM((nx, ny, nz), f32),
            pltpu.VMEM((2, 1, nz), f32),
        ),
        in_specs=[hbm] * 4 + [smem] * 2,
        out_specs=(vmem,) * 4,
        scratch_shapes=[
            pltpu.VMEM((4, nx + 2, ny, nz), f32),
            pltpu.VMEM((4, nx, ny, nz), f32),
            pltpu.VMEM((nx, ny, nz), f32),
            pltpu.VMEM((nx, ny, nz), f32),
            pltpu.VMEM((3, nx, ny, nz), f32),
        ] + face + face + faces[:1] + [
            pltpu.VMEM((2, 5, nx, nz), f32),
            pltpu.VMEM((2, 4, nx, nz), f32),
        ] + faces + face + face + faces + [
            pltpu.VMEM((2, nx, nz), f32),
            pltpu.VMEM((2, ny, nz), f32),
        ] + faces + [
            pltpu.VMEM((slot_count, 2, nz), f32),
            dma((2,)), dma((4,)), dma((11,)),
            dma((len(phases),)), dma((len(phases),)),
            pltpu.SemaphoreType.REGULAR((1 + len(phases),)),
        ],
        compiler_params=pltpu.CompilerParams(collective_id=0, has_side_effects=True),
    )(velocity, pressure, voidage, particle_vel, forcing, target_flux)
    vel_new, source, forcing_new = pl.pallas_call(
        shift_kernel,
        out_shape=(
            jax.ShapeDtypeStruct((3, nx, ny, nz), f32),
            jax.ShapeDtypeStruct((nx, ny, nz), f32),
            jax.ShapeDtypeStruct((1, nz), f32),
        ),
        in_specs=[vmem] * 4,
        out_specs=(hbm,) * 3,
        scratch_shapes=[
            pltpu.VMEM((2, nx, ny, nz), f32),
            dma((3,)),
        ],
    )(*(pltpu.with_memory_space_constraint(a, pltpu.VMEM) for a in results))
    return vel_new, source, forcing_new[0, :1]


def solution(mesh):
    return jax.shard_map(
        local,
        mesh=mesh,
        in_specs=(
            P(None, "gx", "gy", "gz"),
            P("gx", "gy", "gz"),
            P("gx", "gy", "gz"),
            P(None, "gx", "gy", "gz"),
            P(),
            P(),
        ),
        out_specs=(P(None, "gx", "gy", "gz"), P("gx", "gy", "gz"), P()),
        check_vma=False,
    )
```
